512 devices in a mesh: gx: 16 (over z, core), gy: 4 (over x), gz: 8 (over y).
Axes of the slice: x: 4, y: 8, z: 8, core: 2. Of those that a mesh axis runs over, the one named last changes fastest.
Arguments:
- krylov_basis: float32 [60, 64, 32, 1024], P(None, 'gx', 'gy', 'gz'), may hold values from -6 to 6
- schur_vectors: float32 [60, 20], replicated, may hold values from -1 to 1, as said below
- next_vector: float32 [64, 32, 1024], P('gx', 'gy', 'gz'), may hold values from -10 to 10
- diag_shift: float32 [64, 32, 1024], P('gx', 'gy', 'gz'), may hold values from 0.25 to 2
- velocity: float32 [3, 64, 32, 1024], P(None, 'gx', 'gy', 'gz'), may hold values from -1 to 1
Outputs:
- new_basis: float32 [24, 64, 32, 1024], P(None, 'gx', 'gy', 'gz')
- hessenberg: float32 [24, 3], replicated
The draws below stay inside these ranges and needn't reach their ends.
Inputs may be any that keep to these rules, and one draw needn't show every extreme that they name: `schur_vectors`: the columns are orthonormal.
All inputs are finite; a program needn't handle non-finite values.
Results may differ from the reference program's by a relative error of at most 0.0003.
Values sent between devices are 32-bit elements; how exact they have to be, the bound alone decides.
No kernel may reach another device: no remote copies, remote signals or barrier semaphores. Data moves between devices by JAX's collectives and lax.ppermute only.
A program may use at most 64 MiB of HBM per device.

```python
import jax
import jax.numpy as jnp
from jax import lax

BASIS = 60
KEEP = 20
EXPAND = 3
ROWS = 24
NX = 64
NY = 32
NZ = 1024


def draw_schur_vectors(key, part):
    gaussian = jax.random.normal(key, (BASIS, KEEP), jnp.float32)
    orthonormal, triangle = jnp.linalg.qr(gaussian)
    return orthonormal.astype(jnp.float32)


def levels(stream_key, shape, split, least, largest):
    level = 1.0
    for axis_at, parts in split:
        heights = jax.random.uniform(jax.random.fold_in(jax.random.fold_in(stream_key, 6), axis_at), (parts,), jnp.float32, least / len(split), largest / len(split))
        level = level * jnp.repeat(jnp.exp(heights), shape[axis_at] // parts).reshape((-1,) + (1,) * (len(shape) - 1 - axis_at))
    return level


def noise(key, extent, scale, bound, shards=(), dtype=jnp.bfloat16):
    factor_of = levels(key, extent, shards, -0.22, 0.18) if shards else 1.0
    entries = jax.random.normal(key, extent, jnp.float32) * scale * factor_of
    return jnp.minimum(jnp.maximum(entries, -bound), bound).astype(dtype)


def setup_inputs(seed: int = 0) -> dict:
    key_list = jax.random.split(jax.random.key(seed), 6)
    krylov_basis = noise(key_list[0], (BASIS, NX, NY, NZ), 1.0, 6.0, ((1, 16), (2, 4), (3, 8)), jnp.float32)
    schur_vectors = draw_schur_vectors(jax.random.fold_in(key_list[5], 71), 0)
    next_vector = noise(key_list[2], (NX, NY, NZ), 2.0, 10.0, ((0, 16), (1, 4), (2, 8)), jnp.float32)
    diag_shift = jnp.clip(0.25 + 1.75 * jax.random.uniform(key_list[3], (NX, NY, NZ), jnp.float32) ** levels(key_list[3], (NX, NY, NZ), ((0, 16), (1, 4), (2, 8)), -0.2, 0.2), 0.25, 2.0)
    velocity = jnp.clip(jax.random.uniform(key_list[4], (3, NX, NY, NZ), jnp.float32, -1.0, 1.0) * levels(key_list[4], (3, NX, NY, NZ), ((1, 16), (2, 4), (3, 8)), -0.4, 0.0), -1.0, 1.0)
    return {"krylov_basis": krylov_basis, "schur_vectors": schur_vectors, "next_vector": next_vector, "diag_shift": diag_shift, "velocity": velocity}


def operate_field(field, diag_shift, velocity):
    padded = jnp.pad(field, 1)
    x_ahead = padded[2:, 1:-1, 1:-1]
    x_behind = padded[:-2, 1:-1, 1:-1]
    y_ahead = padded[1:-1, 2:, 1:-1]
    y_behind = padded[1:-1, :-2, 1:-1]
    z_ahead = padded[1:-1, 1:-1, 2:]
    z_behind = padded[1:-1, 1:-1, :-2]
    neighbours = x_ahead + x_behind + y_ahead + y_behind + z_ahead + z_behind
    flow = velocity[0] * (x_ahead - x_behind) + velocity[1] * (y_ahead - y_behind) + velocity[2] * (z_ahead - z_behind)
    return (6.0 + diag_shift) * field - neighbours + 0.5 * flow

def reference(krylov_basis, schur_vectors, next_vector, diag_shift, velocity):
    highest = lax.Precision.HIGHEST
    cell_count = NX * NY * NZ
    rotated = jnp.einsum('ik,ixyz->kxyz', schur_vectors, krylov_basis, precision=highest)
    norm_sq = jnp.sum(next_vector * next_vector) / cell_count
    first = next_vector / jnp.maximum(jnp.sqrt(norm_sq), 0.5)
    vectors = jnp.concatenate([rotated, first[None]], axis=0)
    columns = []
    for expansion in range(EXPAND):
        count = vectors.shape[0]
        flat_basis = vectors.reshape(count, -1)
        applied = operate_field(vectors[-1], diag_shift, velocity).reshape(-1)
        first_coeffs = jnp.dot(flat_basis, applied, precision=highest) / cell_count
        partly = applied - jnp.dot(first_coeffs, flat_basis, precision=highest)
        second_coeffs = jnp.dot(flat_basis, partly, precision=highest) / cell_count
        cleaned = partly - jnp.dot(second_coeffs, flat_basis, precision=highest)
        length = jnp.sqrt(jnp.sum(cleaned * cleaned) / cell_count)
        column = jnp.zeros((ROWS,), jnp.float32)
        column = column.at[:count].set(first_coeffs + second_coeffs).at[count].set(length)
        columns.append(column)
        newest = (cleaned / jnp.maximum(length, 0.5)).reshape(NX, NY, NZ)
        vectors = jnp.concatenate([vectors, newest[None]], axis=0)
    return (vectors, jnp.stack(columns, axis=1))
```

```python
import functools

import jax
import jax.numpy as jnp
from jax import lax
from jax.experimental import pallas as pl
from jax.experimental.pallas import tpu as pltpu
from jax.sharding import Mesh
from jax.sharding import PartitionSpec as P

KEEP = 20
EXPAND = 3
ROWS = 24
FIELDS = 25
SPAN = 64
SIGMA = 7.125
GX = ("gx_0", "gx_1")
X, Y, Z = (4, 8, 128)
TILE = (Y, Z)
F32 = jnp.float32


def rows_of():
    return lax.broadcasted_iota(jnp.int32, TILE, 0)


def lanes_of():
    return lax.broadcasted_iota(jnp.int32, TILE, 1)


def shift_rows(tile, by):
    by = by % Y
    return tile if by == 0 else pltpu.roll(tile, by, 0)


def shift_lanes(tile, by):
    return pltpu.roll(tile, by, 1)


def vmem():
    return pl.BlockSpec(memory_space=pltpu.VMEM)


def call(kernel, outs, args, scratch=(), smem=(), flops=100000):
    return pl.pallas_call(
        kernel,
        out_shape=[jax.ShapeDtypeStruct(s, F32) for s in outs],
        in_specs=[
            pl.BlockSpec(memory_space=pltpu.SMEM) if i in smem else vmem() for i in range(len(args))
        ],
        out_specs=[vmem() for _ in outs],
        scratch_shapes=list(scratch),
        cost_estimate=pl.CostEstimate(flops=flops, bytes_accessed=100000, transcendentals=0),
    )(*args)


def rotate_kernel(basis, schur, next_vector, diag, velocity, fields, packed):
    group = 5
    for g in range(KEEP // group):

        def body(i, acc, g=g):
            out = []
            tiles = [basis[i, x] for x in range(X)]
            for f in range(group):
                w = schur[i, g * group + f]
                for x in range(X):
                    out.append(acc[f * X + x] + w * tiles[x])
            return tuple(out)

        zero = tuple(jnp.zeros(TILE, F32) for _ in range(group * X))
        acc = lax.fori_loop(0, basis.shape[0], body, zero, unroll=4)
        for f in range(group):
            for x in range(X):
                fields[g * group + f, x] = acc[f * X + x]
    for x in range(X):
        fields[20, x] = next_vector[x]
        fields[21, x] = 6.0 + diag[x]
        for d in range(3):
            fields[22 + d, x] = 0.5 * velocity[d, x]
    lane = lanes_of()
    for p in range(5):
        total = jnp.zeros(TILE, F32)
        for j in range(20):
            tile = fields[5 * p + j // 4, j % 4]
            moved = shift_lanes(tile, 6 * j + 3)
            total = jnp.where((lane >= 6 * j) & (lane < 6 * j + 6), moved, total)
        packed[p] = total


def pack_y_kernel(fields, from_lo, from_hi, up, down, halo):
    row, lane = rows_of(), lanes_of()
    left = lax.rem(lane, 6) < 3
    for f in range(FIELDS):
        a = jnp.zeros(TILE, F32)
        b = a
        for x in range(X):
            tile = fields[f, x]
            here = (row >= 2 * x) & (row < 2 * x + 2)
            a = jnp.where(here, shift_rows(tile, 2 * x - 6), a)
            b = jnp.where(here, shift_rows(tile, 2 * x), b)
        up[f] = a
        down[f] = b
    a = jnp.zeros(TILE, F32)
    b = a
    for x in range(X):
        tile = fields[20, x]
        a = jnp.where(row == x, shift_rows(tile, x - 5), a)
        b = jnp.where(row == x, shift_rows(tile, x - 2), b)
    up[25] = a
    down[25] = b
    for p in range(5):
        merged = jnp.where(left, from_lo[p], from_hi[p])
        halo[p] = merged
        up[26 + p] = merged
        down[26 + p] = merged


def pack_x_kernel(fields, halo, y_lo, y_hi, up, down):
    first = rows_of() < 4
    for f in range(FIELDS):
        up[2 * f] = fields[f, 2]
        up[2 * f + 1] = fields[f, 3]
        down[2 * f] = fields[f, 0]
        down[2 * f + 1] = fields[f, 1]
        lo, hi = y_lo[f], y_hi[f]
        up[51 + f] = jnp.where(first, shift_rows(lo, 4), hi)
        down[51 + f] = jnp.where(first, lo, shift_rows(hi, 4))
    up[50] = fields[20, 1]
    down[50] = fields[20, 2]
    for out in (up, down):
        for p in range(5):
            out[76 + p] = halo[p]
        out[81] = y_lo[30]
        out[82] = y_hi[30]


def region(radius):
    out = []
    for a, b in ((0, 0), (1, 0), (0, 1), (1, 1)):
        for x in range(-radius + a + b, X + radius - a - b):
            out.append((x, a, b))
    return out


COEF = region(2)


def tile_of(f, key, refs):
    fields, halo, y_lo, y_hi, x_lo, x_hi, y_halo, x_corner = refs
    x, a, b = key
    first = rows_of() < 4
    if b == 0:
        if a == 0:
            if 0 <= x < X:
                return fields[f, x]
            if x == -3:
                return x_lo[50]
            if x == 6:
                return x_hi[50]
            return x_lo[2 * f + x + 2] if x < 0 else x_hi[2 * f + x - 4]
        if 0 <= x < X:
            lo, hi = y_lo[f], y_hi[f]
            tile = jnp.where(first, shift_rows(hi, -2 * x), shift_rows(lo, 6 - 2 * x))
            if isinstance(f, int) and f == 20:
                row = rows_of()
                tile = jnp.where(row == 2, shift_rows(y_hi[25], 2 - x), tile)
                tile = jnp.where(row == 5, shift_rows(y_lo[25], 5 - x), tile)
            return tile
        packed = (x_lo if x < 0 else x_hi)[51 + f]
        if x in (-1, 5):
            return jnp.where(first, shift_rows(packed, 2), shift_rows(packed, 4))
        return jnp.where(first, shift_rows(packed, 4), shift_rows(packed, 6))
    p, q = (f // 5, f % 5) if isinstance(f, int) else (lax.div(f, 5), lax.rem(f, 5))
    place = x if 0 <= x < X else (x + X if x < 0 else x - X)
    by = 128 - 3 - 6 * (4 * q + place)
    if a == 0:
        packed = halo[p] if 0 <= x < X else (x_lo if x < 0 else x_hi)[76 + p]
    elif 0 <= x < X:
        packed = y_halo[p]
    else:
        packed = x_corner[0 if x < 0 else 1]
    return shift_lanes(packed, by)


def apply(get, key, coef):
    x, a, b = key
    row, lane = rows_of(), lanes_of()
    base = COEF.index(key)
    centre = get((x, a, b))
    y_other = get((x, 1 - a, b))
    z_other = get((x, a, 1 - b))
    y_ahead = shift_rows(jnp.where(row == 0, y_other, centre), 7)
    y_behind = shift_rows(jnp.where(row == 7, y_other, centre), 1)
    z_ahead = shift_lanes(jnp.where(lane == 0, z_other, centre), 127)
    z_behind = shift_lanes(jnp.where(lane == 127, z_other, centre), 1)
    near = (
        centre,
        get((x + 1, a, b)),
        get((x - 1, a, b)),
        y_ahead,
        y_behind,
        z_ahead,
        z_behind,
    )
    terms = [coef[base, i] * near[i] for i in range(7)]
    return (terms[0] + (terms[1] + terms[2])) + ((terms[3] + terms[4]) + (terms[5] + terms[6]))


def stencil_kernel(
    copies, fields, halo, y_lo, y_hi, x_lo, x_hi, span, gram, coef, y_halo, x_corner, chain
):
    refs = (fields, halo, y_lo, y_hi, x_lo, x_hi, y_halo, x_corner)
    first = rows_of() < 4
    for p in range(5):
        y_halo[p] = jnp.where(first, y_hi[26 + p], y_lo[26 + p])
    x_corner[0] = jnp.where(first, x_lo[82], x_lo[81])
    x_corner[1] = jnp.where(first, x_hi[82], x_hi[81])
    for at, key in enumerate(COEF):
        diagonal = tile_of(21, key, refs)
        inside = diagonal != 0.0
        coef[at, 0] = jnp.where(inside, diagonal - SIGMA, 0.0)
        for d in range(3):
            half = tile_of(22 + d, key, refs)
            coef[at, 1 + 2 * d] = jnp.where(inside, half - 1.0, 0.0)
            coef[at, 2 + 2 * d] = jnp.where(inside, -1.0 - half, 0.0)

    def store(f, x, tile):
        at = f * (X * Y) + x * Y
        if not isinstance(f, int):
            at = pl.multiple_of(at, Y)
        span[pl.ds(at, Y), :] = tile

    tiles = {key: tile_of(20, key, refs) for key in region(3)}
    for x in range(X):
        store(60, x, tiles[(x, 0, 0)])
    for step in range(EXPAND):
        place = {}
        for at, key in enumerate(tiles):
            chain[at] = tiles[key]
            place[key] = at
        get = lambda key, place=place: chain[place[key]]
        tiles = {key: apply(get, key, coef) for key in region(2 - step)}
        for x in range(X):
            store(61 + step, x, tiles[(x, 0, 0)])

    def body(f, carry):
        held = {}

        def get(key):
            if key not in held:
                held[key] = tile_of(f, key, refs)
            return held[key]

        once = {key: apply(get, key, coef) for key in region(1)}
        for x in range(X):
            store(f, x, get((x, 0, 0)))
            store(f + 20, x, once[(x, 0, 0)])
        for x in range(X):
            store(f + 40, x, apply(once.__getitem__, (x, 0, 0), coef))
        return carry

    lax.fori_loop(0, KEEP, body, 0)

    total = jnp.zeros((SPAN, SPAN), F32)
    for r in range(0, X * Y, 2):
        pair = [span[pl.ds(r + i, SPAN, stride=X * Y), :] for i in range(2)]
        rows = jnp.concatenate(pair, axis=1)
        total = total + lax.dot_general(
            rows,
            rows,
            (((1,), (1,)), ((), ())),
            precision=lax.Precision.HIGHEST,
            preferred_element_type=F32,
        )
    packed = jnp.concatenate([total[:32], total[32:]], axis=1)
    for i in range(copies):
        gram[i] = packed


def sum_kernel(copies, parts, out):
    total = parts[0]
    for i in range(1, parts.shape[0]):
        total = total + parts[i]
    for i in range(copies):
        out[i] = total


def exchange(parts, axis):
    return lax.all_to_all(parts, axis, 0, 0)


def finish_kernel(cell_count, parts, span, basis, hessenberg, spread):
    total = parts[0]
    for i in range(1, parts.shape[0]):
        total = total + parts[i]
    total = total * (1.0 / cell_count)
    lane = lax.broadcasted_iota(jnp.int32, (32, Z), 1)
    gram = jnp.concatenate(
        [jnp.where(lane < SPAN, total, 0.0), jnp.where(lane < SPAN, pltpu.roll(total, 64, 1), 0.0)],
        axis=0,
    )
    row64 = lax.broadcasted_iota(jnp.int32, (SPAN, Z), 0)
    lane64 = lax.broadcasted_iota(jnp.int32, (SPAN, Z), 1)
    eye = row64 == lane64
    row = lax.broadcasted_iota(jnp.int32, (ROWS, Z), 0)
    lane = lax.broadcasted_iota(jnp.int32, (ROWS, Z), 1)
    lane1 = lax.broadcasted_iota(jnp.int32, (1, Z), 1)

    def column(vector):
        return jnp.sum(jnp.where(eye, vector, 0.0), axis=1, keepdims=True)

    first_row = gram[60:61, :]
    norm_sq = jnp.sum(jnp.where(lane1 == 60, first_row, 0.0), axis=1, keepdims=True)
    inverse = 1.0 / jnp.maximum(jnp.sqrt(norm_sq), 0.5)
    last = jnp.where(lane1 == 60, inverse, 0.0)
    last_gram = first_row * inverse
    q = jnp.where((row == lane) & (row < KEEP), 1.0, 0.0)
    q = jnp.where(row == KEEP, last, q)
    qg = jnp.where(row < KEEP, gram[:ROWS, :], 0.0)
    qg = jnp.where(row == KEEP, last_gram, qg)
    spread[3] = jnp.broadcast_to(inverse, TILE)
    columns = []
    for k in range(EXPAND):
        up = jnp.where(
            (lane1 >= KEEP) & (lane1 < 60),
            pltpu.roll(last, KEEP, 1),
            jnp.where((lane1 > 60) & (lane1 < SPAN), pltpu.roll(last, 1, 1), 0.0),
        )
        image = up + SIGMA * last
        image_gram = jnp.sum(column(up) * gram, axis=0, keepdims=True) + SIGMA * last_gram
        c = jnp.sum(q * image_gram, axis=1, keepdims=True)
        partly = image - jnp.sum(c * q, axis=0, keepdims=True)
        partly_gram = image_gram - jnp.sum(c * qg, axis=0, keepdims=True)
        e = jnp.sum(q * partly_gram, axis=1, keepdims=True)
        cleaned = partly - jnp.sum(e * q, axis=0, keepdims=True)
        cleaned_gram = partly_gram - jnp.sum(e * qg, axis=0, keepdims=True)
        length_sq = jnp.sum(cleaned * cleaned_gram, axis=1, keepdims=True)
        length = jnp.sqrt(jnp.maximum(length_sq, 0.0))
        inverse = 1.0 / jnp.maximum(length, 0.5)
        last = cleaned * inverse
        last_gram = cleaned_gram * inverse
        q = jnp.where(row == KEEP + 1 + k, last, q)
        qg = jnp.where(row == KEEP + 1 + k, last_gram, qg)
        columns.append(jnp.where(row == KEEP + 1 + k, length, c + e))
        spread[pl.ds(4 + 8 * k, 8)] = jnp.broadcast_to(column(last), (SPAN, Z)).reshape(8, 8, Z)
    hessenberg[...] = jnp.where(lane == 0, columns[0], jnp.where(lane == 1, columns[1], columns[2]))[
        :, :EXPAND
    ]

    for f in range(KEEP):
        basis[f] = span[f]
    for x in range(X):
        basis[KEEP, x] = span[60, x] * spread[3]
    acc = [[jnp.zeros(TILE, F32) for _ in range(X)] for _ in range(EXPAND)]
    for f in range(SPAN):
        tiles = [span[f, x] for x in range(X)]
        for k in range(EXPAND):
            w = spread[4 + 8 * k + f // 8, f % 8 : f % 8 + 1, :]
            for x in range(X):
                acc[k][x] = acc[k][x] + w * tiles[x]
    for k in range(EXPAND):
        for x in range(X):
            basis[KEEP + 1 + k, x] = acc[k][x]


def send(value, axis, forward):
    count = lax.axis_size(axis)
    up = [(i, i + 1) for i in range(count - 1)]
    return lax.ppermute(value, axis, up if forward else [(j, i) for i, j in up])


def per_device(krylov_basis, schur_vectors, next_vector, diag_shift, velocity):
    axes = (*GX, "gy", "gz")
    cell_count = next_vector.size
    for axis in axes:
        cell_count *= lax.axis_size(axis)
    fields, packed = call(
        rotate_kernel,
        [(FIELDS, X, Y, Z), (5, Y, Z)],
        [krylov_basis, schur_vectors, next_vector, diag_shift, velocity],
        smem=(1,),
    )
    z_lo, z_hi = send(packed, "gz", True), send(packed, "gz", False)
    up, down, halo = call(
        pack_y_kernel, [(31, Y, Z), (31, Y, Z), (5, Y, Z)], [fields, z_lo, z_hi]
    )
    y_lo, y_hi = send(up, "gy", True), send(down, "gy", False)
    up, down = call(pack_x_kernel, [(83, Y, Z), (83, Y, Z)], [fields, halo, y_lo, y_hi])
    x_lo, x_hi = send(up, GX, True), send(down, GX, False)
    stages = (("gx_1", "gy"), ("gz",), ("gx_0",))
    sizes = []
    for stage in stages:
        size = 1
        for axis in stage:
            size *= lax.axis_size(axis)
        sizes.append(size)
    span, parts = call(
        functools.partial(stencil_kernel, sizes[0]),
        [(SPAN * X * Y, Z), (sizes[0], 32, Z)],
        [fields, halo, y_lo, y_hi, x_lo, x_hi],
        scratch=[
            pltpu.VMEM((len(COEF), 7, Y, Z), F32),
            pltpu.VMEM((5, Y, Z), F32),
            pltpu.VMEM((2, Y, Z), F32),
            pltpu.VMEM((len(region(3)), Y, Z), F32),
        ],
    )
    for i, stage in enumerate(stages):
        parts = exchange(parts, stage)
        if i + 1 < len(stages):
            (parts,) = call(
                functools.partial(sum_kernel, sizes[i + 1]), [(sizes[i + 1], 32, Z)], [parts]
            )
    basis, hessenberg = call(
        functools.partial(finish_kernel, cell_count),
        [(ROWS, X, Y, Z), (ROWS, EXPAND)],
        [parts, span.reshape(SPAN, X, Y, Z)],
        scratch=[pltpu.VMEM((4 + 8 * EXPAND, Y, Z), F32)],
    )
    return basis, hessenberg


def solution(mesh):
    split = Mesh(
        mesh.devices.reshape(-1, 2, mesh.shape["gy"], mesh.shape["gz"]),
        ("gx_0", "gx_1", "gy", "gz"),
    )
    return jax.shard_map(
        per_device,
        mesh=split,
        in_specs=(
            P(None, GX, "gy", "gz"),
            P(),
            P(GX, "gy", "gz"),
            P(GX, "gy", "gz"),
            P(None, GX, "gy", "gz"),
        ),
        out_specs=(P(None, GX, "gy", "gz"), P()),
        check_vma=False,
    )
```

```python
import functools

import jax
import jax.numpy as jnp
from jax import lax
from jax.experimental import pallas as pl
from jax.experimental.pallas import tpu as pltpu
from jax.sharding import Mesh
from jax.sharding import PartitionSpec as P

KEEP = 20
EXPAND = 3
ROWS = 24
FIELDS = 25
SPAN = 64
SIGMA = 7.125
GX = ("gx_0", "gx_1")
X, Y, Z = (4, 8, 128)
TILE = (Y, Z)
F32 = jnp.float32


def rows_of():
    return lax.broadcasted_iota(jnp.int32, TILE, 0)


def lanes_of():
    return lax.broadcasted_iota(jnp.int32, TILE, 1)


def shift_rows(tile, by):
    by = by % Y
    return tile if by == 0 else pltpu.roll(tile, by, 0)


def shift_lanes(tile, by):
    return pltpu.roll(tile, by, 1)


def vmem():
    return pl.BlockSpec(memory_space=pltpu.VMEM)


def call(kernel, outs, args, scratch=(), smem=(), flops=100000, limit=2):
    return pl.pallas_call(
        kernel,
        out_shape=[jax.ShapeDtypeStruct(s, F32) for s in outs],
        in_specs=[
            pl.BlockSpec(memory_space=pltpu.SMEM) if i in smem else vmem() for i in range(len(args))
        ],
        out_specs=[vmem() for _ in outs],
        scratch_shapes=list(scratch),
        cost_estimate=pl.CostEstimate(flops=flops, bytes_accessed=100000, transcendentals=0),
        compiler_params=pltpu.CompilerParams(vmem_limit_bytes=limit * 2**20),
    )(*args)


def rotate_kernel(basis, schur, next_vector, diag, velocity, fields, packed):
    group = 5
    for g in range(KEEP // group):

        def body(i, acc, g=g):
            out = []
            tiles = [basis[i, x] for x in range(X)]
            for f in range(group):
                w = schur[g * group + f, i]
                for x in range(X):
                    out.append(acc[f * X + x] + w * tiles[x])
            return tuple(out)

        zero = tuple(jnp.zeros(TILE, F32) for _ in range(group * X))
        acc = lax.fori_loop(0, basis.shape[0], body, zero, unroll=4)
        for f in range(group):
            for x in range(X):
                fields[g * group + f, x] = acc[f * X + x]
    for x in range(X):
        fields[20, x] = next_vector[x]
        fields[21, x] = 6.0 + diag[x]
        for d in range(3):
            fields[22 + d, x] = 0.5 * velocity[d, x]
    lane = lanes_of()
    for p in range(5):
        total = jnp.zeros(TILE, F32)
        for j in range(20):
            tile = fields[5 * p + j // 4, j % 4]
            moved = shift_lanes(tile, 6 * j + 3)
            total = jnp.where((lane >= 6 * j) & (lane < 6 * j + 6), moved, total)
        packed[p] = total


def pack_y_kernel(fields, from_lo, from_hi, up, down, halo):
    row, lane = rows_of(), lanes_of()
    left = lax.rem(lane, 6) < 3
    for f in range(FIELDS):
        a = jnp.zeros(TILE, F32)
        b = a
        for x in range(X):
            tile = fields[f, x]
            here = (row >= 2 * x) & (row < 2 * x + 2)
            a = jnp.where(here, shift_rows(tile, 2 * x - 6), a)
            b = jnp.where(here, shift_rows(tile, 2 * x), b)
        up[f] = a
        down[f] = b
    a = jnp.zeros(TILE, F32)
    b = a
    for x in range(X):
        tile = fields[20, x]
        a = jnp.where(row == x, shift_rows(tile, x - 5), a)
        b = jnp.where(row == x, shift_rows(tile, x - 2), b)
    up[25] = a
    down[25] = b
    for p in range(5):
        merged = jnp.where(left, from_lo[p], from_hi[p])
        halo[p] = merged
        up[26 + p] = merged
        down[26 + p] = merged


def pack_x_kernel(fields, halo, y_lo, y_hi, up, down):
    first = rows_of() < 4
    for f in range(FIELDS):
        up[2 * f] = fields[f, 2]
        up[2 * f + 1] = fields[f, 3]
        down[2 * f] = fields[f, 0]
        down[2 * f + 1] = fields[f, 1]
        lo, hi = y_lo[f], y_hi[f]
        up[51 + f] = jnp.where(first, shift_rows(lo, 4), hi)
        down[51 + f] = jnp.where(first, lo, shift_rows(hi, 4))
    up[50] = fields[20, 1]
    down[50] = fields[20, 2]
    for out in (up, down):
        for p in range(5):
            out[76 + p] = halo[p]
        out[81] = y_lo[30]
        out[82] = y_hi[30]


def region(radius):
    out = []
    for a, b in ((0, 0), (1, 0), (0, 1), (1, 1)):
        for x in range(-radius + a + b, X + radius - a - b):
            out.append((x, a, b))
    return out


COEF = region(2)


def tile_of(f, key, refs):
    fields, halo, y_lo, y_hi, x_lo, x_hi, y_halo, x_corner = refs
    x, a, b = key
    first = rows_of() < 4
    if b == 0:
        if a == 0:
            if 0 <= x < X:
                return fields[f, x]
            if x == -3:
                return x_lo[50]
            if x == 6:
                return x_hi[50]
            return x_lo[2 * f + x + 2] if x < 0 else x_hi[2 * f + x - 4]
        if 0 <= x < X:
            lo, hi = y_lo[f], y_hi[f]
            tile = jnp.where(first, shift_rows(hi, -2 * x), shift_rows(lo, 6 - 2 * x))
            if isinstance(f, int) and f == 20:
                row = rows_of()
                tile = jnp.where(row == 2, shift_rows(y_hi[25], 2 - x), tile)
                tile = jnp.where(row == 5, shift_rows(y_lo[25], 5 - x), tile)
            return tile
        packed = (x_lo if x < 0 else x_hi)[51 + f]
        if x in (-1, 5):
            return jnp.where(first, shift_rows(packed, 2), shift_rows(packed, 4))
        return jnp.where(first, shift_rows(packed, 4), shift_rows(packed, 6))
    p, q = (f // 5, f % 5) if isinstance(f, int) else (lax.div(f, 5), lax.rem(f, 5))
    place = x if 0 <= x < X else (x + X if x < 0 else x - X)
    by = 128 - 3 - 6 * (4 * q + place)
    if a == 0:
        packed = halo[p] if 0 <= x < X else (x_lo if x < 0 else x_hi)[76 + p]
    elif 0 <= x < X:
        packed = y_halo[p]
    else:
        packed = x_corner[0 if x < 0 else 1]
    return shift_lanes(packed, by)


def apply(get, key, coef):
    x, a, b = key
    row, lane = rows_of(), lanes_of()
    base = COEF.index(key)
    centre = get((x, a, b))
    y_other = get((x, 1 - a, b))
    z_other = get((x, a, 1 - b))
    y_ahead = shift_rows(jnp.where(row == 0, y_other, centre), 7)
    y_behind = shift_rows(jnp.where(row == 7, y_other, centre), 1)
    z_ahead = shift_lanes(jnp.where(lane == 0, z_other, centre), 127)
    z_behind = shift_lanes(jnp.where(lane == 127, z_other, centre), 1)
    near = (
        centre,
        get((x + 1, a, b)),
        get((x - 1, a, b)),
        y_ahead,
        y_behind,
        z_ahead,
        z_behind,
    )
    terms = [coef[base, i] * near[i] for i in range(7)]
    return (terms[0] + (terms[1] + terms[2])) + ((terms[3] + terms[4]) + (terms[5] + terms[6]))


def stencil_kernel(
    copies, fields, halo, y_lo, y_hi, x_lo, x_hi, span, gram, coef, y_halo, x_corner, chain
):
    refs = (fields, halo, y_lo, y_hi, x_lo, x_hi, y_halo, x_corner)
    first = rows_of() < 4
    for p in range(5):
        y_halo[p] = jnp.where(first, y_hi[26 + p], y_lo[26 + p])
    x_corner[0] = jnp.where(first, x_lo[82], x_lo[81])
    x_corner[1] = jnp.where(first, x_hi[82], x_hi[81])
    for at, key in enumerate(COEF):
        diagonal = tile_of(21, key, refs)
        inside = diagonal != 0.0
        coef[at, 0] = jnp.where(inside, diagonal - SIGMA, 0.0)
        for d in range(3):
            half = tile_of(22 + d, key, refs)
            coef[at, 1 + 2 * d] = jnp.where(inside, half - 1.0, 0.0)
            coef[at, 2 + 2 * d] = jnp.where(inside, -1.0 - half, 0.0)

    def store(f, x, tile):
        at = f * (X * Y) + x * Y
        if not isinstance(f, int):
            at = pl.multiple_of(at, Y)
        span[pl.ds(at, Y), :] = tile

    tiles = {key: tile_of(20, key, refs) for key in region(3)}
    for x in range(X):
        store(60, x, tiles[(x, 0, 0)])
    for step in range(EXPAND):
        place = {}
        for at, key in enumerate(tiles):
            chain[at] = tiles[key]
            place[key] = at
        get = lambda key, place=place: chain[place[key]]
        tiles = {key: apply(get, key, coef) for key in region(2 - step)}
        for x in range(X):
            store(61 + step, x, tiles[(x, 0, 0)])

    def body(f, carry):
        held = {}

        def get(key):
            if key not in held:
                held[key] = tile_of(f, key, refs)
            return held[key]

        once = {key: apply(get, key, coef) for key in region(1)}
        for x in range(X):
            store(f, x, get((x, 0, 0)))
            store(f + 20, x, once[(x, 0, 0)])
        for x in range(X):
            store(f + 40, x, apply(once.__getitem__, (x, 0, 0), coef))
        return carry

    lax.fori_loop(0, KEEP, body, 0)

    total = jnp.zeros((SPAN, SPAN), F32)
    for r in range(0, X * Y, 2):
        pair = [span[pl.ds(r + i, SPAN, stride=X * Y), :] for i in range(2)]
        rows = jnp.concatenate(pair, axis=1)
        total = total + lax.dot_general(
            rows,
            rows,
            (((1,), (1,)), ((), ())),
            precision=lax.Precision.HIGHEST,
            preferred_element_type=F32,
        )
    packed = jnp.concatenate([total[:32], total[32:]], axis=1)
    for i in range(copies):
        gram[i] = packed


def sum_kernel(copies, parts, out):
    total = parts[0]
    for i in range(1, parts.shape[0]):
        total = total + parts[i]
    for i in range(copies):
        out[i] = total


def exchange(parts, axis):
    return lax.all_to_all(parts, axis, 0, 0)


def finish_kernel(cell_count, parts, span, basis, hessenberg, spread):
    total = parts[0]
    for i in range(1, parts.shape[0]):
        total = total + parts[i]
    total = total * (1.0 / cell_count)
    lane = lax.broadcasted_iota(jnp.int32, (32, Z), 1)
    gram = jnp.concatenate(
        [jnp.where(lane < SPAN, total, 0.0), jnp.where(lane < SPAN, pltpu.roll(total, 64, 1), 0.0)],
        axis=0,
    )
    row64 = lax.broadcasted_iota(jnp.int32, (SPAN, Z), 0)
    lane64 = lax.broadcasted_iota(jnp.int32, (SPAN, Z), 1)
    eye = row64 == lane64
    row = lax.broadcasted_iota(jnp.int32, (ROWS, Z), 0)
    lane = lax.broadcasted_iota(jnp.int32, (ROWS, Z), 1)
    lane1 = lax.broadcasted_iota(jnp.int32, (1, Z), 1)

    def column(vector):
        return jnp.sum(jnp.where(eye, vector, 0.0), axis=1, keepdims=True)

    first_row = gram[60:61, :]
    norm_sq = jnp.sum(jnp.where(lane1 == 60, first_row, 0.0), axis=1, keepdims=True)
    inverse = 1.0 / jnp.maximum(jnp.sqrt(norm_sq), 0.5)
    last = jnp.where(lane1 == 60, inverse, 0.0)
    last_gram = first_row * inverse
    q = jnp.where((row == lane) & (row < KEEP), 1.0, 0.0)
    q = jnp.where(row == KEEP, last, q)
    qg = jnp.where(row < KEEP, gram[:ROWS, :], 0.0)
    qg = jnp.where(row == KEEP, last_gram, qg)
    spread[3] = jnp.broadcast_to(inverse, TILE)
    for k in range(EXPAND):
        up = jnp.where(
            (lane1 >= KEEP) & (lane1 < 60),
            pltpu.roll(last, KEEP, 1),
            jnp.where((lane1 > 60) & (lane1 < SPAN), pltpu.roll(last, 1, 1), 0.0),
        )
        image = up + SIGMA * last
        image_gram = jnp.sum(column(up) * gram, axis=0, keepdims=True) + SIGMA * last_gram
        c = jnp.sum(q * image_gram, axis=1, keepdims=True)
        partly = image - jnp.sum(c * q, axis=0, keepdims=True)
        partly_gram = image_gram - jnp.sum(c * qg, axis=0, keepdims=True)
        e = jnp.sum(q * partly_gram, axis=1, keepdims=True)
        cleaned = partly - jnp.sum(e * q, axis=0, keepdims=True)
        cleaned_gram = partly_gram - jnp.sum(e * qg, axis=0, keepdims=True)
        length_sq = jnp.sum(cleaned * cleaned_gram, axis=1, keepdims=True)
        length = jnp.sqrt(jnp.maximum(length_sq, 0.0))
        inverse = 1.0 / jnp.maximum(length, 0.5)
        last = cleaned * inverse
        last_gram = cleaned_gram * inverse
        q = jnp.where(row == KEEP + 1 + k, last, q)
        qg = jnp.where(row == KEEP + 1 + k, last_gram, qg)
        column_k = jnp.where(row == KEEP + 1 + k, length, c + e)
        turned = jnp.sum(jnp.where(row == lane, column_k, 0.0), axis=0, keepdims=True)
        hessenberg[k : k + 1, :] = turned[:, :ROWS]
        spread[pl.ds(4 + 8 * k, 8)] = jnp.broadcast_to(column(last), (SPAN, Z)).reshape(8, 8, Z)

    for f in range(KEEP):
        basis[f] = span[f]
    for x in range(X):
        basis[KEEP, x] = span[60, x] * spread[3]
    acc = [[jnp.zeros(TILE, F32) for _ in range(X)] for _ in range(EXPAND)]
    for f in range(SPAN):
        tiles = [span[f, x] for x in range(X)]
        for k in range(EXPAND):
            w = spread[4 + 8 * k + f // 8, f % 8 : f % 8 + 1, :]
            for x in range(X):
                acc[k][x] = acc[k][x] + w * tiles[x]
    for k in range(EXPAND):
        for x in range(X):
            basis[KEEP + 1 + k, x] = acc[k][x]


def send(value, axis, forward):
    count = lax.axis_size(axis)
    up = [(i, i + 1) for i in range(count - 1)]
    return lax.ppermute(value, axis, up if forward else [(j, i) for i, j in up])


def per_device(krylov_basis, schur_vectors, next_vector, diag_shift, velocity):
    axes = (*GX, "gy", "gz")
    cell_count = next_vector.size
    for axis in axes:
        cell_count *= lax.axis_size(axis)
    fields, packed = call(
        rotate_kernel,
        [(FIELDS, X, Y, Z), (5, Y, Z)],
        [krylov_basis, schur_vectors.T, next_vector, diag_shift, velocity],
        smem=(1,),
        limit=4,
    )
    z_lo, z_hi = send(packed, "gz", True), send(packed, "gz", False)
    up, down, halo = call(
        pack_y_kernel, [(31, Y, Z), (31, Y, Z), (5, Y, Z)], [fields, z_lo, z_hi]
    )
    y_lo, y_hi = send(up, "gy", True), send(down, "gy", False)
    up, down = call(pack_x_kernel, [(83, Y, Z), (83, Y, Z)], [fields, halo, y_lo, y_hi])
    x_lo, x_hi = send(up, GX, True), send(down, GX, False)
    stages = (("gx_1", "gy"), ("gz",), ("gx_0",))
    sizes = []
    for stage in stages:
        size = 1
        for axis in stage:
            size *= lax.axis_size(axis)
        sizes.append(size)
    span, parts = call(
        functools.partial(stencil_kernel, sizes[0]),
        [(SPAN * X * Y, Z), (sizes[0], 32, Z)],
        [fields, halo, y_lo, y_hi, x_lo, x_hi],
        scratch=[
            pltpu.VMEM((len(COEF), 7, Y, Z), F32),
            pltpu.VMEM((5, Y, Z), F32),
            pltpu.VMEM((2, Y, Z), F32),
            pltpu.VMEM((len(region(3)), Y, Z), F32),
        ],
        limit=8,
    )
    for i, stage in enumerate(stages):
        parts = exchange(parts, stage)
        if i + 1 < len(stages):
            (parts,) = call(
                functools.partial(sum_kernel, sizes[i + 1]), [(sizes[i + 1], 32, Z)], [parts]
            )
    basis, hessenberg = call(
        functools.partial(finish_kernel, cell_count),
        [(ROWS, X, Y, Z), (EXPAND, ROWS)],
        [parts, span.reshape(SPAN, X, Y, Z)],
        scratch=[pltpu.VMEM((4 + 8 * EXPAND, Y, Z), F32)],
        limit=4,
    )
    return basis, hessenberg.T


def solution(mesh):
    split = Mesh(
        mesh.devices.reshape(-1, 2, mesh.shape["gy"], mesh.shape["gz"]),
        ("gx_0", "gx_1", "gy", "gz"),
    )
    return jax.shard_map(
        per_device,
        mesh=split,
        in_specs=(
            P(None, GX, "gy", "gz"),
            P(),
            P(GX, "gy", "gz"),
            P(GX, "gy", "gz"),
            P(None, GX, "gy", "gz"),
        ),
        out_specs=(P(None, GX, "gy", "gz"), P()),
        check_vma=False,
    )
```

```python
import functools

import jax
import jax.numpy as jnp
from jax import lax
from jax.experimental import pallas as pl
from jax.experimental.pallas import tpu as pltpu
from jax.sharding import Mesh
from jax.sharding import PartitionSpec as P

KEEP = 20
EXPAND = 3
ROWS = 24
FIELDS = 25
SPAN = 64
SIGMA = 7.125
GX = ("gx_0", "gx_1")
X, Y, Z = (4, 8, 128)
TILE = (Y, Z)
F32 = jnp.float32


def rows_of():
    return lax.broadcasted_iota(jnp.int32, TILE, 0)


def lanes_of():
    return lax.broadcasted_iota(jnp.int32, TILE, 1)


def shift_rows(tile, by):
    by = by % Y
    return tile if by == 0 else pltpu.roll(tile, by, 0)


def shift_lanes(tile, by):
    return pltpu.roll(tile, by, 1)


def vmem():
    return pl.BlockSpec(memory_space=pltpu.VMEM)


def call(kernel, outs, args, scratch=(), smem=(), flops=100000, limit=2):
    return pl.pallas_call(
        kernel,
        out_shape=[jax.ShapeDtypeStruct(s, F32) for s in outs],
        in_specs=[
            pl.BlockSpec(memory_space=pltpu.SMEM) if i in smem else vmem() for i in range(len(args))
        ],
        out_specs=[vmem() for _ in outs],
        scratch_shapes=list(scratch),
        cost_estimate=pl.CostEstimate(flops=flops, bytes_accessed=100000, transcendentals=0),
        compiler_params=pltpu.CompilerParams(vmem_limit_bytes=limit * 2**20),
    )(*args)


def rotate_kernel(basis, schur, next_vector, diag, velocity, fields, packed):
    group = 5
    for g in range(KEEP // group):

        def body(i, acc, g=g):
            out = []
            tiles = [basis[i, x] for x in range(X)]
            for f in range(group):
                w = schur[g * group + f, i]
                for x in range(X):
                    out.append(acc[f * X + x] + w * tiles[x])
            return tuple(out)

        zero = tuple(jnp.zeros(TILE, F32) for _ in range(group * X))
        acc = lax.fori_loop(0, basis.shape[0], body, zero, unroll=4)
        for f in range(group):
            for x in range(X):
                fields[g * group + f, x] = acc[f * X + x]
    for x in range(X):
        fields[20, x] = next_vector[x]
        fields[21, x] = 6.0 + diag[x]
        for d in range(3):
            fields[22 + d, x] = 0.5 * velocity[d, x]
    lane = lanes_of()
    for p in range(5):
        total = jnp.zeros(TILE, F32)
        for j in range(20):
            tile = fields[5 * p + j // 4, j % 4]
            moved = shift_lanes(tile, 6 * j + 3)
            total = jnp.where((lane >= 6 * j) & (lane < 6 * j + 6), moved, total)
        packed[p] = total


def pack_y_kernel(fields, from_lo, from_hi, up, down, halo):
    row, lane = rows_of(), lanes_of()
    left = lax.rem(lane, 6) < 3
    for f in range(FIELDS):
        a = jnp.zeros(TILE, F32)
        b = a
        for x in range(X):
            tile = fields[f, x]
            here = (row >= 2 * x) & (row < 2 * x + 2)
            a = jnp.where(here, shift_rows(tile, 2 * x - 6), a)
            b = jnp.where(here, shift_rows(tile, 2 * x), b)
        up[f] = a
        down[f] = b
    a = jnp.zeros(TILE, F32)
    b = a
    for x in range(X):
        tile = fields[20, x]
        a = jnp.where(row == x, shift_rows(tile, x - 5), a)
        b = jnp.where(row == x, shift_rows(tile, x - 2), b)
    up[25] = a
    down[25] = b
    for p in range(5):
        merged = jnp.where(left, from_lo[p], from_hi[p])
        halo[p] = merged
        up[26 + p] = merged
        down[26 + p] = merged


def pack_x_kernel(fields, halo, y_lo, y_hi, up, down):
    first = rows_of() < 4
    for f in range(FIELDS):
        up[2 * f] = fields[f, 2]
        up[2 * f + 1] = fields[f, 3]
        down[2 * f] = fields[f, 0]
        down[2 * f + 1] = fields[f, 1]
    up[50] = fields[20, 1]
    down[50] = fields[20, 2]
    lo, hi = y_lo[20], y_hi[20]
    up[51] = jnp.where(first, shift_rows(lo, 4), hi)
    down[51] = jnp.where(first, lo, shift_rows(hi, 4))
    row = rows_of()
    for v in range(6):
        a = jnp.zeros(TILE, F32)
        b = a
        for k in range(4):
            f = 4 * v + k + (1 if v == 5 else 0)
            lo, hi = y_lo[f], y_hi[f]
            a = jnp.where(row == 2 * k, shift_rows(lo, 2 * k - 7), a)
            a = jnp.where(row == 2 * k + 1, shift_rows(hi, 2 * k - 5), a)
            b = jnp.where(row == 2 * k, shift_rows(lo, 2 * k - 1), b)
            b = jnp.where(row == 2 * k + 1, shift_rows(hi, 2 * k + 1), b)
        up[52 + v] = a
        down[52 + v] = b
    for out in (up, down):
        for p in range(5):
            out[58 + p] = halo[p]
        out[63] = y_lo[30]
        out[64] = y_hi[30]


def region(radius):
    out = []
    for a, b in ((0, 0), (1, 0), (0, 1), (1, 1)):
        for x in range(-radius + a + b, X + radius - a - b):
            out.append((x, a, b))
    return out


COEF = region(2)


def tile_of(f, key, refs):
    fields, halo, y_lo, y_hi, x_lo, x_hi, y_halo, x_corner = refs
    x, a, b = key
    first = rows_of() < 4
    if b == 0:
        if a == 0:
            if 0 <= x < X:
                return fields[f, x]
            if x == -3:
                return x_lo[50]
            if x == 6:
                return x_hi[50]
            return x_lo[2 * f + x + 2] if x < 0 else x_hi[2 * f + x - 4]
        if 0 <= x < X:
            lo, hi = y_lo[f], y_hi[f]
            tile = jnp.where(first, shift_rows(hi, -2 * x), shift_rows(lo, 6 - 2 * x))
            if isinstance(f, int) and f == 20:
                row = rows_of()
                tile = jnp.where(row == 2, shift_rows(y_hi[25], 2 - x), tile)
                tile = jnp.where(row == 5, shift_rows(y_lo[25], 5 - x), tile)
            return tile
        side = x_lo if x < 0 else x_hi
        if not (isinstance(f, int) and f == 20):
            g = f - 1 if isinstance(f, int) and f > 20 else f
            v, k = (g // 4, g % 4) if isinstance(g, int) else (lax.div(g, 4), lax.rem(g, 4))
            return pltpu.roll(side[52 + v], 7 - 2 * k, 0)
        packed = side[51]
        if x in (-1, 5):
            return jnp.where(first, shift_rows(packed, 2), shift_rows(packed, 4))
        return jnp.where(first, shift_rows(packed, 4), shift_rows(packed, 6))
    p, q = (f // 5, f % 5) if isinstance(f, int) else (lax.div(f, 5), lax.rem(f, 5))
    place = x if 0 <= x < X else (x + X if x < 0 else x - X)
    by = 128 - 3 - 6 * (4 * q + place)
    if a == 0:
        packed = halo[p] if 0 <= x < X else (x_lo if x < 0 else x_hi)[58 + p]
    elif 0 <= x < X:
        packed = y_halo[p]
    else:
        packed = x_corner[0 if x < 0 else 1]
    return shift_lanes(packed, by)


def apply(get, key, coef):
    x, a, b = key
    row, lane = rows_of(), lanes_of()
    base = COEF.index(key)
    centre = get((x, a, b))
    y_other = get((x, 1 - a, b))
    z_other = get((x, a, 1 - b))
    y_ahead = shift_rows(jnp.where(row == 0, y_other, centre), 7)
    y_behind = shift_rows(jnp.where(row == 7, y_other, centre), 1)
    z_ahead = shift_lanes(jnp.where(lane == 0, z_other, centre), 127)
    z_behind = shift_lanes(jnp.where(lane == 127, z_other, centre), 1)
    near = (
        centre,
        get((x + 1, a, b)),
        get((x - 1, a, b)),
        y_ahead,
        y_behind,
        z_ahead,
        z_behind,
    )
    terms = [coef[base, i] * near[i] for i in range(7)]
    return (terms[0] + (terms[1] + terms[2])) + ((terms[3] + terms[4]) + (terms[5] + terms[6]))


def stencil_kernel(
    copies, fields, halo, y_lo, y_hi, x_lo, x_hi, span, gram, coef, y_halo, x_corner, chain
):
    refs = (fields, halo, y_lo, y_hi, x_lo, x_hi, y_halo, x_corner)
    first = rows_of() < 4
    for p in range(5):
        y_halo[p] = jnp.where(first, y_hi[26 + p], y_lo[26 + p])
    x_corner[0] = jnp.where(first, x_lo[64], x_lo[63])
    x_corner[1] = jnp.where(first, x_hi[64], x_hi[63])
    for at, key in enumerate(COEF):
        diagonal = tile_of(21, key, refs)
        inside = diagonal != 0.0
        coef[at, 0] = jnp.where(inside, diagonal - SIGMA, 0.0)
        for d in range(3):
            half = tile_of(22 + d, key, refs)
            coef[at, 1 + 2 * d] = jnp.where(inside, half - 1.0, 0.0)
            coef[at, 2 + 2 * d] = jnp.where(inside, -1.0 - half, 0.0)

    def store(f, x, tile):
        at = f * (X * Y) + x * Y
        if not isinstance(f, int):
            at = pl.multiple_of(at, Y)
        span[pl.ds(at, Y), :] = tile

    tiles = {key: tile_of(20, key, refs) for key in region(3)}
    for x in range(X):
        store(60, x, tiles[(x, 0, 0)])
    for step in range(EXPAND):
        place = {}
        for at, key in enumerate(tiles):
            chain[at] = tiles[key]
            place[key] = at
        get = lambda key, place=place: chain[place[key]]
        tiles = {key: apply(get, key, coef) for key in region(2 - step)}
        for x in range(X):
            store(61 + step, x, tiles[(x, 0, 0)])

    def body(f, carry):
        held = {}

        def get(key):
            if key not in held:
                held[key] = tile_of(f, key, refs)
            return held[key]

        once = {key: apply(get, key, coef) for key in region(1)}
        for x in range(X):
            store(f, x, get((x, 0, 0)))
            store(f + 20, x, once[(x, 0, 0)])
        for x in range(X):
            store(f + 40, x, apply(once.__getitem__, (x, 0, 0), coef))
        return carry

    lax.fori_loop(0, KEEP, body, 0, unroll=4)

    total = jnp.zeros((SPAN, SPAN), F32)
    for r in range(0, X * Y, 2):
        pair = [span[pl.ds(r + i, SPAN, stride=X * Y), :] for i in range(2)]
        rows = jnp.concatenate(pair, axis=1)
        total = total + lax.dot_general(
            rows,
            rows,
            (((1,), (1,)), ((), ())),
            precision=lax.Precision.HIGHEST,
            preferred_element_type=F32,
        )
    packed = jnp.concatenate([total[:32], total[32:]], axis=1)
    for i in range(copies):
        gram[i] = packed[:16] if i < copies // 2 else packed[16:]


def sum_kernel(copies, parts, out):
    total = parts[0]
    for i in range(1, parts.shape[0]):
        total = total + parts[i]
    for i in range(copies):
        out[i] = total


def exchange(parts, axis):
    return lax.all_to_all(parts, axis, 0, 0)


def finish_kernel(cell_count, parts, span, basis, hessenberg, spread):
    total = jnp.concatenate([parts[0], parts[1]], axis=0) * (1.0 / cell_count)
    lane = lax.broadcasted_iota(jnp.int32, (32, Z), 1)
    gram = jnp.concatenate(
        [jnp.where(lane < SPAN, total, 0.0), jnp.where(lane < SPAN, pltpu.roll(total, 64, 1), 0.0)],
        axis=0,
    )
    row64 = lax.broadcasted_iota(jnp.int32, (SPAN, Z), 0)
    lane64 = lax.broadcasted_iota(jnp.int32, (SPAN, Z), 1)
    eye = row64 == lane64
    row = lax.broadcasted_iota(jnp.int32, (ROWS, Z), 0)
    lane = lax.broadcasted_iota(jnp.int32, (ROWS, Z), 1)
    lane1 = lax.broadcasted_iota(jnp.int32, (1, Z), 1)

    def column(vector):
        return jnp.sum(jnp.where(eye, vector, 0.0), axis=1, keepdims=True)

    first_row = gram[60:61, :]
    norm_sq = jnp.sum(jnp.where(lane1 == 60, first_row, 0.0), axis=1, keepdims=True)
    inverse = 1.0 / jnp.maximum(jnp.sqrt(norm_sq), 0.5)
    last = jnp.where(lane1 == 60, inverse, 0.0)
    last_gram = first_row * inverse
    q = jnp.where((row == lane) & (row < KEEP), 1.0, 0.0)
    q = jnp.where(row == KEEP, last, q)
    qg = jnp.where(row < KEEP, gram[:ROWS, :], 0.0)
    qg = jnp.where(row == KEEP, last_gram, qg)
    spread[3] = jnp.broadcast_to(inverse, TILE)
    for k in range(EXPAND):
        up = jnp.where(
            (lane1 >= KEEP) & (lane1 < 60),
            pltpu.roll(last, KEEP, 1),
            jnp.where((lane1 > 60) & (lane1 < SPAN), pltpu.roll(last, 1, 1), 0.0),
        )
        image = up + SIGMA * last
        image_gram = jnp.sum(column(up) * gram, axis=0, keepdims=True) + SIGMA * last_gram
        c = jnp.sum(q * image_gram, axis=1, keepdims=True)
        partly = image - jnp.sum(c * q, axis=0, keepdims=True)
        partly_gram = image_gram - jnp.sum(c * qg, axis=0, keepdims=True)
        e = jnp.sum(q * partly_gram, axis=1, keepdims=True)
        cleaned = partly - jnp.sum(e * q, axis=0, keepdims=True)
        cleaned_gram = partly_gram - jnp.sum(e * qg, axis=0, keepdims=True)
        length_sq = jnp.sum(cleaned * cleaned_gram, axis=1, keepdims=True)
        length = jnp.sqrt(jnp.maximum(length_sq, 0.0))
        inverse = 1.0 / jnp.maximum(length, 0.5)
        last = cleaned * inverse
        last_gram = cleaned_gram * inverse
        q = jnp.where(row == KEEP + 1 + k, last, q)
        qg = jnp.where(row == KEEP + 1 + k, last_gram, qg)
        column_k = jnp.where(row == KEEP + 1 + k, length, c + e)
        turned = jnp.sum(jnp.where(row == lane, column_k, 0.0), axis=0, keepdims=True)
        hessenberg[k : k + 1, :] = turned[:, :ROWS]
        spread[pl.ds(4 + 8 * k, 8)] = jnp.broadcast_to(column(last), (SPAN, Z)).reshape(8, 8, Z)

    for f in range(KEEP):
        basis[f] = span[f]
    for x in range(X):
        basis[KEEP, x] = span[60, x] * spread[3]
    acc = [[jnp.zeros(TILE, F32) for _ in range(X)] for _ in range(EXPAND)]
    for f in range(SPAN):
        tiles = [span[f, x] for x in range(X)]
        for k in range(EXPAND):
            w = spread[4 + 8 * k + f // 8, f % 8 : f % 8 + 1, :]
            for x in range(X):
                acc[k][x] = acc[k][x] + w * tiles[x]
    for k in range(EXPAND):
        for x in range(X):
            basis[KEEP + 1 + k, x] = acc[k][x]


def send(value, axis, forward):
    count = lax.axis_size(axis)
    up = [(i, i + 1) for i in range(count - 1)]
    return lax.ppermute(value, axis, up if forward else [(j, i) for i, j in up])


def per_device(krylov_basis, schur_vectors, next_vector, diag_shift, velocity):
    axes = (*GX, "gy", "gz")
    cell_count = next_vector.size
    for axis in axes:
        cell_count *= lax.axis_size(axis)
    fields, packed = call(
        rotate_kernel,
        [(FIELDS, X, Y, Z), (5, Y, Z)],
        [krylov_basis, schur_vectors.T, next_vector, diag_shift, velocity],
        smem=(1,),
        limit=4,
    )
    z_lo, z_hi = send(packed, "gz", True), send(packed, "gz", False)
    up, down, halo = call(
        pack_y_kernel, [(31, Y, Z), (31, Y, Z), (5, Y, Z)], [fields, z_lo, z_hi]
    )
    y_lo, y_hi = send(up, "gy", True), send(down, "gy", False)
    up, down = call(pack_x_kernel, [(65, Y, Z), (65, Y, Z)], [fields, halo, y_lo, y_hi])
    x_lo, x_hi = send(up, GX, True), send(down, GX, False)
    stages = (("gx_1", "gz"), ("gx_0", "gy"))
    sizes = [lax.axis_size(stage) for stage in stages]
    span, parts = call(
        functools.partial(stencil_kernel, sizes[0]),
        [(SPAN * X * Y, Z), (sizes[0], 16, Z)],
        [fields, halo, y_lo, y_hi, x_lo, x_hi],
        scratch=[
            pltpu.VMEM((len(COEF), 7, Y, Z), F32),
            pltpu.VMEM((5, Y, Z), F32),
            pltpu.VMEM((2, Y, Z), F32),
            pltpu.VMEM((len(region(3)), Y, Z), F32),
        ],
        limit=8,
    )
    parts = exchange(parts, stages[0])
    (parts,) = call(functools.partial(sum_kernel, sizes[1]), [(sizes[1], 16, Z)], [parts])
    parts = exchange(parts, stages[1])
    (half,) = call(functools.partial(sum_kernel, 1), [(1, 16, Z)], [parts])
    whole = lax.all_gather(half, "gx_1", axis=0, tiled=True)
    basis, hessenberg = call(
        functools.partial(finish_kernel, cell_count),
        [(ROWS, X, Y, Z), (EXPAND, ROWS)],
        [whole, span.reshape(SPAN, X, Y, Z)],
        scratch=[pltpu.VMEM((4 + 8 * EXPAND, Y, Z), F32)],
        limit=4,
    )
    return basis, hessenberg.T


def solution(mesh):
    split = Mesh(
        mesh.devices.reshape(-1, 2, mesh.shape["gy"], mesh.shape["gz"]),
        ("gx_0", "gx_1", "gy", "gz"),
    )
    return jax.shard_map(
        per_device,
        mesh=split,
        in_specs=(
            P(None, GX, "gy", "gz"),
            P(),
            P(GX, "gy", "gz"),
            P(GX, "gy", "gz"),
            P(None, GX, "gy", "gz"),
        ),
        out_specs=(P(None, GX, "gy", "gz"), P()),
        check_vma=False,
    )
```

```python
import functools

import jax
import jax.numpy as jnp
from jax import lax
from jax.experimental import pallas as pl
from jax.experimental.pallas import tpu as pltpu
from jax.sharding import Mesh
from jax.sharding import PartitionSpec as P

KEEP = 20
EXPAND = 3
ROWS = 24
FIELDS = 25
SPAN = 64
SIGMA = 7.125
GX = ("gx_0", "gx_1")
X, Y, Z = (4, 8, 128)
TILE = (Y, Z)
F32 = jnp.float32


def rows_of():
    return lax.broadcasted_iota(jnp.int32, TILE, 0)


def lanes_of():
    return lax.broadcasted_iota(jnp.int32, TILE, 1)


def shift_rows(tile, by):
    by = by % Y
    return tile if by == 0 else pltpu.roll(tile, by, 0)


def shift_lanes(tile, by):
    return pltpu.roll(tile, by, 1)


def place_of(kind):
    return pl.BlockSpec(memory_space={"v": pltpu.VMEM, "s": pltpu.SMEM, "h": pltpu.HBM}[kind])


def call(kernel, outs, args, scratch=(), ins="", out="", flops=100000, limit=2):
    ins, out = ins or "v" * len(args), out or "v" * len(outs)
    return pl.pallas_call(
        kernel,
        out_shape=[jax.ShapeDtypeStruct(s, F32) for s in outs],
        in_specs=[place_of(k) for k in ins],
        out_specs=[place_of(k) for k in out],
        scratch_shapes=list(scratch),
        cost_estimate=pl.CostEstimate(flops=flops, bytes_accessed=100000, transcendentals=0),
        compiler_params=pltpu.CompilerParams(vmem_limit_bytes=limit * 2**20),
    )(*args)


CHUNK = 10


def edge_kernel(
    basis, schur, next_vector, diag, velocity, held, rest, packed, weights, small, sems
):
    chunks = basis.shape[0] // CHUNK
    copies = [
        pltpu.make_async_copy(schur, weights, sems.at[0]),
        *(
            pltpu.make_async_copy(
                basis.at[pl.ds(c * CHUNK, CHUNK)], held.at[pl.ds(c * CHUNK, CHUNK)], sems.at[1 + c]
            )
            for c in range(chunks)
        ),
        pltpu.make_async_copy(next_vector, rest.at[0], sems.at[1 + chunks]),
        pltpu.make_async_copy(diag, small.at[0], sems.at[2 + chunks]),
        pltpu.make_async_copy(velocity, small.at[pl.ds(1, 3)], sems.at[3 + chunks]),
    ]
    for copy in copies:
        copy.start()
    lane = lanes_of()
    copies[0].wait()
    acc = [jnp.zeros(TILE, F32) for _ in range(KEEP)]
    for c in range(chunks):
        copies[1 + c].wait()
        for i in range(c * CHUNK, (c + 1) * CHUNK):
            edge = jnp.zeros(TILE, F32)
            for x in range(X):
                here = (lane >= 6 * x) & (lane < 6 * x + 6)
                edge = jnp.where(here, shift_lanes(held[i, x], 6 * x + 3), edge)
            for f in range(KEEP):
                acc[f] = acc[f] + weights[f, i] * edge
    for p in range(4):
        total = acc[5 * p]
        for q in range(1, 5):
            total = jnp.where(lane < 24 * q, total, shift_lanes(acc[5 * p + q], 24 * q))
        packed[p] = total
    for copy in copies[1 + chunks :]:
        copy.wait()
    for x in range(X):
        rest[1, x] = 6.0 + small[0, x]
        for d in range(3):
            rest[2 + d, x] = 0.5 * small[1 + d, x]
    total = jnp.zeros(TILE, F32)
    for j in range(20):
        moved = shift_lanes(rest[j // 4, j % 4], 6 * j + 3)
        total = jnp.where((lane >= 6 * j) & (lane < 6 * j + 6), moved, total)
    packed[4] = total


def rotate_kernel(basis, schur, rotated):
    group = 5
    for g in range(KEEP // group):

        def body(i, acc, g=g):
            out = []
            tiles = [basis[i, x] for x in range(X)]
            for f in range(group):
                w = schur[g * group + f, i]
                for x in range(X):
                    out.append(acc[f * X + x] + w * tiles[x])
            return tuple(out)

        zero = tuple(jnp.zeros(TILE, F32) for _ in range(group * X))
        acc = lax.fori_loop(0, basis.shape[0], body, zero, unroll=4)
        for f in range(group):
            for x in range(X):
                rotated[g * group + f, x] = acc[f * X + x]


class Fields:
    def __init__(self, rotated, rest):
        self.rotated, self.rest = rotated, rest

    def __getitem__(self, at):
        f, x = at
        if isinstance(f, int) and f >= KEEP:
            return self.rest[f - KEEP, x]
        return self.rotated[f, x]


def pack_y_kernel(rotated, rest, from_lo, from_hi, up, down, halo):
    fields = Fields(rotated, rest)
    row, lane = rows_of(), lanes_of()
    left = lax.rem(lane, 6) < 3
    for f in range(FIELDS):
        a = jnp.zeros(TILE, F32)
        b = a
        for x in range(X):
            tile = fields[f, x]
            here = (row >= 2 * x) & (row < 2 * x + 2)
            a = jnp.where(here, shift_rows(tile, 2 * x - 6), a)
            b = jnp.where(here, shift_rows(tile, 2 * x), b)
        up[f] = a
        down[f] = b
    a = jnp.zeros(TILE, F32)
    b = a
    for x in range(X):
        tile = fields[20, x]
        a = jnp.where(row == x, shift_rows(tile, x - 5), a)
        b = jnp.where(row == x, shift_rows(tile, x - 2), b)
    up[25] = a
    down[25] = b
    for p in range(5):
        merged = jnp.where(left, from_lo[p], from_hi[p])
        halo[p] = merged
        up[26 + p] = merged
        down[26 + p] = merged


def pack_x_kernel(rotated, rest, halo, y_lo, y_hi, off, on):
    fields = Fields(rotated, rest)
    first, row = rows_of() < 4, rows_of()
    upper = lax.axis_index("gx_1") == 1

    def put(at, up, down):
        off[at] = jnp.where(upper, up, down)
        on[at] = jnp.where(upper, down, up)

    for f in range(FIELDS):
        put(2 * f, fields[f, 2], fields[f, 0])
        put(2 * f + 1, fields[f, 3], fields[f, 1])
    put(50, fields[20, 1], fields[20, 2])
    lo, hi = y_lo[20], y_hi[20]
    put(51, jnp.where(first, shift_rows(lo, 4), hi), jnp.where(first, lo, shift_rows(hi, 4)))
    for v in range(6):
        a = jnp.zeros(TILE, F32)
        b = a
        for k in range(4):
            f = 4 * v + k + (1 if v == 5 else 0)
            lo, hi = y_lo[f], y_hi[f]
            a = jnp.where(row == 2 * k, shift_rows(lo, 2 * k - 7), a)
            a = jnp.where(row == 2 * k + 1, shift_rows(hi, 2 * k - 5), a)
            b = jnp.where(row == 2 * k, shift_rows(lo, 2 * k - 1), b)
            b = jnp.where(row == 2 * k + 1, shift_rows(hi, 2 * k + 1), b)
        put(52 + v, a, b)
    for out in (off, on):
        for p in range(5):
            out[58 + p] = halo[p]
        out[63] = y_lo[30]
        out[64] = y_hi[30]


def region(radius):
    out = []
    for a, b in ((0, 0), (1, 0), (0, 1), (1, 1)):
        for x in range(-radius + a + b, X + radius - a - b):
            out.append((x, a, b))
    return out


COEF = region(2)


def tile_of(f, key, refs):
    fields, halo, y_lo, y_hi, x_lo, x_hi, y_halo, x_corner = refs
    x, a, b = key
    first = rows_of() < 4
    if b == 0:
        if a == 0:
            if 0 <= x < X:
                return fields[f, x]
            if x == -3:
                return x_lo[50]
            if x == 6:
                return x_hi[50]
            return x_lo[2 * f + x + 2] if x < 0 else x_hi[2 * f + x - 4]
        if 0 <= x < X:
            lo, hi = y_lo[f], y_hi[f]
            tile = jnp.where(first, shift_rows(hi, -2 * x), shift_rows(lo, 6 - 2 * x))
            if isinstance(f, int) and f == 20:
                row = rows_of()
                tile = jnp.where(row == 2, shift_rows(y_hi[25], 2 - x), tile)
                tile = jnp.where(row == 5, shift_rows(y_lo[25], 5 - x), tile)
            return tile
        side = x_lo if x < 0 else x_hi
        if not (isinstance(f, int) and f == 20):
            g = f - 1 if isinstance(f, int) and f > 20 else f
            v, k = (g // 4, g % 4) if isinstance(g, int) else (lax.div(g, 4), lax.rem(g, 4))
            return pltpu.roll(side[52 + v], 7 - 2 * k, 0)
        packed = side[51]
        if x in (-1, 5):
            return jnp.where(first, shift_rows(packed, 2), shift_rows(packed, 4))
        return jnp.where(first, shift_rows(packed, 4), shift_rows(packed, 6))
    p, q = (f // 5, f % 5) if isinstance(f, int) else (lax.div(f, 5), lax.rem(f, 5))
    place = x if 0 <= x < X else (x + X if x < 0 else x - X)
    by = 128 - 3 - 6 * (4 * q + place)
    if a == 0:
        packed = halo[p] if 0 <= x < X else (x_lo if x < 0 else x_hi)[58 + p]
    elif 0 <= x < X:
        packed = y_halo[p]
    else:
        packed = x_corner[0 if x < 0 else 1]
    return shift_lanes(packed, by)


def apply(get, key, coef):
    x, a, b = key
    row, lane = rows_of(), lanes_of()
    base = COEF.index(key)
    centre = get((x, a, b))
    y_other = get((x, 1 - a, b))
    z_other = get((x, a, 1 - b))
    y_ahead = shift_rows(jnp.where(row == 0, y_other, centre), 7)
    y_behind = shift_rows(jnp.where(row == 7, y_other, centre), 1)
    z_ahead = shift_lanes(jnp.where(lane == 0, z_other, centre), 127)
    z_behind = shift_lanes(jnp.where(lane == 127, z_other, centre), 1)
    near = (
        centre,
        get((x + 1, a, b)),
        get((x - 1, a, b)),
        y_ahead,
        y_behind,
        z_ahead,
        z_behind,
    )
    terms = [coef[base, i] * near[i] for i in range(7)]
    return (terms[0] + (terms[1] + terms[2])) + ((terms[3] + terms[4]) + (terms[5] + terms[6]))


def stencil_kernel(
    copies,
    rotated,
    rest,
    halo,
    y_lo,
    y_hi,
    off,
    on,
    span,
    gram,
    coef,
    y_halo,
    x_corner,
    chain,
    x_lo,
    x_hi,
):
    fields = Fields(rotated, rest)
    upper = lax.axis_index("gx_1") == 1
    for i in range(off.shape[0]):
        x_lo[i] = jnp.where(upper, on[i], off[i])
        x_hi[i] = jnp.where(upper, off[i], on[i])
    refs = (fields, halo, y_lo, y_hi, x_lo, x_hi, y_halo, x_corner)
    first = rows_of() < 4
    for p in range(5):
        y_halo[p] = jnp.where(first, y_hi[26 + p], y_lo[26 + p])
    x_corner[0] = jnp.where(first, x_lo[64], x_lo[63])
    x_corner[1] = jnp.where(first, x_hi[64], x_hi[63])
    for at, key in enumerate(COEF):
        diagonal = tile_of(21, key, refs)
        inside = diagonal != 0.0
        coef[at, 0] = jnp.where(inside, diagonal - SIGMA, 0.0)
        for d in range(3):
            half = tile_of(22 + d, key, refs)
            coef[at, 1 + 2 * d] = jnp.where(inside, half - 1.0, 0.0)
            coef[at, 2 + 2 * d] = jnp.where(inside, -1.0 - half, 0.0)

    def store(f, x, tile):
        at = f * (X * Y) + x * Y
        if not isinstance(f, int):
            at = pl.multiple_of(at, Y)
        span[pl.ds(at, Y), :] = tile

    tiles = {key: tile_of(20, key, refs) for key in region(3)}
    for x in range(X):
        store(60, x, tiles[(x, 0, 0)])
    for step in range(EXPAND):
        place = {}
        for at, key in enumerate(tiles):
            chain[at] = tiles[key]
            place[key] = at
        get = lambda key, place=place: chain[place[key]]
        tiles = {key: apply(get, key, coef) for key in region(2 - step)}
        for x in range(X):
            store(61 + step, x, tiles[(x, 0, 0)])

    def body(f, carry):
        held = {}

        def get(key):
            if key not in held:
                held[key] = tile_of(f, key, refs)
            return held[key]

        once = {key: apply(get, key, coef) for key in region(1)}
        for x in range(X):
            store(f, x, get((x, 0, 0)))
            store(f + 20, x, once[(x, 0, 0)])
        for x in range(X):
            store(f + 40, x, apply(once.__getitem__, (x, 0, 0), coef))
        return carry

    lax.fori_loop(0, KEEP, body, 0, unroll=4)

    total = jnp.zeros((SPAN, SPAN), F32)
    for r in range(0, X * Y, 2):
        pair = [span[pl.ds(r + i, SPAN, stride=X * Y), :] for i in range(2)]
        rows = jnp.concatenate(pair, axis=1)
        total = total + lax.dot_general(
            rows,
            rows,
            (((1,), (1,)), ((), ())),
            precision=lax.Precision.HIGHEST,
            preferred_element_type=F32,
        )
    packed = jnp.concatenate([total[:32], total[32:]], axis=1)
    for i in range(copies):
        gram[i] = packed[:16] if i < copies // 2 else packed[16:]


def sum_kernel(copies, parts, out):
    total = parts[0]
    for i in range(1, parts.shape[0]):
        total = total + parts[i]
    for i in range(copies):
        out[i] = total


def exchange(parts, axis):
    return lax.all_to_all(parts, axis, 0, 0)


def finish_kernel(cell_count, parts, span, basis, hessenberg, spread, fresh, sems):
    early = pltpu.make_async_copy(
        span.at[pl.ds(0, KEEP)], basis.at[pl.ds(0, KEEP)], sems.at[0]
    )
    early.start()
    total = jnp.concatenate([parts[0], parts[1]], axis=0) * (1.0 / cell_count)
    lane = lax.broadcasted_iota(jnp.int32, (32, Z), 1)
    gram = jnp.concatenate(
        [jnp.where(lane < SPAN, total, 0.0), jnp.where(lane < SPAN, pltpu.roll(total, 64, 1), 0.0)],
        axis=0,
    )
    row64 = lax.broadcasted_iota(jnp.int32, (SPAN, Z), 0)
    lane64 = lax.broadcasted_iota(jnp.int32, (SPAN, Z), 1)
    eye = row64 == lane64
    moved = ((row64 >= KEEP) & (row64 < 60) & (lane64 == row64 - KEEP)) | (
        (row64 > 60) & (lane64 == row64 - 1)
    )
    row = lax.broadcasted_iota(jnp.int32, (ROWS, Z), 0)
    lane = lax.broadcasted_iota(jnp.int32, (ROWS, Z), 1)
    lane1 = lax.broadcasted_iota(jnp.int32, (1, Z), 1)

    def column(vector, picks):
        return jnp.sum(jnp.where(picks, vector, 0.0), axis=1, keepdims=True)

    first_row = gram[60:61, :]
    norm_sq = jnp.sum(jnp.where(lane1 == 60, first_row, 0.0), axis=1, keepdims=True)
    inverse = lax.rsqrt(jnp.maximum(norm_sq, 0.25))
    last = jnp.where(lane1 == 60, inverse, 0.0)
    last_gram = first_row * inverse
    up_column = jnp.where(lax.broadcasted_iota(jnp.int32, (SPAN, 1), 0) == 61, inverse, 0.0)
    q = jnp.where((row == lane) & (row < KEEP), 1.0, 0.0)
    q = jnp.where(row == KEEP, last, q)
    qg = jnp.where(row < KEEP, gram[:ROWS, :], 0.0)
    qg = jnp.where(row == KEEP, last_gram, qg)
    spread[3] = jnp.broadcast_to(inverse, TILE)
    for k in range(EXPAND):
        up = jnp.where(
            (lane1 >= KEEP) & (lane1 < 60),
            pltpu.roll(last, KEEP, 1),
            jnp.where((lane1 > 60) & (lane1 < SPAN), pltpu.roll(last, 1, 1), 0.0),
        )
        image = up + SIGMA * last
        image_gram = jnp.sum(up_column * gram, axis=0, keepdims=True) + SIGMA * last_gram
        c = jnp.sum(q * image_gram, axis=1, keepdims=True)
        partly = image - jnp.sum(c * q, axis=0, keepdims=True)
        partly_gram = image_gram - jnp.sum(c * qg, axis=0, keepdims=True)
        e = jnp.sum(q * partly_gram, axis=1, keepdims=True)
        cleaned = partly - jnp.sum(e * q, axis=0, keepdims=True)
        cleaned_gram = partly_gram - jnp.sum(e * qg, axis=0, keepdims=True)
        length_sq = jnp.sum(cleaned * cleaned_gram, axis=1, keepdims=True)
        here, shifted = column(cleaned, eye), column(cleaned, moved)
        inverse = lax.rsqrt(jnp.maximum(length_sq, 0.25))
        last = cleaned * inverse
        last_gram = cleaned_gram * inverse
        up_column = shifted * inverse
        q = jnp.where(row == KEEP + 1 + k, last, q)
        qg = jnp.where(row == KEEP + 1 + k, last_gram, qg)
        length = jnp.sqrt(jnp.maximum(length_sq, 0.0))
        entries = jnp.where(row == KEEP + 1 + k, length, c + e)
        turned = jnp.sum(jnp.where(row == lane, entries, 0.0), axis=0, keepdims=True)
        hessenberg[k : k + 1, :] = turned[:, :ROWS]
        spread[pl.ds(4 + 8 * k, 8)] = jnp.broadcast_to(here * inverse, (SPAN, Z)).reshape(8, 8, Z)

    for x in range(X):
        fresh[0, x] = span[60, x] * spread[3]
    acc = [[jnp.zeros(TILE, F32) for _ in range(X)] for _ in range(EXPAND)]
    for f in range(SPAN):
        tiles = [span[f, x] for x in range(X)]
        for k in range(EXPAND):
            w = spread[4 + 8 * k + f // 8, f % 8 : f % 8 + 1, :]
            for x in range(X):
                acc[k][x] = acc[k][x] + w * tiles[x]
    for k in range(EXPAND):
        for x in range(X):
            fresh[1 + k, x] = acc[k][x]
    late = pltpu.make_async_copy(fresh, basis.at[pl.ds(KEEP, ROWS - KEEP)], sems.at[1])
    late.start()
    early.wait()
    late.wait()


def send(value, axis, forward):
    count = lax.axis_size(axis)
    up = [(i, i + 1) for i in range(count - 1)]
    return lax.ppermute(value, axis, up if forward else [(j, i) for i, j in up])


def per_device(krylov_basis, schur_vectors, next_vector, diag_shift, velocity):
    axes = (*GX, "gy", "gz")
    cell_count = next_vector.size
    for axis in axes:
        cell_count *= lax.axis_size(axis)
    held, rest, packed = call(
        edge_kernel,
        [krylov_basis.shape, (FIELDS - KEEP, X, Y, Z), (5, Y, Z)],
        [
            pltpu.with_memory_space_constraint(value, pltpu.HBM)
            for value in (krylov_basis, schur_vectors.T, next_vector, diag_shift, velocity)
        ],
        scratch=[
            pltpu.SMEM((KEEP, krylov_basis.shape[0]), F32),
            pltpu.VMEM((4, X, Y, Z), F32),
            pltpu.SemaphoreType.DMA((4 + krylov_basis.shape[0] // CHUNK,)),
        ],
        ins="hhhhh",
        limit=4,
    )
    z_lo, z_hi = send(packed, "gz", True), send(packed, "gz", False)
    (rotated,) = call(
        rotate_kernel,
        [(KEEP, X, Y, Z)],
        [held, schur_vectors.T],
        ins="vs",
        limit=4,
        flops=10**9,
    )
    up, down, halo = call(
        pack_y_kernel, [(31, Y, Z), (31, Y, Z), (5, Y, Z)], [rotated, rest, z_lo, z_hi]
    )
    y_lo, y_hi = send(up, "gy", True), send(down, "gy", False)
    off, on = call(
        pack_x_kernel, [(65, Y, Z), (65, Y, Z)], [rotated, rest, halo, y_lo, y_hi]
    )
    count = lax.axis_size(GX)
    swap = [(i, i + 1) for i in range(1, count - 1, 2)]
    off = lax.ppermute(off, GX, swap + [(j, i) for i, j in swap])
    on = lax.ppermute(on, "gx_1", [(0, 1), (1, 0)])
    stages = (("gx_1", "gz"), ("gx_0", "gy"))
    sizes = [lax.axis_size(stage) for stage in stages]
    span, parts = call(
        functools.partial(stencil_kernel, sizes[0]),
        [(SPAN * X * Y, Z), (sizes[0], 16, Z)],
        [rotated, rest, halo, y_lo, y_hi, off, on],
        scratch=[
            pltpu.VMEM((len(COEF), 7, Y, Z), F32),
            pltpu.VMEM((5, Y, Z), F32),
            pltpu.VMEM((2, Y, Z), F32),
            pltpu.VMEM((len(region(3)), Y, Z), F32),
            pltpu.VMEM((65, Y, Z), F32),
            pltpu.VMEM((65, Y, Z), F32),
        ],
        limit=8,
    )
    parts = exchange(parts, stages[0])
    (parts,) = call(functools.partial(sum_kernel, sizes[1]), [(sizes[1], 16, Z)], [parts])
    parts = exchange(parts, stages[1])
    (half,) = call(functools.partial(sum_kernel, 1), [(1, 16, Z)], [parts])
    whole = lax.all_gather(half, "gx_1", axis=0, tiled=True)
    basis, hessenberg = call(
        functools.partial(finish_kernel, cell_count),
        [(ROWS, X, Y, Z), (EXPAND, ROWS)],
        [whole, span.reshape(SPAN, X, Y, Z)],
        scratch=[
            pltpu.VMEM((4 + 8 * EXPAND, Y, Z), F32),
            pltpu.VMEM((ROWS - KEEP, X, Y, Z), F32),
            pltpu.SemaphoreType.DMA((2,)),
        ],
        out="hv",
        limit=4,
    )
    return basis, hessenberg.T


def solution(mesh):
    split = Mesh(
        mesh.devices.reshape(-1, 2, mesh.shape["gy"], mesh.shape["gz"]),
        ("gx_0", "gx_1", "gy", "gz"),
    )
    return jax.shard_map(
        per_device,
        mesh=split,
        in_specs=(
            P(None, GX, "gy", "gz"),
            P(),
            P(GX, "gy", "gz"),
            P(GX, "gy", "gz"),
            P(None, GX, "gy", "gz"),
        ),
        out_specs=(P(None, GX, "gy", "gz"), P()),
        check_vma=False,
    )
```

```python
import functools

import jax
import jax.numpy as jnp
from jax import lax
from jax.experimental import pallas as pl
from jax.experimental.pallas import tpu as pltpu
from jax.sharding import Mesh
from jax.sharding import PartitionSpec as P

KEEP = 20
EXPAND = 3
ROWS = 24
FIELDS = 25
SPAN = 64
SIGMA = 7.125
GX = ("gx_0", "gx_1")
X, Y, Z = (4, 8, 128)
TILE = (Y, Z)
F32 = jnp.float32


def rows_of():
    return lax.broadcasted_iota(jnp.int32, TILE, 0)


def lanes_of():
    return lax.broadcasted_iota(jnp.int32, TILE, 1)


def shift_rows(tile, by):
    by = by % Y
    return tile if by == 0 else pltpu.roll(tile, by, 0)


def shift_lanes(tile, by):
    return pltpu.roll(tile, by, 1)


def place_of(kind):
    return pl.BlockSpec(memory_space={"v": pltpu.VMEM, "s": pltpu.SMEM, "h": pltpu.HBM}[kind])


def call(kernel, outs, args, scratch=(), ins="", out="", flops=100000, limit=2):
    ins, out = ins or "v" * len(args), out or "v" * len(outs)
    return pl.pallas_call(
        kernel,
        out_shape=[jax.ShapeDtypeStruct(s, F32) for s in outs],
        in_specs=[place_of(k) for k in ins],
        out_specs=[place_of(k) for k in out],
        scratch_shapes=list(scratch),
        cost_estimate=pl.CostEstimate(flops=flops, bytes_accessed=100000, transcendentals=0),
        compiler_params=pltpu.CompilerParams(vmem_limit_bytes=limit * 2**20),
    )(*args)


CHUNK = 10


def edge_kernel(
    basis, schur, next_vector, diag, velocity, held, rest, packed, weights, small, sems
):
    chunks = basis.shape[0] // CHUNK
    copies = [
        pltpu.make_async_copy(schur, weights, sems.at[0]),
        *(
            pltpu.make_async_copy(
                basis.at[pl.ds(c * CHUNK, CHUNK)], held.at[pl.ds(c * CHUNK, CHUNK)], sems.at[1 + c]
            )
            for c in range(chunks)
        ),
        pltpu.make_async_copy(next_vector, rest.at[0], sems.at[1 + chunks]),
        pltpu.make_async_copy(diag, small.at[0], sems.at[2 + chunks]),
        pltpu.make_async_copy(velocity, small.at[pl.ds(1, 3)], sems.at[3 + chunks]),
    ]
    for copy in copies:
        copy.start()
    lane = lanes_of()
    copies[0].wait()
    acc = [jnp.zeros(TILE, F32) for _ in range(KEEP)]
    for c in range(chunks):
        copies[1 + c].wait()
        for i in range(c * CHUNK, (c + 1) * CHUNK):
            edge = jnp.zeros(TILE, F32)
            for x in range(X):
                here = (lane >= 6 * x) & (lane < 6 * x + 6)
                edge = jnp.where(here, shift_lanes(held[i, x], 6 * x + 3), edge)
            for f in range(KEEP):
                acc[f] = acc[f] + weights[f, i] * edge
    for p in range(4):
        total = acc[5 * p]
        for q in range(1, 5):
            total = jnp.where(lane < 24 * q, total, shift_lanes(acc[5 * p + q], 24 * q))
        packed[p] = total
    for copy in copies[1 + chunks :]:
        copy.wait()
    for x in range(X):
        rest[1, x] = 6.0 + small[0, x]
        for d in range(3):
            rest[2 + d, x] = 0.5 * small[1 + d, x]
    total = jnp.zeros(TILE, F32)
    for j in range(20):
        moved = shift_lanes(rest[j // 4, j % 4], 6 * j + 3)
        total = jnp.where((lane >= 6 * j) & (lane < 6 * j + 6), moved, total)
    packed[4] = total


def rotate_kernel(basis, schur, rotated):
    group = 5
    for g in range(KEEP // group):

        def body(i, acc, g=g):
            out = []
            tiles = [basis[i, x] for x in range(X)]
            for f in range(group):
                w = schur[g * group + f, i]
                for x in range(X):
                    out.append(acc[f * X + x] + w * tiles[x])
            return tuple(out)

        zero = tuple(jnp.zeros(TILE, F32) for _ in range(group * X))
        acc = lax.fori_loop(0, basis.shape[0], body, zero, unroll=4)
        for f in range(group):
            for x in range(X):
                rotated[g * group + f, x] = acc[f * X + x]


class Fields:
    def __init__(self, rotated, rest):
        self.rotated, self.rest = rotated, rest

    def __getitem__(self, at):
        f, x = at
        if isinstance(f, int) and f >= KEEP:
            return self.rest[f - KEEP, x]
        return self.rotated[f, x]


def pack_y_kernel(rotated, rest, from_lo, from_hi, up, down, halo):
    fields = Fields(rotated, rest)
    row, lane = rows_of(), lanes_of()
    left = lax.rem(lane, 6) < 3
    for f in range(FIELDS):
        a = jnp.zeros(TILE, F32)
        b = a
        for x in range(X):
            tile = fields[f, x]
            here = (row >= 2 * x) & (row < 2 * x + 2)
            a = jnp.where(here, shift_rows(tile, 2 * x - 6), a)
            b = jnp.where(here, shift_rows(tile, 2 * x), b)
        up[f] = a
        down[f] = b
    a = jnp.zeros(TILE, F32)
    b = a
    for x in range(X):
        tile = fields[20, x]
        a = jnp.where(row == x, shift_rows(tile, x - 5), a)
        b = jnp.where(row == x, shift_rows(tile, x - 2), b)
    up[25] = a
    down[25] = b
    for p in range(5):
        merged = jnp.where(left, from_lo[p], from_hi[p])
        halo[p] = merged
        up[26 + p] = merged
        down[26 + p] = merged


def pack_x_kernel(rotated, rest, halo, y_lo, y_hi, off, on):
    fields = Fields(rotated, rest)
    first, row = rows_of() < 4, rows_of()
    upper = lax.axis_index("gx_1") == 1

    def put(at, up, down):
        off[at] = jnp.where(upper, up, down)
        on[at] = jnp.where(upper, down, up)

    for f in range(FIELDS):
        put(2 * f, fields[f, 2], fields[f, 0])
        put(2 * f + 1, fields[f, 3], fields[f, 1])
    put(50, fields[20, 1], fields[20, 2])
    lo, hi = y_lo[20], y_hi[20]
    put(51, jnp.where(first, shift_rows(lo, 4), hi), jnp.where(first, lo, shift_rows(hi, 4)))
    for v in range(6):
        a = jnp.zeros(TILE, F32)
        b = a
        for k in range(4):
            f = 4 * v + k + (1 if v == 5 else 0)
            lo, hi = y_lo[f], y_hi[f]
            a = jnp.where(row == 2 * k, shift_rows(lo, 2 * k - 7), a)
            a = jnp.where(row == 2 * k + 1, shift_rows(hi, 2 * k - 5), a)
            b = jnp.where(row == 2 * k, shift_rows(lo, 2 * k - 1), b)
            b = jnp.where(row == 2 * k + 1, shift_rows(hi, 2 * k + 1), b)
        put(52 + v, a, b)
    for out in (off, on):
        for p in range(5):
            out[58 + p] = halo[p]
        out[63] = y_lo[30]
        out[64] = y_hi[30]


def region(radius):
    out = []
    for a, b in ((0, 0), (1, 0), (0, 1), (1, 1)):
        for x in range(-radius + a + b, X + radius - a - b):
            out.append((x, a, b))
    return out


COEF = region(2)


def tile_of(f, key, refs):
    fields, halo, y_lo, y_hi, x_lo, x_hi, y_halo, x_corner = refs
    x, a, b = key
    first = rows_of() < 4
    if b == 0:
        if a == 0:
            if 0 <= x < X:
                return fields[f, x]
            if x == -3:
                return x_lo[50]
            if x == 6:
                return x_hi[50]
            return x_lo[2 * f + x + 2] if x < 0 else x_hi[2 * f + x - 4]
        if 0 <= x < X:
            lo, hi = y_lo[f], y_hi[f]
            tile = jnp.where(first, shift_rows(hi, -2 * x), shift_rows(lo, 6 - 2 * x))
            if isinstance(f, int) and f == 20:
                row = rows_of()
                tile = jnp.where(row == 2, shift_rows(y_hi[25], 2 - x), tile)
                tile = jnp.where(row == 5, shift_rows(y_lo[25], 5 - x), tile)
            return tile
        side = x_lo if x < 0 else x_hi
        if not (isinstance(f, int) and f == 20):
            g = f - 1 if isinstance(f, int) and f > 20 else f
            v, k = (g // 4, g % 4) if isinstance(g, int) else (lax.div(g, 4), lax.rem(g, 4))
            return pltpu.roll(side[52 + v], 7 - 2 * k, 0)
        packed = side[51]
        if x in (-1, 5):
            return jnp.where(first, shift_rows(packed, 2), shift_rows(packed, 4))
        return jnp.where(first, shift_rows(packed, 4), shift_rows(packed, 6))
    p, q = (f // 5, f % 5) if isinstance(f, int) else (lax.div(f, 5), lax.rem(f, 5))
    place = x if 0 <= x < X else (x + X if x < 0 else x - X)
    by = 128 - 3 - 6 * (4 * q + place)
    if a == 0:
        packed = halo[p] if 0 <= x < X else (x_lo if x < 0 else x_hi)[58 + p]
    elif 0 <= x < X:
        packed = y_halo[p]
    else:
        packed = x_corner[0 if x < 0 else 1]
    return shift_lanes(packed, by)


def apply(get, key, coef, skip=()):
    x, a, b = key
    row, lane = rows_of(), lanes_of()
    centre = get((x, a, b))
    y_other = get((x, 1 - a, b))
    z_other = get((x, a, 1 - b))
    y_ahead = shift_rows(jnp.where(row == 0, y_other, centre), 7)
    y_behind = shift_rows(jnp.where(row == 7, y_other, centre), 1)
    z_ahead = shift_lanes(jnp.where(lane == 0, z_other, centre), 127)
    z_behind = shift_lanes(jnp.where(lane == 127, z_other, centre), 1)
    total = coef(key, 3) * y_ahead + coef(key, 4) * y_behind
    total = total + (coef(key, 5) * z_ahead + coef(key, 6) * z_behind)
    total = total + coef(key, 0) * centre
    for i, at in ((1, (x + 1, a, b)), (2, (x - 1, a, b))):
        if i not in skip:
            total = total + coef(key, i) * get(at)
    return total


def fill_coefficients(keys, out, refs):
    for at, key in enumerate(keys):
        diagonal = tile_of(21, key, refs)
        inside = diagonal != 0.0
        out[at, 0] = jnp.where(inside, diagonal - SIGMA, 0.0)
        for d in range(3):
            half = tile_of(22 + d, key, refs)
            out[at, 1 + 2 * d] = jnp.where(inside, half - 1.0, 0.0)
            out[at, 2 + 2 * d] = jnp.where(inside, -1.0 - half, 0.0)


def cached(f, refs):
    held = {}

    def get(key):
        if key not in held:
            held[key] = tile_of(f, key, refs)
        return held[key]

    return get


INNER = [key for key in COEF if 0 <= key[0] < X]
OUTER = [key for key in COEF if not 0 <= key[0] < X]
ONCE = [key for key in region(1) if 0 <= key[0] < X]
SIDES = {0: (2, -1), X - 1: (1, X)}


def inner_kernel(rotated, rest, halo, y_lo, y_hi, coef_in, partial, y_halo):
    first = rows_of() < 4
    for p in range(5):
        y_halo[p] = jnp.where(first, y_hi[26 + p], y_lo[26 + p])
    refs = (Fields(rotated, rest), halo, y_lo, y_hi, None, None, y_halo, None)
    fill_coefficients(INNER, coef_in, refs)
    coef = lambda key, i: coef_in[INNER.index(key), i]

    def body(f, carry):
        get = cached(f, refs)
        for at, key in enumerate(ONCE):
            skip = (SIDES[key[0]][0],) if key[0] in SIDES else ()
            partial[f, at] = apply(get, key, coef, skip)
        return carry

    lax.fori_loop(0, KEEP, body, 0, unroll=4)


def stencil_kernel(
    copies,
    rotated,
    rest,
    halo,
    y_lo,
    y_hi,
    coef_in,
    partial,
    off,
    on,
    span,
    gram,
    coef_out,
    y_halo,
    x_corner,
    chain,
    x_lo,
    x_hi,
):
    fields = Fields(rotated, rest)
    upper = lax.axis_index("gx_1") == 1
    for i in range(off.shape[0]):
        x_lo[i] = jnp.where(upper, on[i], off[i])
        x_hi[i] = jnp.where(upper, off[i], on[i])
    refs = (fields, halo, y_lo, y_hi, x_lo, x_hi, y_halo, x_corner)
    first = rows_of() < 4
    for p in range(5):
        y_halo[p] = jnp.where(first, y_hi[26 + p], y_lo[26 + p])
    x_corner[0] = jnp.where(first, x_lo[64], x_lo[63])
    x_corner[1] = jnp.where(first, x_hi[64], x_hi[63])
    fill_coefficients(OUTER, coef_out, refs)

    def coef(key, i):
        if key in INNER:
            return coef_in[INNER.index(key), i]
        return coef_out[OUTER.index(key), i]

    def store(f, x, tile):
        at = f * (X * Y) + x * Y
        if not isinstance(f, int):
            at = pl.multiple_of(at, Y)
        span[pl.ds(at, Y), :] = tile

    tiles = {key: tile_of(20, key, refs) for key in region(3)}
    for x in range(X):
        store(60, x, tiles[(x, 0, 0)])
    for step in range(EXPAND):
        place = {}
        for at, key in enumerate(tiles):
            chain[at] = tiles[key]
            place[key] = at
        get = lambda key, place=place: chain[place[key]]
        tiles = {key: apply(get, key, coef) for key in region(2 - step)}
        for x in range(X):
            store(61 + step, x, tiles[(x, 0, 0)])

    def body(f, carry):
        get = cached(f, refs)
        once = {}
        for at, key in enumerate(ONCE):
            x, a, b = key
            tile = partial[f, at]
            if x in SIDES:
                i, side = SIDES[x]
                tile = tile + coef(key, i) * get((side, a, b))
            once[key] = tile
        for x in (-1, X):
            once[(x, 0, 0)] = apply(get, (x, 0, 0), coef)
        for x in range(X):
            store(f, x, get((x, 0, 0)))
            store(f + 20, x, once[(x, 0, 0)])
        for x in range(X):
            store(f + 40, x, apply(once.__getitem__, (x, 0, 0), coef))
        return carry

    lax.fori_loop(0, KEEP, body, 0, unroll=4)

    total = jnp.zeros((SPAN, SPAN), F32)
    for r in range(0, X * Y, 2):
        pair = [span[pl.ds(r + i, SPAN, stride=X * Y), :] for i in range(2)]
        rows = jnp.concatenate(pair, axis=1)
        total = total + lax.dot_general(
            rows,
            rows,
            (((1,), (1,)), ((), ())),
            precision=lax.Precision.HIGHEST,
            preferred_element_type=F32,
        )
    packed = jnp.concatenate([total[:32], total[32:]], axis=1)
    for i in range(copies):
        gram[i] = packed[:16] if i < copies // 2 else packed[16:]


def sum_kernel(copies, parts, out):
    total = parts[0]
    for i in range(1, parts.shape[0]):
        total = total + parts[i]
    for i in range(copies):
        out[i] = total


def exchange(parts, axis):
    return lax.all_to_all(parts, axis, 0, 0)


def finish_kernel(cell_count, parts, span, basis, hessenberg, spread, fresh, sems):
    early = pltpu.make_async_copy(
        span.at[pl.ds(0, KEEP)], basis.at[pl.ds(0, KEEP)], sems.at[0]
    )
    early.start()
    late = [
        pltpu.make_async_copy(fresh.at[k], basis.at[KEEP + k], sems.at[1 + k])
        for k in range(ROWS - KEEP)
    ]
    total = jnp.concatenate([parts[0], parts[1]], axis=0) * (1.0 / cell_count)
    lane = lax.broadcasted_iota(jnp.int32, (32, Z), 1)
    gram = jnp.concatenate(
        [jnp.where(lane < SPAN, total, 0.0), jnp.where(lane < SPAN, pltpu.roll(total, 64, 1), 0.0)],
        axis=0,
    )
    row64 = lax.broadcasted_iota(jnp.int32, (SPAN, Z), 0)
    lane64 = lax.broadcasted_iota(jnp.int32, (SPAN, Z), 1)
    eye = row64 == lane64
    moved = ((row64 >= KEEP) & (row64 < 60) & (lane64 == row64 - KEEP)) | (
        (row64 > 60) & (lane64 == row64 - 1)
    )
    row = lax.broadcasted_iota(jnp.int32, (ROWS, Z), 0)
    lane = lax.broadcasted_iota(jnp.int32, (ROWS, Z), 1)
    lane1 = lax.broadcasted_iota(jnp.int32, (1, Z), 1)

    def column(vector, picks):
        return jnp.sum(jnp.where(picks, vector, 0.0), axis=1, keepdims=True)

    first_row = gram[60:61, :]
    norm_sq = jnp.sum(jnp.where(lane1 == 60, first_row, 0.0), axis=1, keepdims=True)
    inverse = lax.rsqrt(jnp.maximum(norm_sq, 0.25))
    last = jnp.where(lane1 == 60, inverse, 0.0)
    last_gram = first_row * inverse
    up_column = jnp.where(lax.broadcasted_iota(jnp.int32, (SPAN, 1), 0) == 61, inverse, 0.0)
    q = jnp.where((row == lane) & (row < KEEP), 1.0, 0.0)
    q = jnp.where(row == KEEP, last, q)
    qg = jnp.where(row < KEEP, gram[:ROWS, :], 0.0)
    qg = jnp.where(row == KEEP, last_gram, qg)
    scale = jnp.broadcast_to(inverse, TILE)
    for x in range(X):
        fresh[0, x] = span[60, x] * scale
    late[0].start()
    for k in range(EXPAND):
        up = jnp.where(
            (lane1 >= KEEP) & (lane1 < 60),
            pltpu.roll(last, KEEP, 1),
            jnp.where((lane1 > 60) & (lane1 < SPAN), pltpu.roll(last, 1, 1), 0.0),
        )
        image = up + SIGMA * last
        image_gram = jnp.sum(up_column * gram, axis=0, keepdims=True) + SIGMA * last_gram
        c = jnp.sum(q * image_gram, axis=1, keepdims=True)
        partly = image - jnp.sum(c * q, axis=0, keepdims=True)
        partly_gram = image_gram - jnp.sum(c * qg, axis=0, keepdims=True)
        e = jnp.sum(q * partly_gram, axis=1, keepdims=True)
        cleaned = partly - jnp.sum(e * q, axis=0, keepdims=True)
        cleaned_gram = partly_gram - jnp.sum(e * qg, axis=0, keepdims=True)
        length_sq = jnp.sum(cleaned * cleaned_gram, axis=1, keepdims=True)
        here, shifted = column(cleaned, eye), column(cleaned, moved)
        inverse = lax.rsqrt(jnp.maximum(length_sq, 0.25))
        last = cleaned * inverse
        last_gram = cleaned_gram * inverse
        up_column = shifted * inverse
        q = jnp.where(row == KEEP + 1 + k, last, q)
        qg = jnp.where(row == KEEP + 1 + k, last_gram, qg)
        length = jnp.sqrt(jnp.maximum(length_sq, 0.0))
        entries = jnp.where(row == KEEP + 1 + k, length, c + e)
        turned = jnp.sum(jnp.where(row == lane, entries, 0.0), axis=0, keepdims=True)
        hessenberg[k : k + 1, :] = turned[:, :ROWS]
        spread[pl.ds(8 * k, 8)] = jnp.broadcast_to(here * inverse, (SPAN, Z)).reshape(8, 8, Z)
        fields = [*range(KEEP * (k + 1)), *range(60, 62 + k)]
        acc = [jnp.zeros(TILE, F32) for _ in range(X)]
        for f in fields:
            w = spread[8 * k + f // 8, f % 8 : f % 8 + 1, :]
            for x in range(X):
                acc[x] = acc[x] + w * span[f, x]
        for x in range(X):
            fresh[1 + k, x] = acc[x]
        late[1 + k].start()
    early.wait()
    for copy in late:
        copy.wait()


def send(value, axis, forward):
    count = lax.axis_size(axis)
    up = [(i, i + 1) for i in range(count - 1)]
    return lax.ppermute(value, axis, up if forward else [(j, i) for i, j in up])


def per_device(krylov_basis, schur_vectors, next_vector, diag_shift, velocity):
    axes = (*GX, "gy", "gz")
    cell_count = next_vector.size
    for axis in axes:
        cell_count *= lax.axis_size(axis)
    held, rest, packed = call(
        edge_kernel,
        [krylov_basis.shape, (FIELDS - KEEP, X, Y, Z), (5, Y, Z)],
        [
            pltpu.with_memory_space_constraint(value, pltpu.HBM)
            for value in (krylov_basis, schur_vectors.T, next_vector, diag_shift, velocity)
        ],
        scratch=[
            pltpu.SMEM((KEEP, krylov_basis.shape[0]), F32),
            pltpu.VMEM((4, X, Y, Z), F32),
            pltpu.SemaphoreType.DMA((4 + krylov_basis.shape[0] // CHUNK,)),
        ],
        ins="hhhhh",
        limit=4,
    )
    z_lo, z_hi = send(packed, "gz", True), send(packed, "gz", False)
    (rotated,) = call(
        rotate_kernel,
        [(KEEP, X, Y, Z)],
        [held, schur_vectors.T],
        ins="vs",
        limit=4,
        flops=10**9,
    )
    up, down, halo = call(
        pack_y_kernel, [(31, Y, Z), (31, Y, Z), (5, Y, Z)], [rotated, rest, z_lo, z_hi]
    )
    y_lo, y_hi = send(up, "gy", True), send(down, "gy", False)
    off, on = call(
        pack_x_kernel, [(65, Y, Z), (65, Y, Z)], [rotated, rest, halo, y_lo, y_hi]
    )
    count = lax.axis_size(GX)
    swap = [(i, i + 1) for i in range(1, count - 1, 2)]
    off = lax.ppermute(off, GX, swap + [(j, i) for i, j in swap])
    on = lax.ppermute(on, "gx_1", [(0, 1), (1, 0)])
    stages = (("gx_1", "gz"), ("gx_0", "gy"))
    sizes = [lax.axis_size(stage) for stage in stages]
    coef_in, partial = call(
        inner_kernel,
        [(len(INNER), 7, Y, Z), (KEEP, len(ONCE), Y, Z)],
        [rotated, rest, halo, y_lo, y_hi],
        scratch=[pltpu.VMEM((5, Y, Z), F32)],
        limit=6,
        flops=10**9,
    )
    span, parts = call(
        functools.partial(stencil_kernel, sizes[0]),
        [(SPAN * X * Y, Z), (sizes[0], 16, Z)],
        [rotated, rest, halo, y_lo, y_hi, coef_in, partial, off, on],
        scratch=[
            pltpu.VMEM((len(OUTER), 7, Y, Z), F32),
            pltpu.VMEM((5, Y, Z), F32),
            pltpu.VMEM((2, Y, Z), F32),
            pltpu.VMEM((len(region(3)), Y, Z), F32),
            pltpu.VMEM((65, Y, Z), F32),
            pltpu.VMEM((65, Y, Z), F32),
        ],
        limit=8,
    )
    parts = exchange(parts, stages[0])
    (parts,) = call(functools.partial(sum_kernel, sizes[1]), [(sizes[1], 16, Z)], [parts])
    parts = exchange(parts, stages[1])
    (half,) = call(functools.partial(sum_kernel, 1), [(1, 16, Z)], [parts])
    whole = lax.all_gather(half, "gx_1", axis=0, tiled=True)
    basis, hessenberg = call(
        functools.partial(finish_kernel, cell_count),
        [(ROWS, X, Y, Z), (EXPAND, ROWS)],
        [whole, span.reshape(SPAN, X, Y, Z)],
        scratch=[
            pltpu.VMEM((8 * EXPAND, Y, Z), F32),
            pltpu.VMEM((ROWS - KEEP, X, Y, Z), F32),
            pltpu.SemaphoreType.DMA((1 + ROWS - KEEP,)),
        ],
        out="hv",
        limit=4,
    )
    return basis, hessenberg.T


def solution(mesh):
    split = Mesh(
        mesh.devices.reshape(-1, 2, mesh.shape["gy"], mesh.shape["gz"]),
        ("gx_0", "gx_1", "gy", "gz"),
    )
    return jax.shard_map(
        per_device,
        mesh=split,
        in_specs=(
            P(None, GX, "gy", "gz"),
            P(),
            P(GX, "gy", "gz"),
            P(GX, "gy", "gz"),
            P(None, GX, "gy", "gz"),
        ),
        out_specs=(P(None, GX, "gy", "gz"), P()),
        check_vma=False,
    )
```

```python
import functools

import jax
import jax.numpy as jnp
from jax import lax
from jax.experimental import pallas as pl
from jax.experimental.pallas import tpu as pltpu
from jax.sharding import Mesh
from jax.sharding import PartitionSpec as P

KEEP = 20
EXPAND = 3
ROWS = 24
FIELDS = 25
SPAN = 64
SIGMA = 7.125
WIRE = 1280
GX = ("gx_0", "gx_1")
X, Y, Z = (4, 8, 128)
TILE = (Y, Z)
F32 = jnp.float32


def rows_of():
    return lax.broadcasted_iota(jnp.int32, TILE, 0)


def lanes_of():
    return lax.broadcasted_iota(jnp.int32, TILE, 1)


def shift_rows(tile, by):
    by = by % Y
    return tile if by == 0 else pltpu.roll(tile, by, 0)


def shift_lanes(tile, by):
    return pltpu.roll(tile, by, 1)


def place_of(kind):
    return pl.BlockSpec(memory_space={"v": pltpu.VMEM, "s": pltpu.SMEM, "h": pltpu.HBM}[kind])


def call(kernel, outs, args, scratch=(), ins="", out="", flops=100000, limit=2):
    ins, out = ins or "v" * len(args), out or "v" * len(outs)
    return pl.pallas_call(
        kernel,
        out_shape=[jax.ShapeDtypeStruct(s, F32) for s in outs],
        in_specs=[place_of(k) for k in ins],
        out_specs=[place_of(k) for k in out],
        scratch_shapes=list(scratch),
        cost_estimate=pl.CostEstimate(flops=flops, bytes_accessed=100000, transcendentals=0),
        compiler_params=pltpu.CompilerParams(vmem_limit_bytes=limit * 2**20),
    )(*args)


CHUNK = 10


def edge_kernel(
    basis, schur, next_vector, diag, velocity, held, rest, packed, weights, small, sems
):
    chunks = basis.shape[0] // CHUNK
    copies = [
        pltpu.make_async_copy(schur, weights, sems.at[0]),
        *(
            pltpu.make_async_copy(
                basis.at[pl.ds(c * CHUNK, CHUNK)], held.at[pl.ds(c * CHUNK, CHUNK)], sems.at[1 + c]
            )
            for c in range(chunks)
        ),
        pltpu.make_async_copy(next_vector, rest.at[0], sems.at[1 + chunks]),
        pltpu.make_async_copy(diag, small.at[0], sems.at[2 + chunks]),
        pltpu.make_async_copy(velocity, small.at[pl.ds(1, 3)], sems.at[3 + chunks]),
    ]
    for copy in copies:
        copy.start()
    lane = lanes_of()
    copies[0].wait()
    acc = [jnp.zeros(TILE, F32) for _ in range(KEEP)]
    for c in range(chunks):
        copies[1 + c].wait()
        for i in range(c * CHUNK, (c + 1) * CHUNK):
            edge = jnp.zeros(TILE, F32)
            for x in range(X):
                here = (lane >= 6 * x) & (lane < 6 * x + 6)
                edge = jnp.where(here, shift_lanes(held[i, x], 6 * x + 3), edge)
            for f in range(KEEP):
                acc[f] = acc[f] + weights[f, i] * edge
    for p in range(4):
        total = acc[5 * p]
        for q in range(1, 5):
            total = jnp.where(lane < 24 * q, total, shift_lanes(acc[5 * p + q], 24 * q))
        packed[p] = total
    for copy in copies[1 + chunks :]:
        copy.wait()
    for x in range(X):
        rest[1, x] = 6.0 + small[0, x]
        for d in range(3):
            rest[2 + d, x] = 0.5 * small[1 + d, x]
    total = jnp.zeros(TILE, F32)
    for j in range(20):
        moved = shift_lanes(rest[j // 4, j % 4], 6 * j + 3)
        total = jnp.where((lane >= 6 * j) & (lane < 6 * j + 6), moved, total)
    packed[4] = total


def rotate_kernel(basis, schur, rotated):
    group = 5
    for g in range(KEEP // group):

        def body(i, acc, g=g):
            out = []
            tiles = [basis[i, x] for x in range(X)]
            for f in range(group):
                w = schur[g * group + f, i]
                for x in range(X):
                    out.append(acc[f * X + x] + w * tiles[x])
            return tuple(out)

        zero = tuple(jnp.zeros(TILE, F32) for _ in range(group * X))
        acc = lax.fori_loop(0, basis.shape[0], body, zero, unroll=4)
        for f in range(group):
            for x in range(X):
                rotated[g * group + f, x] = acc[f * X + x]


class Fields:
    def __init__(self, rotated, rest):
        self.rotated, self.rest = rotated, rest

    def __getitem__(self, at):
        f, x = at
        if isinstance(f, int) and f >= KEEP:
            return self.rest[f - KEEP, x]
        return self.rotated[f, x]


def pack_y_kernel(rotated, rest, from_lo, from_hi, up, down, halo):
    fields = Fields(rotated, rest)
    row, lane = rows_of(), lanes_of()
    left = lax.rem(lane, 6) < 3
    for f in range(FIELDS):
        a = jnp.zeros(TILE, F32)
        b = a
        for x in range(X):
            tile = fields[f, x]
            here = (row >= 2 * x) & (row < 2 * x + 2)
            a = jnp.where(here, shift_rows(tile, 2 * x - 6), a)
            b = jnp.where(here, shift_rows(tile, 2 * x), b)
        up[f] = a
        down[f] = b
    a = jnp.zeros(TILE, F32)
    b = a
    for x in range(X):
        tile = fields[20, x]
        a = jnp.where(row == x, shift_rows(tile, x - 5), a)
        b = jnp.where(row == x, shift_rows(tile, x - 2), b)
    up[25] = a
    down[25] = b
    for p in range(5):
        merged = jnp.where(left, from_lo[p], from_hi[p])
        halo[p] = merged
        up[26 + p] = merged
        down[26 + p] = merged


def pack_x_kernel(rotated, rest, halo, y_lo, y_hi, off, on):
    fields = Fields(rotated, rest)
    first, row = rows_of() < 4, rows_of()
    upper = lax.axis_index("gx_1") == 1

    def put(at, up, down):
        off[at] = jnp.where(upper, up, down)
        on[at] = jnp.where(upper, down, up)

    for f in range(FIELDS):
        put(2 * f, fields[f, 2], fields[f, 0])
        put(2 * f + 1, fields[f, 3], fields[f, 1])
    put(50, fields[20, 1], fields[20, 2])
    lo, hi = y_lo[20], y_hi[20]
    put(51, jnp.where(first, shift_rows(lo, 4), hi), jnp.where(first, lo, shift_rows(hi, 4)))
    for v in range(6):
        a = jnp.zeros(TILE, F32)
        b = a
        for k in range(4):
            f = 4 * v + k + (1 if v == 5 else 0)
            lo, hi = y_lo[f], y_hi[f]
            a = jnp.where(row == 2 * k, shift_rows(lo, 2 * k - 7), a)
            a = jnp.where(row == 2 * k + 1, shift_rows(hi, 2 * k - 5), a)
            b = jnp.where(row == 2 * k, shift_rows(lo, 2 * k - 1), b)
            b = jnp.where(row == 2 * k + 1, shift_rows(hi, 2 * k + 1), b)
        put(52 + v, a, b)
    for out in (off, on):
        for p in range(5):
            out[58 + p] = halo[p]
        out[63] = y_lo[30]
        out[64] = y_hi[30]


def region(radius):
    out = []
    for a, b in ((0, 0), (1, 0), (0, 1), (1, 1)):
        reach = radius - a - b
        if reach >= 0:
            out.extend((x, a, b) for x in range(-reach, X + reach))
    return out


COEF = region(2)


def tile_of(f, key, refs):
    fields, halo, y_lo, y_hi, x_lo, x_hi, y_halo, x_corner = refs
    x, a, b = key
    first = rows_of() < 4
    if b == 0:
        if a == 0:
            if 0 <= x < X:
                return fields[f, x]
            if x == -3:
                return x_lo[50]
            if x == 6:
                return x_hi[50]
            return x_lo[2 * f + x + 2] if x < 0 else x_hi[2 * f + x - 4]
        if 0 <= x < X:
            lo, hi = y_lo[f], y_hi[f]
            tile = jnp.where(first, shift_rows(hi, -2 * x), shift_rows(lo, 6 - 2 * x))
            if isinstance(f, int) and f == 20:
                row = rows_of()
                tile = jnp.where(row == 2, shift_rows(y_hi[25], 2 - x), tile)
                tile = jnp.where(row == 5, shift_rows(y_lo[25], 5 - x), tile)
            return tile
        side = x_lo if x < 0 else x_hi
        if not (isinstance(f, int) and f == 20):
            g = f - 1 if isinstance(f, int) and f > 20 else f
            v, k = (g // 4, g % 4) if isinstance(g, int) else (lax.div(g, 4), lax.rem(g, 4))
            return pltpu.roll(side[52 + v], 7 - 2 * k, 0)
        packed = side[51]
        if x in (-1, 5):
            return jnp.where(first, shift_rows(packed, 2), shift_rows(packed, 4))
        return jnp.where(first, shift_rows(packed, 4), shift_rows(packed, 6))
    p, q = (f // 5, f % 5) if isinstance(f, int) else (lax.div(f, 5), lax.rem(f, 5))
    place = x if 0 <= x < X else (x + X if x < 0 else x - X)
    by = 128 - 3 - 6 * (4 * q + place)
    if a == 0:
        packed = halo[p] if 0 <= x < X else (x_lo if x < 0 else x_hi)[58 + p]
    elif 0 <= x < X:
        packed = y_halo[p]
    else:
        packed = x_corner[0 if x < 0 else 1]
    return shift_lanes(packed, by)


def apply(get, key, coef, skip=()):
    x, a, b = key
    row, lane = rows_of(), lanes_of()
    centre = get((x, a, b))
    y_other = get((x, 1 - a, b))
    z_other = get((x, a, 1 - b))
    y_ahead = shift_rows(jnp.where(row == 0, y_other, centre), 7)
    y_behind = shift_rows(jnp.where(row == 7, y_other, centre), 1)
    z_ahead = shift_lanes(jnp.where(lane == 0, z_other, centre), 127)
    z_behind = shift_lanes(jnp.where(lane == 127, z_other, centre), 1)
    total = coef(key, 3) * y_ahead + coef(key, 4) * y_behind
    total = total + (coef(key, 5) * z_ahead + coef(key, 6) * z_behind)
    total = total + coef(key, 0) * centre
    for i, at in ((1, (x + 1, a, b)), (2, (x - 1, a, b))):
        if i not in skip:
            total = total + coef(key, i) * get(at)
    return total


def fill_coefficients(keys, out, refs):
    for at, key in enumerate(keys):
        diagonal = tile_of(21, key, refs)
        inside = diagonal != 0.0
        out[at, 0] = jnp.where(inside, diagonal - SIGMA, 0.0)
        for d in range(3):
            half = tile_of(22 + d, key, refs)
            out[at, 1 + 2 * d] = jnp.where(inside, half - 1.0, 0.0)
            out[at, 2 + 2 * d] = jnp.where(inside, -1.0 - half, 0.0)


def cached(f, refs):
    held = {}

    def get(key):
        if key not in held:
            held[key] = tile_of(f, key, refs)
        return held[key]

    return get


INNER = [key for key in COEF if 0 <= key[0] < X]
OUTER = [key for key in COEF if not 0 <= key[0] < X]
ONCE = [key for key in region(1) if 0 <= key[0] < X]
SIDES = {0: (2, -1), X - 1: (1, X)}


def inner_kernel(rotated, rest, halo, y_lo, y_hi, coef_in, partial, y_halo):
    first = rows_of() < 4
    for p in range(5):
        y_halo[p] = jnp.where(first, y_hi[26 + p], y_lo[26 + p])
    refs = (Fields(rotated, rest), halo, y_lo, y_hi, None, None, y_halo, None)
    fill_coefficients(INNER, coef_in, refs)
    coef = lambda key, i: coef_in[INNER.index(key), i]

    def body(f, carry):
        get = cached(f, refs)
        for at, key in enumerate(ONCE):
            skip = (SIDES[key[0]][0],) if key[0] in SIDES else ()
            partial[f, at] = apply(get, key, coef, skip)
        return carry

    lax.fori_loop(0, KEEP, body, 0, unroll=4)


def stencil_kernel(
    copies,
    rotated,
    rest,
    halo,
    y_lo,
    y_hi,
    coef_in,
    partial,
    off,
    on,
    span,
    gram,
    coef_out,
    y_halo,
    x_corner,
    chain,
    x_lo,
    x_hi,
):
    fields = Fields(rotated, rest)
    upper = lax.axis_index("gx_1") == 1
    for i in range(off.shape[0]):
        x_lo[i] = jnp.where(upper, on[i], off[i])
        x_hi[i] = jnp.where(upper, off[i], on[i])
    refs = (fields, halo, y_lo, y_hi, x_lo, x_hi, y_halo, x_corner)
    first = rows_of() < 4
    for p in range(5):
        y_halo[p] = jnp.where(first, y_hi[26 + p], y_lo[26 + p])
    x_corner[0] = jnp.where(first, x_lo[64], x_lo[63])
    x_corner[1] = jnp.where(first, x_hi[64], x_hi[63])
    fill_coefficients(OUTER, coef_out, refs)

    def coef(key, i):
        if key in INNER:
            return coef_in[INNER.index(key), i]
        return coef_out[OUTER.index(key), i]

    def store(f, x, tile):
        at = f * (X * Y) + x * Y
        if not isinstance(f, int):
            at = pl.multiple_of(at, Y)
        span[pl.ds(at, Y), :] = tile

    tiles = {key: tile_of(20, key, refs) for key in region(3)}
    for x in range(X):
        store(60, x, tiles[(x, 0, 0)])
    for step in range(EXPAND):
        place = {}
        for at, key in enumerate(tiles):
            chain[at] = tiles[key]
            place[key] = at
        get = lambda key, place=place: chain[place[key]]
        tiles = {key: apply(get, key, coef) for key in region(2 - step)}
        for x in range(X):
            store(61 + step, x, tiles[(x, 0, 0)])

    def body(f, carry):
        get = cached(f, refs)
        once = {}
        for at, key in enumerate(ONCE):
            x, a, b = key
            tile = partial[f, at]
            if x in SIDES:
                i, side = SIDES[x]
                tile = tile + coef(key, i) * get((side, a, b))
            once[key] = tile
        for x in (-1, X):
            once[(x, 0, 0)] = apply(get, (x, 0, 0), coef)
        for x in range(X):
            store(f, x, get((x, 0, 0)))
            store(f + 20, x, once[(x, 0, 0)])
        for x in range(X):
            store(f + 40, x, apply(once.__getitem__, (x, 0, 0), coef))
        return carry

    lax.fori_loop(0, KEEP, body, 0, unroll=4)

    total = jnp.zeros((SPAN, SPAN), F32)
    for r in range(0, X * Y, 2):
        pair = [span[pl.ds(r + i, SPAN, stride=X * Y), :] for i in range(2)]
        rows = jnp.concatenate(pair, axis=1)
        total = total + lax.dot_general(
            rows,
            rows,
            (((1,), (1,)), ((), ())),
            precision=lax.Precision.HIGHEST,
            preferred_element_type=F32,
        )
    wide = jnp.concatenate([total, jnp.zeros((SPAN, Z - SPAN), F32)], axis=1)
    lane = lax.broadcasted_iota(jnp.int32, (16, Z), 1)
    main = jnp.where(
        lane < 64,
        wide[:16],
        jnp.where(lane < 112, pltpu.roll(wide[16:32], 48, 1), pltpu.roll(wide[48:], 64, 1)),
    )
    lane = lanes_of()
    extra = jnp.zeros(TILE, F32)
    for g in range(4):
        tile = shift_rows(wide[32 + 8 * (g // 2) : 40 + 8 * (g // 2)], -4 * (g % 2))
        tile = tile if g == 1 else shift_lanes(tile, (32 * g - 32) % Z)
        extra = jnp.where((lane >= 32 * g) & (lane < 32 * g + 32), tile, extra)
    for i in range(copies):
        c = i // (copies // 2)
        for k in range(8):
            gram[i, :, Z * k : Z * (k + 1)] = main[8 * c + k : 8 * c + k + 1]
        for k in range(2):
            gram[i, :, Z * (8 + k) : Z * (9 + k)] = extra[2 * c + k : 2 * c + k + 1]


def sum_kernel(copies, parts, out):
    total = parts[0]
    for i in range(1, parts.shape[0]):
        total = total + parts[i]
    for i in range(copies):
        out[i] = total


def exchange(parts, axis):
    return lax.all_to_all(parts, axis, 0, 0)


def finish_kernel(cell_count, parts, span, basis, hessenberg, spread, fresh, sems):
    early = pltpu.make_async_copy(
        span.at[pl.ds(0, KEEP)], basis.at[pl.ds(0, KEEP)], sems.at[0]
    )
    early.start()
    late = [
        pltpu.make_async_copy(fresh.at[k], basis.at[KEEP + k], sems.at[1 + k])
        for k in range(ROWS - KEEP)
    ]
    row = lax.broadcasted_iota(jnp.int32, (16, Z), 0)
    lane = lax.broadcasted_iota(jnp.int32, (16, Z), 1)
    main = jnp.zeros((16, Z), F32)
    extra = jnp.zeros(TILE, F32)
    for c in range(2):
        for k in range(8):
            main = jnp.where(row == 8 * c + k, parts[c, :, Z * k : Z * (k + 1)], main)
        for k in range(2):
            here = rows_of() == 2 * c + k
            extra = jnp.where(here, parts[c, :, Z * (8 + k) : Z * (9 + k)], extra)
    main, extra = main * (1.0 / cell_count), extra * (1.0 / cell_count)
    upper = []
    for g in (0, 2):
        tile = jnp.where(
            rows_of() < 4,
            shift_lanes(extra, (32 - 32 * g) % Z),
            shift_lanes(shift_rows(extra, 4), -32 * g % Z) if g else shift_rows(extra, 4),
        )
        upper.append(jnp.where((lanes_of() >= 32) & (lanes_of() < SPAN), tile, 0.0))
    blocks = jnp.concatenate(
        [
            jnp.where(lane < SPAN, main, 0.0),
            jnp.where((lane >= 16) & (lane < SPAN), pltpu.roll(main, Z - 48, 1), 0.0),
            *upper,
            jnp.where((lane >= 48) & (lane < SPAN), pltpu.roll(main, 64, 1), 0.0),
            jnp.zeros((Z - SPAN, Z), F32),
        ],
        axis=0,
    )
    across = lax.broadcasted_iota(jnp.int32, (Z, Z), 1) // 16
    down = lax.broadcasted_iota(jnp.int32, (Z, Z), 0) // 16
    gram = (blocks + jnp.where(across < down, blocks.T, 0.0))[:SPAN]
    row64 = lax.broadcasted_iota(jnp.int32, (SPAN, Z), 0)
    lane64 = lax.broadcasted_iota(jnp.int32, (SPAN, Z), 1)
    eye = row64 == lane64
    moved = ((row64 >= KEEP) & (row64 < 60) & (lane64 == row64 - KEEP)) | (
        (row64 > 60) & (lane64 == row64 - 1)
    )
    row = lax.broadcasted_iota(jnp.int32, (ROWS, Z), 0)
    lane = lax.broadcasted_iota(jnp.int32, (ROWS, Z), 1)
    lane1 = lax.broadcasted_iota(jnp.int32, (1, Z), 1)

    def column(vector, picks):
        return jnp.sum(jnp.where(picks, vector, 0.0), axis=1, keepdims=True)

    first_row = gram[60:61, :]
    norm_sq = jnp.sum(jnp.where(lane1 == 60, first_row, 0.0), axis=1, keepdims=True)
    inverse = lax.rsqrt(jnp.maximum(norm_sq, 0.25))
    last = jnp.where(lane1 == 60, inverse, 0.0)
    last_gram = first_row * inverse
    up_column = jnp.where(lax.broadcasted_iota(jnp.int32, (SPAN, 1), 0) == 61, inverse, 0.0)
    q = jnp.where((row == lane) & (row < KEEP), 1.0, 0.0)
    q = jnp.where(row == KEEP, last, q)
    qg = jnp.where(row < KEEP, gram[:ROWS, :], 0.0)
    qg = jnp.where(row == KEEP, last_gram, qg)
    scale = jnp.broadcast_to(inverse, TILE)
    for x in range(X):
        fresh[0, x] = span[60, x] * scale
    late[0].start()
    for k in range(EXPAND):
        up = jnp.where(
            (lane1 >= KEEP) & (lane1 < 60),
            pltpu.roll(last, KEEP, 1),
            jnp.where((lane1 > 60) & (lane1 < SPAN), pltpu.roll(last, 1, 1), 0.0),
        )
        image = up + SIGMA * last
        image_gram = jnp.sum(up_column * gram, axis=0, keepdims=True) + SIGMA * last_gram
        c = jnp.sum(q * image_gram, axis=1, keepdims=True)
        partly = image - jnp.sum(c * q, axis=0, keepdims=True)
        partly_gram = image_gram - jnp.sum(c * qg, axis=0, keepdims=True)
        e = jnp.sum(q * partly_gram, axis=1, keepdims=True)
        cleaned = partly - jnp.sum(e * q, axis=0, keepdims=True)
        cleaned_gram = partly_gram - jnp.sum(e * qg, axis=0, keepdims=True)
        length_sq = jnp.sum(cleaned * cleaned_gram, axis=1, keepdims=True)
        here, shifted = column(cleaned, eye), column(cleaned, moved)
        inverse = lax.rsqrt(jnp.maximum(length_sq, 0.25))
        last = cleaned * inverse
        last_gram = cleaned_gram * inverse
        up_column = shifted * inverse
        q = jnp.where(row == KEEP + 1 + k, last, q)
        qg = jnp.where(row == KEEP + 1 + k, last_gram, qg)
        length = jnp.sqrt(jnp.maximum(length_sq, 0.0))
        entries = jnp.where(row == KEEP + 1 + k, length, c + e)
        turned = jnp.sum(jnp.where(row == lane, entries, 0.0), axis=0, keepdims=True)
        hessenberg[k : k + 1, :] = turned[:, :ROWS]
        spread[pl.ds(8 * k, 8)] = jnp.broadcast_to(here * inverse, (SPAN, Z)).reshape(8, 8, Z)
        fields = [*range(KEEP * (k + 1)), *range(60, 62 + k)]
        acc = [jnp.zeros(TILE, F32) for _ in range(X)]
        for f in fields:
            w = spread[8 * k + f // 8, f % 8 : f % 8 + 1, :]
            for x in range(X):
                acc[x] = acc[x] + w * span[f, x]
        for x in range(X):
            fresh[1 + k, x] = acc[x]
        late[1 + k].start()
    early.wait()
    for copy in late:
        copy.wait()


def send(value, axis, forward):
    count = lax.axis_size(axis)
    up = [(i, i + 1) for i in range(count - 1)]
    return lax.ppermute(value, axis, up if forward else [(j, i) for i, j in up])


def per_device(krylov_basis, schur_vectors, next_vector, diag_shift, velocity):
    axes = (*GX, "gy", "gz")
    cell_count = next_vector.size
    for axis in axes:
        cell_count *= lax.axis_size(axis)
    held, rest, packed = call(
        edge_kernel,
        [krylov_basis.shape, (FIELDS - KEEP, X, Y, Z), (5, Y, Z)],
        [
            pltpu.with_memory_space_constraint(value, pltpu.HBM)
            for value in (krylov_basis, schur_vectors.T, next_vector, diag_shift, velocity)
        ],
        scratch=[
            pltpu.SMEM((KEEP, krylov_basis.shape[0]), F32),
            pltpu.VMEM((4, X, Y, Z), F32),
            pltpu.SemaphoreType.DMA((4 + krylov_basis.shape[0] // CHUNK,)),
        ],
        ins="hhhhh",
        limit=4,
    )
    z_lo, z_hi = send(packed, "gz", True), send(packed, "gz", False)
    (rotated,) = call(
        rotate_kernel,
        [(KEEP, X, Y, Z)],
        [held, schur_vectors.T],
        ins="vs",
        limit=4,
        flops=10**9,
    )
    up, down, halo = call(
        pack_y_kernel, [(31, Y, Z), (31, Y, Z), (5, Y, Z)], [rotated, rest, z_lo, z_hi]
    )
    y_lo, y_hi = send(up, "gy", True), send(down, "gy", False)
    off, on = call(
        pack_x_kernel, [(65, Y, Z), (65, Y, Z)], [rotated, rest, halo, y_lo, y_hi]
    )
    count = lax.axis_size(GX)
    swap = [(i, i + 1) for i in range(1, count - 1, 2)]
    off = lax.ppermute(off, GX, swap + [(j, i) for i, j in swap])
    on = lax.ppermute(on, "gx_1", [(0, 1), (1, 0)])
    stages = (("gx_1", "gz"), ("gx_0", "gy"))
    sizes = [lax.axis_size(stage) for stage in stages]
    coef_in, partial = call(
        inner_kernel,
        [(len(INNER), 7, Y, Z), (KEEP, len(ONCE), Y, Z)],
        [rotated, rest, halo, y_lo, y_hi],
        scratch=[pltpu.VMEM((5, Y, Z), F32)],
        limit=6,
        flops=10**9,
    )
    span, parts = call(
        functools.partial(stencil_kernel, sizes[0]),
        [(SPAN * X * Y, Z), (sizes[0], 1, WIRE)],
        [rotated, rest, halo, y_lo, y_hi, coef_in, partial, off, on],
        scratch=[
            pltpu.VMEM((len(OUTER), 7, Y, Z), F32),
            pltpu.VMEM((5, Y, Z), F32),
            pltpu.VMEM((2, Y, Z), F32),
            pltpu.VMEM((len(region(3)), Y, Z), F32),
            pltpu.VMEM((65, Y, Z), F32),
            pltpu.VMEM((65, Y, Z), F32),
        ],
        limit=8,
    )
    parts = exchange(parts, stages[0])
    (parts,) = call(functools.partial(sum_kernel, sizes[1]), [(sizes[1], 1, WIRE)], [parts])
    parts = exchange(parts, stages[1])
    (half,) = call(functools.partial(sum_kernel, 1), [(1, 1, WIRE)], [parts])
    whole = lax.all_gather(half, "gx_1", axis=0, tiled=True)
    basis, hessenberg = call(
        functools.partial(finish_kernel, cell_count),
        [(ROWS, X, Y, Z), (EXPAND, ROWS)],
        [whole, span.reshape(SPAN, X, Y, Z)],
        scratch=[
            pltpu.VMEM((8 * EXPAND, Y, Z), F32),
            pltpu.VMEM((ROWS - KEEP, X, Y, Z), F32),
            pltpu.SemaphoreType.DMA((1 + ROWS - KEEP,)),
        ],
        out="hv",
        limit=4,
    )
    return basis, hessenberg.T


def solution(mesh):
    split = Mesh(
        mesh.devices.reshape(-1, 2, mesh.shape["gy"], mesh.shape["gz"]),
        ("gx_0", "gx_1", "gy", "gz"),
    )
    return jax.shard_map(
        per_device,
        mesh=split,
        in_specs=(
            P(None, GX, "gy", "gz"),
            P(),
            P(GX, "gy", "gz"),
            P(GX, "gy", "gz"),
            P(None, GX, "gy", "gz"),
        ),
        out_specs=(P(None, GX, "gy", "gz"), P()),
        check_vma=False,
    )
```

```python
import functools

import jax
import jax.numpy as jnp
from jax import lax
from jax.experimental import pallas as pl
from jax.experimental.pallas import tpu as pltpu
from jax.sharding import Mesh
from jax.sharding import PartitionSpec as P

KEEP = 20
EXPAND = 3
ROWS = 24
FIELDS = 25
SPAN = 64
SIGMA = 7.125
WIRE = 1280
GX = ("gx_0", "gx_1")
X, Y, Z = (4, 8, 128)
TILE = (Y, Z)
F32 = jnp.float32


def rows_of():
    return lax.broadcasted_iota(jnp.int32, TILE, 0)


def lanes_of():
    return lax.broadcasted_iota(jnp.int32, TILE, 1)


def shift_rows(tile, by):
    by = by % Y
    return tile if by == 0 else pltpu.roll(tile, by, 0)


def shift_lanes(tile, by):
    return pltpu.roll(tile, by, 1)


def place_of(kind):
    return pl.BlockSpec(memory_space={"v": pltpu.VMEM, "s": pltpu.SMEM, "h": pltpu.HBM}[kind])


def call(kernel, outs, args, scratch=(), ins="", out="", flops=100000, limit=2):
    ins, out = ins or "v" * len(args), out or "v" * len(outs)
    return pl.pallas_call(
        kernel,
        out_shape=[jax.ShapeDtypeStruct(s, F32) for s in outs],
        in_specs=[place_of(k) for k in ins],
        out_specs=[place_of(k) for k in out],
        scratch_shapes=list(scratch),
        cost_estimate=pl.CostEstimate(flops=flops, bytes_accessed=100000, transcendentals=0),
        compiler_params=pltpu.CompilerParams(vmem_limit_bytes=limit * 2**20),
    )(*args)


CHUNK = 10


def edge_kernel(
    basis, schur, next_vector, diag, velocity, held, rest, packed, weights, small, sems
):
    chunks = basis.shape[0] // CHUNK
    copies = [
        pltpu.make_async_copy(schur, weights, sems.at[0]),
        *(
            pltpu.make_async_copy(
                basis.at[pl.ds(c * CHUNK, CHUNK)], held.at[pl.ds(c * CHUNK, CHUNK)], sems.at[1 + c]
            )
            for c in range(chunks)
        ),
        pltpu.make_async_copy(next_vector, rest.at[0], sems.at[1 + chunks]),
        pltpu.make_async_copy(diag, small.at[0], sems.at[2 + chunks]),
        pltpu.make_async_copy(velocity, small.at[pl.ds(1, 3)], sems.at[3 + chunks]),
    ]
    for copy in copies:
        copy.start()
    lane = lanes_of()
    copies[0].wait()
    acc = [jnp.zeros(TILE, F32) for _ in range(KEEP)]
    for c in range(chunks):
        copies[1 + c].wait()
        for i in range(c * CHUNK, (c + 1) * CHUNK):
            edge = jnp.zeros(TILE, F32)
            for x in range(X):
                here = (lane >= 6 * x) & (lane < 6 * x + 6)
                edge = jnp.where(here, shift_lanes(held[i, x], 6 * x + 3), edge)
            for f in range(KEEP):
                acc[f] = acc[f] + weights[f, i] * edge
    for p in range(4):
        total = acc[5 * p]
        for q in range(1, 5):
            total = jnp.where(lane < 24 * q, total, shift_lanes(acc[5 * p + q], 24 * q))
        packed[p] = total
    for copy in copies[1 + chunks :]:
        copy.wait()
    for x in range(X):
        rest[1, x] = 6.0 + small[0, x]
        for d in range(3):
            rest[2 + d, x] = 0.5 * small[1 + d, x]
    total = jnp.zeros(TILE, F32)
    for j in range(20):
        moved = shift_lanes(rest[j // 4, j % 4], 6 * j + 3)
        total = jnp.where((lane >= 6 * j) & (lane < 6 * j + 6), moved, total)
    packed[4] = total


def rotate_kernel(basis, schur, rotated):
    group = 5
    for g in range(KEEP // group):

        def body(i, acc, g=g):
            out = []
            tiles = [basis[i, x] for x in range(X)]
            for f in range(group):
                w = schur[g * group + f, i]
                for x in range(X):
                    out.append(acc[f * X + x] + w * tiles[x])
            return tuple(out)

        zero = tuple(jnp.zeros(TILE, F32) for _ in range(group * X))
        acc = lax.fori_loop(0, basis.shape[0], body, zero, unroll=4)
        for f in range(group):
            for x in range(X):
                rotated[g * group + f, x] = acc[f * X + x]


class Fields:
    def __init__(self, rotated, rest):
        self.rotated, self.rest = rotated, rest

    def __getitem__(self, at):
        f, x = at
        if isinstance(f, int) and f >= KEEP:
            return self.rest[f - KEEP, x]
        return self.rotated[f, x]


def pack_y_kernel(rotated, rest, from_lo, from_hi, up, down, halo):
    fields = Fields(rotated, rest)
    row, lane = rows_of(), lanes_of()
    left = lax.rem(lane, 6) < 3
    for f in range(FIELDS):
        a = jnp.zeros(TILE, F32)
        b = a
        for x in range(X):
            tile = fields[f, x]
            here = (row >= 2 * x) & (row < 2 * x + 2)
            a = jnp.where(here, shift_rows(tile, 2 * x - 6), a)
            b = jnp.where(here, shift_rows(tile, 2 * x), b)
        up[f] = a
        down[f] = b
    a = jnp.zeros(TILE, F32)
    b = a
    for x in range(X):
        tile = fields[20, x]
        a = jnp.where(row == x, shift_rows(tile, x - 5), a)
        b = jnp.where(row == x, shift_rows(tile, x - 2), b)
    up[25] = a
    down[25] = b
    a = jnp.zeros(TILE, F32)
    b = a
    for p in range(5):
        merged = jnp.where(left, from_lo[p], from_hi[p])
        halo[p] = merged
        a = jnp.where(row == p, shift_rows(merged, p - 7), a)
        b = jnp.where(row == p, shift_rows(merged, p), b)
    up[26] = jnp.where(row == 5, shift_rows(merged, -1), a)
    down[26] = jnp.where(row == 5, shift_rows(merged, 4), b)


def corner_of(p, y_lo, y_hi):
    row = rows_of()
    lo, hi = y_lo[26], y_hi[26]
    tile = jnp.where(row == 0, shift_rows(hi, -p), jnp.zeros(TILE, F32))
    tile = jnp.where(row == 7, shift_rows(lo, 7 - p), tile)
    if p == 4:
        tile = jnp.where(row == 1, shift_rows(hi, -4), tile)
        tile = jnp.where(row == 6, shift_rows(lo, 1), tile)
    return tile


def pack_x_kernel(rotated, rest, halo, y_lo, y_hi, off, on):
    fields = Fields(rotated, rest)
    first, row = rows_of() < 4, rows_of()
    upper = lax.axis_index("gx_1") == 1

    def put(at, up, down):
        off[at] = jnp.where(upper, up, down)
        on[at] = jnp.where(upper, down, up)

    for f in range(FIELDS):
        put(2 * f, fields[f, 2], fields[f, 0])
        put(2 * f + 1, fields[f, 3], fields[f, 1])
    put(50, fields[20, 1], fields[20, 2])
    lo, hi = y_lo[20], y_hi[20]
    put(51, jnp.where(first, shift_rows(lo, 4), hi), jnp.where(first, lo, shift_rows(hi, 4)))
    for v in range(6):
        a = jnp.zeros(TILE, F32)
        b = a
        for k in range(4):
            f = 4 * v + k + (1 if v == 5 else 0)
            lo, hi = y_lo[f], y_hi[f]
            a = jnp.where(row == 2 * k, shift_rows(lo, 2 * k - 7), a)
            a = jnp.where(row == 2 * k + 1, shift_rows(hi, 2 * k - 5), a)
            b = jnp.where(row == 2 * k, shift_rows(lo, 2 * k - 1), b)
            b = jnp.where(row == 2 * k + 1, shift_rows(hi, 2 * k + 1), b)
        put(52 + v, a, b)
    part = lax.rem(lanes_of(), 24)
    a = jnp.zeros(TILE, F32)
    b = a
    for p in range(4):
        tile = halo[p]
        here = (part >= 18 - 6 * p) & (part < 24 - 6 * p)
        a = jnp.where(here, shift_lanes(tile, -6 * p % Z) if p else tile, a)
        here = (part >= 6 * p) & (part < 6 * p + 6)
        b = jnp.where(here, shift_lanes(tile, 6 * p) if p else tile, b)
    put(58, a, b)
    corner = corner_of(4, y_lo, y_hi)
    put(59, halo[4], halo[4])
    put(60, corner, corner)


def region(radius):
    out = []
    for a, b in ((0, 0), (1, 0), (0, 1), (1, 1)):
        reach = radius - a - b
        if reach >= 0:
            out.extend((x, a, b) for x in range(-reach, X + reach))
    return out


COEF = region(2)


def tile_of(f, key, refs):
    fields, halo, y_lo, y_hi, x_lo, x_hi, y_halo, x_corner = refs
    x, a, b = key
    first = rows_of() < 4
    if b == 0:
        if a == 0:
            if 0 <= x < X:
                return fields[f, x]
            if x == -3:
                return x_lo[50]
            if x == 6:
                return x_hi[50]
            return x_lo[2 * f + x + 2] if x < 0 else x_hi[2 * f + x - 4]
        if 0 <= x < X:
            lo, hi = y_lo[f], y_hi[f]
            tile = jnp.where(first, shift_rows(hi, -2 * x), shift_rows(lo, 6 - 2 * x))
            if isinstance(f, int) and f == 20:
                row = rows_of()
                tile = jnp.where(row == 2, shift_rows(y_hi[25], 2 - x), tile)
                tile = jnp.where(row == 5, shift_rows(y_lo[25], 5 - x), tile)
            return tile
        side = x_lo if x < 0 else x_hi
        if not (isinstance(f, int) and f == 20):
            g = f - 1 if isinstance(f, int) and f > 20 else f
            v, k = (g // 4, g % 4) if isinstance(g, int) else (lax.div(g, 4), lax.rem(g, 4))
            return pltpu.roll(side[52 + v], 7 - 2 * k, 0)
        packed = side[51]
        if x in (-1, 5):
            return jnp.where(first, shift_rows(packed, 2), shift_rows(packed, 4))
        return jnp.where(first, shift_rows(packed, 4), shift_rows(packed, 6))
    p, q = (f // 5, f % 5) if isinstance(f, int) else (lax.div(f, 5), lax.rem(f, 5))
    place = x if 0 <= x < X else (x + X if x < 0 else x - X)
    by = 128 - 3 - 6 * (4 * q + place)
    if a == 0 and not 0 <= x < X and not (isinstance(f, int) and f >= KEEP):
        packed = (x_lo if x < 0 else x_hi)[58]
        by = 128 - 3 - 24 * q - (18 - 6 * p if x < 0 else 6 * p)
    elif a == 0:
        packed = halo[p] if 0 <= x < X else (x_lo if x < 0 else x_hi)[59]
    elif 0 <= x < X:
        packed = y_halo[p]
    else:
        packed = x_corner[0 if x < 0 else 1]
    return shift_lanes(packed, by)


def apply(get, key, coef, skip=()):
    x, a, b = key
    row, lane = rows_of(), lanes_of()
    centre = get((x, a, b))
    y_other = get((x, 1 - a, b))
    z_other = get((x, a, 1 - b))
    y_ahead = shift_rows(jnp.where(row == 0, y_other, centre), 7)
    y_behind = shift_rows(jnp.where(row == 7, y_other, centre), 1)
    z_ahead = shift_lanes(jnp.where(lane == 0, z_other, centre), 127)
    z_behind = shift_lanes(jnp.where(lane == 127, z_other, centre), 1)
    total = coef(key, 3) * y_ahead + coef(key, 4) * y_behind
    total = total + (coef(key, 5) * z_ahead + coef(key, 6) * z_behind)
    total = total + coef(key, 0) * centre
    for i, at in ((1, (x + 1, a, b)), (2, (x - 1, a, b))):
        if i not in skip:
            total = total + coef(key, i) * get(at)
    return total


def fill_coefficients(keys, out, refs):
    for at, key in enumerate(keys):
        diagonal = tile_of(21, key, refs)
        inside = diagonal != 0.0
        out[at, 0] = jnp.where(inside, diagonal - SIGMA, 0.0)
        for d in range(3):
            half = tile_of(22 + d, key, refs)
            out[at, 1 + 2 * d] = jnp.where(inside, half - 1.0, 0.0)
            out[at, 2 + 2 * d] = jnp.where(inside, -1.0 - half, 0.0)


def cached(f, refs):
    held = {}

    def get(key):
        if key not in held:
            held[key] = tile_of(f, key, refs)
        return held[key]

    return get


INNER = [key for key in COEF if 0 <= key[0] < X]
OUTER = [key for key in COEF if not 0 <= key[0] < X]
ONCE = [key for key in region(1) if 0 <= key[0] < X]
SIDES = {0: (2, -1), X - 1: (1, X)}


def inner_kernel(rotated, rest, halo, y_lo, y_hi, coef_in, partial, y_halo):
    for p in range(5):
        y_halo[p] = corner_of(p, y_lo, y_hi)
    refs = (Fields(rotated, rest), halo, y_lo, y_hi, None, None, y_halo, None)
    fill_coefficients(INNER, coef_in, refs)
    coef = lambda key, i: coef_in[INNER.index(key), i]

    def body(f, carry):
        get = cached(f, refs)
        once = {}
        for at, key in enumerate(ONCE):
            skip = (SIDES[key[0]][0],) if key[0] in SIDES else ()
            once[key] = apply(get, key, coef, skip)
            partial[f, at] = once[key]
        for x, skip in ((1, (2,)), (2, (1,))):
            partial[f, len(ONCE) + x - 1] = apply(once.__getitem__, (x, 0, 0), coef, skip)
        return carry

    lax.fori_loop(0, KEEP, body, 0, unroll=4)


def stencil_kernel(
    copies,
    rotated,
    rest,
    halo,
    y_lo,
    y_hi,
    coef_in,
    partial,
    off,
    on,
    span,
    gram,
    coef_out,
    y_halo,
    x_corner,
    chain,
    x_lo,
    x_hi,
):
    fields = Fields(rotated, rest)
    upper = lax.axis_index("gx_1") == 1
    for i in range(off.shape[0]):
        x_lo[i] = jnp.where(upper, on[i], off[i])
        x_hi[i] = jnp.where(upper, off[i], on[i])
    refs = (fields, halo, y_lo, y_hi, x_lo, x_hi, y_halo, x_corner)
    for p in range(5):
        y_halo[p] = corner_of(p, y_lo, y_hi)
    x_corner[0] = x_lo[60]
    x_corner[1] = x_hi[60]
    fill_coefficients(OUTER, coef_out, refs)

    def coef(key, i):
        if key in INNER:
            return coef_in[INNER.index(key), i]
        return coef_out[OUTER.index(key), i]

    def store(f, x, tile):
        at = f * (X * Y) + x * Y
        if not isinstance(f, int):
            at = pl.multiple_of(at, Y)
        span[pl.ds(at, Y), :] = tile

    tiles = {key: tile_of(20, key, refs) for key in region(3)}
    for x in range(X):
        store(60, x, tiles[(x, 0, 0)])
    for step in range(EXPAND):
        place = {}
        for at, key in enumerate(tiles):
            chain[at] = tiles[key]
            place[key] = at
        get = lambda key, place=place: chain[place[key]]
        tiles = {key: apply(get, key, coef) for key in region(2 - step)}
        for x in range(X):
            store(61 + step, x, tiles[(x, 0, 0)])

    def body(f, carry):
        get = cached(f, refs)
        once = {}
        for at, key in enumerate(ONCE):
            x, a, b = key
            if x not in SIDES and (a or b):
                continue
            tile = partial[f, at]
            if x in SIDES:
                i, side = SIDES[x]
                tile = tile + coef(key, i) * get((side, a, b))
            once[key] = tile
        for x in (-1, X):
            once[(x, 0, 0)] = apply(get, (x, 0, 0), coef)
        for x in range(X):
            store(f, x, get((x, 0, 0)))
            store(f + 20, x, once[(x, 0, 0)])
        for x in SIDES:
            store(f + 40, x, apply(once.__getitem__, (x, 0, 0), coef))
        for x, i, near in ((1, 2, 0), (2, 1, 3)):
            term = coef((x, 0, 0), i) * once[(near, 0, 0)]
            store(f + 40, x, partial[f, len(ONCE) + x - 1] + term)
        return carry

    lax.fori_loop(0, KEEP, body, 0, unroll=4)

    total = jnp.zeros((SPAN, SPAN), F32)
    for r in range(0, X * Y, 2):
        pair = [span[pl.ds(r + i, SPAN, stride=X * Y), :] for i in range(2)]
        rows = jnp.concatenate(pair, axis=1)
        total = total + lax.dot_general(
            rows,
            rows,
            (((1,), (1,)), ((), ())),
            precision=lax.Precision.HIGHEST,
            preferred_element_type=F32,
        )
    wide = jnp.concatenate([total, jnp.zeros((SPAN, Z - SPAN), F32)], axis=1)
    lane = lax.broadcasted_iota(jnp.int32, (16, Z), 1)
    main = jnp.where(
        lane < 64,
        wide[:16],
        jnp.where(lane < 112, pltpu.roll(wide[16:32], 48, 1), pltpu.roll(wide[48:], 64, 1)),
    )
    lane = lanes_of()
    extra = jnp.zeros(TILE, F32)
    for g in range(4):
        tile = shift_rows(wide[32 + 8 * (g // 2) : 40 + 8 * (g // 2)], -4 * (g % 2))
        tile = tile if g == 1 else shift_lanes(tile, (32 * g - 32) % Z)
        extra = jnp.where((lane >= 32 * g) & (lane < 32 * g + 32), tile, extra)
    for i in range(copies):
        c = i // (copies // 2)
        for k in range(8):
            gram[i, :, Z * k : Z * (k + 1)] = main[8 * c + k : 8 * c + k + 1]
        for k in range(2):
            gram[i, :, Z * (8 + k) : Z * (9 + k)] = extra[2 * c + k : 2 * c + k + 1]


def sum_kernel(copies, parts, out):
    total = parts[0]
    for i in range(1, parts.shape[0]):
        total = total + parts[i]
    for i in range(copies):
        out[i] = total


def exchange(parts, axis):
    return lax.all_to_all(parts, axis, 0, 0)


def finish_kernel(cell_count, parts, span, basis, hessenberg, spread, fresh, sems):
    early = pltpu.make_async_copy(
        span.at[pl.ds(0, KEEP)], basis.at[pl.ds(0, KEEP)], sems.at[0]
    )
    early.start()
    late = [
        pltpu.make_async_copy(fresh.at[k], basis.at[KEEP + k], sems.at[1 + k])
        for k in range(ROWS - KEEP)
    ]
    row = lax.broadcasted_iota(jnp.int32, (16, Z), 0)
    lane = lax.broadcasted_iota(jnp.int32, (16, Z), 1)
    main = jnp.zeros((16, Z), F32)
    extra = jnp.zeros(TILE, F32)
    for c in range(2):
        for k in range(8):
            main = jnp.where(row == 8 * c + k, parts[c, :, Z * k : Z * (k + 1)], main)
        for k in range(2):
            here = rows_of() == 2 * c + k
            extra = jnp.where(here, parts[c, :, Z * (8 + k) : Z * (9 + k)], extra)
    main, extra = main * (1.0 / cell_count), extra * (1.0 / cell_count)
    upper = []
    for g in (0, 2):
        tile = jnp.where(
            rows_of() < 4,
            shift_lanes(extra, (32 - 32 * g) % Z),
            shift_lanes(shift_rows(extra, 4), -32 * g % Z) if g else shift_rows(extra, 4),
        )
        upper.append(jnp.where((lanes_of() >= 32) & (lanes_of() < SPAN), tile, 0.0))
    blocks = jnp.concatenate(
        [
            jnp.where(lane < SPAN, main, 0.0),
            jnp.where((lane >= 16) & (lane < SPAN), pltpu.roll(main, Z - 48, 1), 0.0),
            *upper,
            jnp.where((lane >= 48) & (lane < SPAN), pltpu.roll(main, 64, 1), 0.0),
            jnp.zeros((Z - SPAN, Z), F32),
        ],
        axis=0,
    )
    across = lax.broadcasted_iota(jnp.int32, (Z, Z), 1) // 16
    down = lax.broadcasted_iota(jnp.int32, (Z, Z), 0) // 16
    gram = (blocks + jnp.where(across < down, blocks.T, 0.0))[:SPAN]
    row64 = lax.broadcasted_iota(jnp.int32, (SPAN, Z), 0)
    lane64 = lax.broadcasted_iota(jnp.int32, (SPAN, Z), 1)
    eye = row64 == lane64
    moved = ((row64 >= KEEP) & (row64 < 60) & (lane64 == row64 - KEEP)) | (
        (row64 > 60) & (lane64 == row64 - 1)
    )
    row = lax.broadcasted_iota(jnp.int32, (ROWS, Z), 0)
    lane = lax.broadcasted_iota(jnp.int32, (ROWS, Z), 1)
    lane1 = lax.broadcasted_iota(jnp.int32, (1, Z), 1)

    def column(vector, picks):
        return jnp.sum(jnp.where(picks, vector, 0.0), axis=1, keepdims=True)

    first_row = gram[60:61, :]
    norm_sq = jnp.sum(jnp.where(lane1 == 60, first_row, 0.0), axis=1, keepdims=True)
    inverse = lax.rsqrt(jnp.maximum(norm_sq, 0.25))
    last = jnp.where(lane1 == 60, inverse, 0.0)
    last_gram = first_row * inverse
    up_column = jnp.where(lax.broadcasted_iota(jnp.int32, (SPAN, 1), 0) == 61, inverse, 0.0)
    q = jnp.where((row == lane) & (row < KEEP), 1.0, 0.0)
    q = jnp.where(row == KEEP, last, q)
    qg = jnp.where(row < KEEP, gram[:ROWS, :], 0.0)
    qg = jnp.where(row == KEEP, last_gram, qg)
    scale = jnp.broadcast_to(inverse, TILE)
    for x in range(X):
        fresh[0, x] = span[60, x] * scale
    late[0].start()
    for k in range(EXPAND):
        up = jnp.where(
            (lane1 >= KEEP) & (lane1 < 60),
            pltpu.roll(last, KEEP, 1),
            jnp.where((lane1 > 60) & (lane1 < SPAN), pltpu.roll(last, 1, 1), 0.0),
        )
        image = up + SIGMA * last
        image_gram = jnp.sum(up_column * gram, axis=0, keepdims=True) + SIGMA * last_gram
        c = jnp.sum(q * image_gram, axis=1, keepdims=True)
        partly = image - jnp.sum(c * q, axis=0, keepdims=True)
        partly_gram = image_gram - jnp.sum(c * qg, axis=0, keepdims=True)
        e = jnp.sum(q * partly_gram, axis=1, keepdims=True)
        cleaned = partly - jnp.sum(e * q, axis=0, keepdims=True)
        cleaned_gram = partly_gram - jnp.sum(e * qg, axis=0, keepdims=True)
        length_sq = jnp.sum(cleaned * cleaned_gram, axis=1, keepdims=True)
        here, shifted = column(cleaned, eye), column(cleaned, moved)
        inverse = lax.rsqrt(jnp.maximum(length_sq, 0.25))
        last = cleaned * inverse
        last_gram = cleaned_gram * inverse
        up_column = shifted * inverse
        q = jnp.where(row == KEEP + 1 + k, last, q)
        qg = jnp.where(row == KEEP + 1 + k, last_gram, qg)
        length = jnp.sqrt(jnp.maximum(length_sq, 0.0))
        entries = jnp.where(row == KEEP + 1 + k, length, c + e)
        turned = jnp.sum(jnp.where(row == lane, entries, 0.0), axis=0, keepdims=True)
        hessenberg[k : k + 1, :] = turned[:, :ROWS]
        spread[pl.ds(8 * k, 8)] = jnp.broadcast_to(here * inverse, (SPAN, Z)).reshape(8, 8, Z)
        fields = [*range(KEEP * (k + 1)), *range(60, 62 + k)]
        acc = [jnp.zeros(TILE, F32) for _ in range(X)]
        for f in fields:
            w = spread[8 * k + f // 8, f % 8 : f % 8 + 1, :]
            for x in range(X):
                acc[x] = acc[x] + w * span[f, x]
        for x in range(X):
            fresh[1 + k, x] = acc[x]
        late[1 + k].start()
    early.wait()
    for copy in late:
        copy.wait()


def send(value, axis, forward):
    count = lax.axis_size(axis)
    up = [(i, i + 1) for i in range(count - 1)]
    return lax.ppermute(value, axis, up if forward else [(j, i) for i, j in up])


def per_device(krylov_basis, schur_vectors, next_vector, diag_shift, velocity):
    axes = (*GX, "gy", "gz")
    cell_count = next_vector.size
    for axis in axes:
        cell_count *= lax.axis_size(axis)
    held, rest, packed = call(
        edge_kernel,
        [krylov_basis.shape, (FIELDS - KEEP, X, Y, Z), (5, Y, Z)],
        [
            pltpu.with_memory_space_constraint(value, pltpu.HBM)
            for value in (krylov_basis, schur_vectors.T, next_vector, diag_shift, velocity)
        ],
        scratch=[
            pltpu.SMEM((KEEP, krylov_basis.shape[0]), F32),
            pltpu.VMEM((4, X, Y, Z), F32),
            pltpu.SemaphoreType.DMA((4 + krylov_basis.shape[0] // CHUNK,)),
        ],
        ins="hhhhh",
        limit=4,
    )
    z_lo, z_hi = send(packed, "gz", True), send(packed, "gz", False)
    (rotated,) = call(
        rotate_kernel,
        [(KEEP, X, Y, Z)],
        [held, schur_vectors.T],
        ins="vs",
        limit=4,
        flops=10**9,
    )
    up, down, halo = call(
        pack_y_kernel, [(27, Y, Z), (27, Y, Z), (5, Y, Z)], [rotated, rest, z_lo, z_hi]
    )
    y_lo, y_hi = send(up, "gy", True), send(down, "gy", False)
    off, on = call(
        pack_x_kernel, [(61, Y, Z), (61, Y, Z)], [rotated, rest, halo, y_lo, y_hi]
    )
    count = lax.axis_size(GX)
    swap = [(i, i + 1) for i in range(1, count - 1, 2)]
    off = lax.ppermute(off, GX, swap + [(j, i) for i, j in swap])
    on = lax.ppermute(on, "gx_1", [(0, 1), (1, 0)])
    stages = (("gx_1", "gz"), ("gx_0", "gy"))
    sizes = [lax.axis_size(stage) for stage in stages]
    coef_in, partial = call(
        inner_kernel,
        [(len(INNER), 7, Y, Z), (KEEP, len(ONCE) + 2, Y, Z)],
        [rotated, rest, halo, y_lo, y_hi],
        scratch=[pltpu.VMEM((5, Y, Z), F32)],
        limit=6,
        flops=10**9,
    )
    span, parts = call(
        functools.partial(stencil_kernel, sizes[0]),
        [(SPAN * X * Y, Z), (sizes[0], 1, WIRE)],
        [rotated, rest, halo, y_lo, y_hi, coef_in, partial, off, on],
        scratch=[
            pltpu.VMEM((len(OUTER), 7, Y, Z), F32),
            pltpu.VMEM((5, Y, Z), F32),
            pltpu.VMEM((2, Y, Z), F32),
            pltpu.VMEM((len(region(3)), Y, Z), F32),
            pltpu.VMEM((61, Y, Z), F32),
            pltpu.VMEM((61, Y, Z), F32),
        ],
        limit=8,
    )
    parts = exchange(parts, stages[0])
    (parts,) = call(functools.partial(sum_kernel, sizes[1]), [(sizes[1], 1, WIRE)], [parts])
    parts = exchange(parts, stages[1])
    (half,) = call(functools.partial(sum_kernel, 1), [(1, 1, WIRE)], [parts])
    whole = lax.all_gather(half, "gx_1", axis=0, tiled=True)
    basis, hessenberg = call(
        functools.partial(finish_kernel, cell_count),
        [(ROWS, X, Y, Z), (EXPAND, ROWS)],
        [whole, span.reshape(SPAN, X, Y, Z)],
        scratch=[
            pltpu.VMEM((8 * EXPAND, Y, Z), F32),
            pltpu.VMEM((ROWS - KEEP, X, Y, Z), F32),
            pltpu.SemaphoreType.DMA((1 + ROWS - KEEP,)),
        ],
        out="hv",
        limit=4,
    )
    return basis, hessenberg.T


def solution(mesh):
    split = Mesh(
        mesh.devices.reshape(-1, 2, mesh.shape["gy"], mesh.shape["gz"]),
        ("gx_0", "gx_1", "gy", "gz"),
    )
    return jax.shard_map(
        per_device,
        mesh=split,
        in_specs=(
            P(None, GX, "gy", "gz"),
            P(),
            P(GX, "gy", "gz"),
            P(GX, "gy", "gz"),
            P(None, GX, "gy", "gz"),
        ),
        out_specs=(P(None, GX, "gy", "gz"), P()),
        check_vma=False,
    )
```

```python
import functools

import jax
import jax.numpy as jnp
from jax import lax
from jax.experimental import pallas as pl
from jax.experimental.pallas import tpu as pltpu
from jax.sharding import Mesh
from jax.sharding import PartitionSpec as P

KEEP = 20
EXPAND = 3
ROWS = 24
FIELDS = 25
SPAN = 64
SIGMA = 7.125
PLANES = 51
WIRE = 1280
GX = ("gx_0", "gx_1")
X, Y, Z = (4, 8, 128)
TILE = (Y, Z)
F32 = jnp.float32


def rows_of():
    return lax.broadcasted_iota(jnp.int32, TILE, 0)


def lanes_of():
    return lax.broadcasted_iota(jnp.int32, TILE, 1)


def shift_rows(tile, by):
    by = by % Y
    return tile if by == 0 else pltpu.roll(tile, by, 0)


def shift_lanes(tile, by):
    return pltpu.roll(tile, by, 1)


def place_of(kind):
    return pl.BlockSpec(memory_space={"v": pltpu.VMEM, "s": pltpu.SMEM, "h": pltpu.HBM}[kind])


def call(kernel, outs, args, scratch=(), ins="", out="", flops=100000, limit=2):
    ins, out = ins or "v" * len(args), out or "v" * len(outs)
    return pl.pallas_call(
        kernel,
        out_shape=[jax.ShapeDtypeStruct(s, F32) for s in outs],
        in_specs=[place_of(k) for k in ins],
        out_specs=[place_of(k) for k in out],
        scratch_shapes=list(scratch),
        cost_estimate=pl.CostEstimate(flops=flops, bytes_accessed=100000, transcendentals=0),
        compiler_params=pltpu.CompilerParams(vmem_limit_bytes=limit * 2**20),
    )(*args)


CHUNK = 10


def edge_kernel(
    basis, schur, next_vector, diag, velocity, held, rest, packed, weights, small, sems
):
    chunks = basis.shape[0] // CHUNK
    copies = [
        pltpu.make_async_copy(schur, weights, sems.at[0]),
        *(
            pltpu.make_async_copy(
                basis.at[pl.ds(c * CHUNK, CHUNK)], held.at[pl.ds(c * CHUNK, CHUNK)], sems.at[1 + c]
            )
            for c in range(chunks)
        ),
        pltpu.make_async_copy(next_vector, rest.at[0], sems.at[1 + chunks]),
        pltpu.make_async_copy(diag, small.at[0], sems.at[2 + chunks]),
        pltpu.make_async_copy(velocity, small.at[pl.ds(1, 3)], sems.at[3 + chunks]),
    ]
    for copy in copies:
        copy.start()
    lane = lanes_of()
    copies[0].wait()
    acc = [jnp.zeros(TILE, F32) for _ in range(KEEP)]
    for c in range(chunks):
        copies[1 + c].wait()
        for i in range(c * CHUNK, (c + 1) * CHUNK):
            edge = jnp.zeros(TILE, F32)
            for x in range(X):
                here = (lane >= 6 * x) & (lane < 6 * x + 6)
                edge = jnp.where(here, shift_lanes(held[i, x], 6 * x + 3), edge)
            for f in range(KEEP):
                acc[f] = acc[f] + weights[f, i] * edge
    for p in range(4):
        total = acc[5 * p]
        for q in range(1, 5):
            total = jnp.where(lane < 24 * q, total, shift_lanes(acc[5 * p + q], 24 * q))
        packed[p] = total
    for copy in copies[1 + chunks :]:
        copy.wait()
    for x in range(X):
        rest[1, x] = 6.0 + small[0, x]
        for d in range(3):
            rest[2 + d, x] = 0.5 * small[1 + d, x]
    total = jnp.zeros(TILE, F32)
    for j in range(20):
        moved = shift_lanes(rest[j // 4, j % 4], 6 * j + 3)
        total = jnp.where((lane >= 6 * j) & (lane < 6 * j + 6), moved, total)
    packed[4] = total


def rotate_kernel(basis, schur, rotated):
    group = 5
    for g in range(KEEP // group):

        def body(i, acc, g=g):
            out = []
            tiles = [basis[i, x] for x in range(X)]
            for f in range(group):
                w = schur[g * group + f, i]
                for x in range(X):
                    out.append(acc[f * X + x] + w * tiles[x])
            return tuple(out)

        zero = tuple(jnp.zeros(TILE, F32) for _ in range(group * X))
        acc = lax.fori_loop(0, basis.shape[0], body, zero, unroll=4)
        for f in range(group):
            for x in range(X):
                rotated[g * group + f, x] = acc[f * X + x]


class Fields:
    def __init__(self, rotated, rest):
        self.rotated, self.rest = rotated, rest

    def __getitem__(self, at):
        f, x = at
        if isinstance(f, int) and f >= KEEP:
            return self.rest[f - KEEP, x]
        return self.rotated[f, x]


def pack_y_kernel(rotated, rest, from_lo, from_hi, up, down, halo):
    fields = Fields(rotated, rest)
    row, lane = rows_of(), lanes_of()
    left = lax.rem(lane, 6) < 3
    for f in range(FIELDS):
        a = jnp.zeros(TILE, F32)
        b = a
        for x in range(X):
            tile = fields[f, x]
            here = (row >= 2 * x) & (row < 2 * x + 2)
            a = jnp.where(here, shift_rows(tile, 2 * x - 6), a)
            b = jnp.where(here, shift_rows(tile, 2 * x), b)
        up[f] = a
        down[f] = b
    a = jnp.zeros(TILE, F32)
    b = a
    for x in range(X):
        tile = fields[20, x]
        a = jnp.where(row == x, shift_rows(tile, x - 5), a)
        b = jnp.where(row == x, shift_rows(tile, x - 2), b)
    up[25] = a
    down[25] = b
    a = jnp.zeros(TILE, F32)
    b = a
    for p in range(5):
        merged = jnp.where(left, from_lo[p], from_hi[p])
        halo[p] = merged
        a = jnp.where(row == p, shift_rows(merged, p - 7), a)
        b = jnp.where(row == p, shift_rows(merged, p), b)
    up[26] = jnp.where(row == 5, shift_rows(merged, -1), a)
    down[26] = jnp.where(row == 5, shift_rows(merged, 4), b)


def corner_of(p, y_lo, y_hi):
    row = rows_of()
    lo, hi = y_lo[26], y_hi[26]
    tile = jnp.where(row == 0, shift_rows(hi, -p), jnp.zeros(TILE, F32))
    tile = jnp.where(row == 7, shift_rows(lo, 7 - p), tile)
    if p == 4:
        tile = jnp.where(row == 1, shift_rows(hi, -4), tile)
        tile = jnp.where(row == 6, shift_rows(lo, 1), tile)
    return tile


def planes_kernel(rotated, rest, early):
    fields = Fields(rotated, rest)
    upper = lax.axis_index("gx_1") == 1
    for f in range(FIELDS):
        early[2 * f] = jnp.where(upper, fields[f, 2], fields[f, 0])
        early[2 * f + 1] = jnp.where(upper, fields[f, 3], fields[f, 1])
    early[PLANES - 1] = jnp.where(upper, fields[20, 1], fields[20, 2])


def keep_kernel(source, out):
    out[...] = source[...]


def pack_x_kernel(rotated, rest, halo, y_lo, y_hi, off, on):
    fields = Fields(rotated, rest)
    first, row = rows_of() < 4, rows_of()
    upper = lax.axis_index("gx_1") == 1

    def put(at, up, down):
        if at >= PLANES:
            off[at - PLANES] = jnp.where(upper, up, down)
        on[at] = jnp.where(upper, down, up)

    for f in range(FIELDS):
        put(2 * f, fields[f, 2], fields[f, 0])
        put(2 * f + 1, fields[f, 3], fields[f, 1])
    put(50, fields[20, 1], fields[20, 2])
    lo, hi = y_lo[20], y_hi[20]
    put(51, jnp.where(first, shift_rows(lo, 4), hi), jnp.where(first, lo, shift_rows(hi, 4)))
    for v in range(6):
        a = jnp.zeros(TILE, F32)
        b = a
        for k in range(4):
            f = 4 * v + k + (1 if v == 5 else 0)
            lo, hi = y_lo[f], y_hi[f]
            a = jnp.where(row == 2 * k, shift_rows(lo, 2 * k - 7), a)
            a = jnp.where(row == 2 * k + 1, shift_rows(hi, 2 * k - 5), a)
            b = jnp.where(row == 2 * k, shift_rows(lo, 2 * k - 1), b)
            b = jnp.where(row == 2 * k + 1, shift_rows(hi, 2 * k + 1), b)
        put(52 + v, a, b)
    part = lax.rem(lanes_of(), 24)
    a = jnp.zeros(TILE, F32)
    b = a
    for p in range(4):
        tile = halo[p]
        here = (part >= 18 - 6 * p) & (part < 24 - 6 * p)
        a = jnp.where(here, shift_lanes(tile, -6 * p % Z) if p else tile, a)
        here = (part >= 6 * p) & (part < 6 * p + 6)
        b = jnp.where(here, shift_lanes(tile, 6 * p) if p else tile, b)
    put(58, a, b)
    corner = corner_of(4, y_lo, y_hi)
    put(59, halo[4], halo[4])
    put(60, corner, corner)


def region(radius):
    out = []
    for a, b in ((0, 0), (1, 0), (0, 1), (1, 1)):
        reach = radius - a - b
        if reach >= 0:
            out.extend((x, a, b) for x in range(-reach, X + reach))
    return out


COEF = region(2)


def tile_of(f, key, refs):
    fields, halo, y_lo, y_hi, x_lo, x_hi, y_halo, x_corner = refs
    x, a, b = key
    first = rows_of() < 4
    if b == 0:
        if a == 0:
            if 0 <= x < X:
                return fields[f, x]
            if x == -3:
                return x_lo[50]
            if x == 6:
                return x_hi[50]
            return x_lo[2 * f + x + 2] if x < 0 else x_hi[2 * f + x - 4]
        if 0 <= x < X:
            lo, hi = y_lo[f], y_hi[f]
            tile = jnp.where(first, shift_rows(hi, -2 * x), shift_rows(lo, 6 - 2 * x))
            if isinstance(f, int) and f == 20:
                row = rows_of()
                tile = jnp.where(row == 2, shift_rows(y_hi[25], 2 - x), tile)
                tile = jnp.where(row == 5, shift_rows(y_lo[25], 5 - x), tile)
            return tile
        side = x_lo if x < 0 else x_hi
        if not (isinstance(f, int) and f == 20):
            g = f - 1 if isinstance(f, int) and f > 20 else f
            v, k = (g // 4, g % 4) if isinstance(g, int) else (lax.div(g, 4), lax.rem(g, 4))
            return pltpu.roll(side[52 + v], 7 - 2 * k, 0)
        packed = side[51]
        if x in (-1, 5):
            return jnp.where(first, shift_rows(packed, 2), shift_rows(packed, 4))
        return jnp.where(first, shift_rows(packed, 4), shift_rows(packed, 6))
    p, q = (f // 5, f % 5) if isinstance(f, int) else (lax.div(f, 5), lax.rem(f, 5))
    place = x if 0 <= x < X else (x + X if x < 0 else x - X)
    by = 128 - 3 - 6 * (4 * q + place)
    if a == 0 and not 0 <= x < X and not (isinstance(f, int) and f >= KEEP):
        packed = (x_lo if x < 0 else x_hi)[58]
        by = 128 - 3 - 24 * q - (18 - 6 * p if x < 0 else 6 * p)
    elif a == 0:
        packed = halo[p] if 0 <= x < X else (x_lo if x < 0 else x_hi)[59]
    elif 0 <= x < X:
        packed = y_halo[p]
    else:
        packed = x_corner[0 if x < 0 else 1]
    return shift_lanes(packed, by)


def apply(get, key, coef, skip=()):
    x, a, b = key
    row, lane = rows_of(), lanes_of()
    centre = get((x, a, b))
    y_other = get((x, 1 - a, b))
    z_other = get((x, a, 1 - b))
    y_ahead = shift_rows(jnp.where(row == 0, y_other, centre), 7)
    y_behind = shift_rows(jnp.where(row == 7, y_other, centre), 1)
    z_ahead = shift_lanes(jnp.where(lane == 0, z_other, centre), 127)
    z_behind = shift_lanes(jnp.where(lane == 127, z_other, centre), 1)
    total = coef(key, 3) * y_ahead + coef(key, 4) * y_behind
    total = total + (coef(key, 5) * z_ahead + coef(key, 6) * z_behind)
    total = total + coef(key, 0) * centre
    for i, at in ((1, (x + 1, a, b)), (2, (x - 1, a, b))):
        if i not in skip:
            total = total + coef(key, i) * get(at)
    return total


def fill_coefficients(keys, out, refs):
    for at, key in enumerate(keys):
        diagonal = tile_of(21, key, refs)
        inside = diagonal != 0.0
        out[at, 0] = jnp.where(inside, diagonal - SIGMA, 0.0)
        for d in range(3):
            half = tile_of(22 + d, key, refs)
            out[at, 1 + 2 * d] = jnp.where(inside, half - 1.0, 0.0)
            out[at, 2 + 2 * d] = jnp.where(inside, -1.0 - half, 0.0)


def cached(f, refs):
    held = {}

    def get(key):
        if key not in held:
            held[key] = tile_of(f, key, refs)
        return held[key]

    return get


INNER = [key for key in COEF if 0 <= key[0] < X]
OUTER = [key for key in COEF if not 0 <= key[0] < X]
ONCE = [key for key in region(1) if 0 <= key[0] < X]
SIDES = {0: (2, -1), X - 1: (1, X)}


def inner_kernel(rotated, rest, halo, y_lo, y_hi, coef_in, partial, y_halo):
    for p in range(5):
        y_halo[p] = corner_of(p, y_lo, y_hi)
    refs = (Fields(rotated, rest), halo, y_lo, y_hi, None, None, y_halo, None)
    fill_coefficients(INNER, coef_in, refs)
    coef = lambda key, i: coef_in[INNER.index(key), i]

    def body(f, carry):
        get = cached(f, refs)
        once = {}
        for at, key in enumerate(ONCE):
            skip = (SIDES[key[0]][0],) if key[0] in SIDES else ()
            once[key] = apply(get, key, coef, skip)
            partial[f, at] = once[key]
        for x, skip in ((1, (2,)), (2, (1,))):
            partial[f, len(ONCE) + x - 1] = apply(once.__getitem__, (x, 0, 0), coef, skip)
        return carry

    lax.fori_loop(0, KEEP, body, 0, unroll=4)


def stencil_kernel(
    copies,
    rotated,
    rest,
    halo,
    y_lo,
    y_hi,
    coef_in,
    partial,
    early,
    off,
    on,
    span,
    gram,
    coef_out,
    y_halo,
    x_corner,
    chain,
    x_lo,
    x_hi,
):
    fields = Fields(rotated, rest)
    upper = lax.axis_index("gx_1") == 1
    for i in range(on.shape[0]):
        far = early[i] if i < PLANES else off[i - PLANES]
        x_lo[i] = jnp.where(upper, on[i], far)
        x_hi[i] = jnp.where(upper, far, on[i])
    refs = (fields, halo, y_lo, y_hi, x_lo, x_hi, y_halo, x_corner)
    for p in range(5):
        y_halo[p] = corner_of(p, y_lo, y_hi)
    x_corner[0] = x_lo[60]
    x_corner[1] = x_hi[60]
    fill_coefficients(OUTER, coef_out, refs)

    def coef(key, i):
        if key in INNER:
            return coef_in[INNER.index(key), i]
        return coef_out[OUTER.index(key), i]

    def store(f, x, tile):
        at = f * (X * Y) + x * Y
        if not isinstance(f, int):
            at = pl.multiple_of(at, Y)
        span[pl.ds(at, Y), :] = tile

    tiles = {key: tile_of(20, key, refs) for key in region(3)}
    for x in range(X):
        store(60, x, tiles[(x, 0, 0)])
    for step in range(EXPAND):
        place = {}
        for at, key in enumerate(tiles):
            chain[at] = tiles[key]
            place[key] = at
        get = lambda key, place=place: chain[place[key]]
        tiles = {key: apply(get, key, coef) for key in region(2 - step)}
        for x in range(X):
            store(61 + step, x, tiles[(x, 0, 0)])

    def body(f, carry):
        get = cached(f, refs)
        once = {}
        for at, key in enumerate(ONCE):
            x, a, b = key
            if x not in SIDES and (a or b):
                continue
            tile = partial[f, at]
            if x in SIDES:
                i, side = SIDES[x]
                tile = tile + coef(key, i) * get((side, a, b))
            once[key] = tile
        for x in (-1, X):
            once[(x, 0, 0)] = apply(get, (x, 0, 0), coef)
        for x in range(X):
            store(f, x, get((x, 0, 0)))
            store(f + 20, x, once[(x, 0, 0)])
        for x in SIDES:
            store(f + 40, x, apply(once.__getitem__, (x, 0, 0), coef))
        for x, i, near in ((1, 2, 0), (2, 1, 3)):
            term = coef((x, 0, 0), i) * once[(near, 0, 0)]
            store(f + 40, x, partial[f, len(ONCE) + x - 1] + term)
        return carry

    lax.fori_loop(0, KEEP, body, 0, unroll=4)

    total = jnp.zeros((SPAN, SPAN), F32)
    for r in range(0, X * Y, 2):
        pair = [span[pl.ds(r + i, SPAN, stride=X * Y), :] for i in range(2)]
        rows = jnp.concatenate(pair, axis=1)
        total = total + lax.dot_general(
            rows,
            rows,
            (((1,), (1,)), ((), ())),
            precision=lax.Precision.HIGHEST,
            preferred_element_type=F32,
        )
    wide = jnp.concatenate([total, jnp.zeros((SPAN, Z - SPAN), F32)], axis=1)
    lane = lax.broadcasted_iota(jnp.int32, (16, Z), 1)
    main = jnp.where(
        lane < 64,
        wide[:16],
        jnp.where(lane < 112, pltpu.roll(wide[16:32], 48, 1), pltpu.roll(wide[48:], 64, 1)),
    )
    lane = lanes_of()
    extra = jnp.zeros(TILE, F32)
    for g in range(4):
        tile = shift_rows(wide[32 + 8 * (g // 2) : 40 + 8 * (g // 2)], -4 * (g % 2))
        tile = tile if g == 1 else shift_lanes(tile, (32 * g - 32) % Z)
        extra = jnp.where((lane >= 32 * g) & (lane < 32 * g + 32), tile, extra)
    for i in range(copies):
        c = i // (copies // 2)
        for k in range(8):
            gram[i, :, Z * k : Z * (k + 1)] = main[8 * c + k : 8 * c + k + 1]
        for k in range(2):
            gram[i, :, Z * (8 + k) : Z * (9 + k)] = extra[2 * c + k : 2 * c + k + 1]


def sum_kernel(copies, parts, out):
    total = parts[0]
    for i in range(1, parts.shape[0]):
        total = total + parts[i]
    for i in range(copies):
        out[i] = total


def exchange(parts, axis):
    return lax.all_to_all(parts, axis, 0, 0)


def finish_kernel(cell_count, parts, span, basis, hessenberg, spread, fresh, sems):
    early = pltpu.make_async_copy(
        span.at[pl.ds(0, KEEP)], basis.at[pl.ds(0, KEEP)], sems.at[0]
    )
    early.start()
    late = [
        pltpu.make_async_copy(fresh.at[k], basis.at[KEEP + k], sems.at[1 + k])
        for k in range(ROWS - KEEP)
    ]
    row = lax.broadcasted_iota(jnp.int32, (16, Z), 0)
    lane = lax.broadcasted_iota(jnp.int32, (16, Z), 1)
    main = jnp.zeros((16, Z), F32)
    extra = jnp.zeros(TILE, F32)
    for c in range(2):
        for k in range(8):
            main = jnp.where(row == 8 * c + k, parts[c, :, Z * k : Z * (k + 1)], main)
        for k in range(2):
            here = rows_of() == 2 * c + k
            extra = jnp.where(here, parts[c, :, Z * (8 + k) : Z * (9 + k)], extra)
    main, extra = main * (1.0 / cell_count), extra * (1.0 / cell_count)
    upper = []
    for g in (0, 2):
        tile = jnp.where(
            rows_of() < 4,
            shift_lanes(extra, (32 - 32 * g) % Z),
            shift_lanes(shift_rows(extra, 4), -32 * g % Z) if g else shift_rows(extra, 4),
        )
        upper.append(jnp.where((lanes_of() >= 32) & (lanes_of() < SPAN), tile, 0.0))
    blocks = jnp.concatenate(
        [
            jnp.where(lane < SPAN, main, 0.0),
            jnp.where((lane >= 16) & (lane < SPAN), pltpu.roll(main, Z - 48, 1), 0.0),
            *upper,
            jnp.where((lane >= 48) & (lane < SPAN), pltpu.roll(main, 64, 1), 0.0),
            jnp.zeros((Z - SPAN, Z), F32),
        ],
        axis=0,
    )
    across = lax.broadcasted_iota(jnp.int32, (Z, Z), 1) // 16
    down = lax.broadcasted_iota(jnp.int32, (Z, Z), 0) // 16
    gram = (blocks + jnp.where(across < down, blocks.T, 0.0))[:SPAN]
    row64 = lax.broadcasted_iota(jnp.int32, (SPAN, Z), 0)
    lane64 = lax.broadcasted_iota(jnp.int32, (SPAN, Z), 1)
    eye = row64 == lane64
    moved = ((row64 >= KEEP) & (row64 < 60) & (lane64 == row64 - KEEP)) | (
        (row64 > 60) & (lane64 == row64 - 1)
    )
    row = lax.broadcasted_iota(jnp.int32, (ROWS, Z), 0)
    lane = lax.broadcasted_iota(jnp.int32, (ROWS, Z), 1)
    lane1 = lax.broadcasted_iota(jnp.int32, (1, Z), 1)

    def column(vector, picks):
        return jnp.sum(jnp.where(picks, vector, 0.0), axis=1, keepdims=True)

    first_row = gram[60:61, :]
    norm_sq = jnp.sum(jnp.where(lane1 == 60, first_row, 0.0), axis=1, keepdims=True)
    inverse = lax.rsqrt(jnp.maximum(norm_sq, 0.25))
    last = jnp.where(lane1 == 60, inverse, 0.0)
    last_gram = first_row * inverse
    up_column = jnp.where(lax.broadcasted_iota(jnp.int32, (SPAN, 1), 0) == 61, inverse, 0.0)
    q = jnp.where((row == lane) & (row < KEEP), 1.0, 0.0)
    q = jnp.where(row == KEEP, last, q)
    qg = jnp.where(row < KEEP, gram[:ROWS, :], 0.0)
    qg = jnp.where(row == KEEP, last_gram, qg)
    scale = jnp.broadcast_to(inverse, TILE)
    for x in range(X):
        fresh[0, x] = span[60, x] * scale
    late[0].start()
    for k in range(EXPAND):
        up = jnp.where(
            (lane1 >= KEEP) & (lane1 < 60),
            pltpu.roll(last, KEEP, 1),
            jnp.where((lane1 > 60) & (lane1 < SPAN), pltpu.roll(last, 1, 1), 0.0),
        )
        image = up + SIGMA * last
        image_gram = jnp.sum(up_column * gram, axis=0, keepdims=True) + SIGMA * last_gram
        c = jnp.sum(q * image_gram, axis=1, keepdims=True)
        partly = image - jnp.sum(c * q, axis=0, keepdims=True)
        partly_gram = image_gram - jnp.sum(c * qg, axis=0, keepdims=True)
        e = jnp.sum(q * partly_gram, axis=1, keepdims=True)
        cleaned = partly - jnp.sum(e * q, axis=0, keepdims=True)
        cleaned_gram = partly_gram - jnp.sum(e * qg, axis=0, keepdims=True)
        length_sq = jnp.sum(cleaned * cleaned_gram, axis=1, keepdims=True)
        here, shifted = column(cleaned, eye), column(cleaned, moved)
        inverse = lax.rsqrt(jnp.maximum(length_sq, 0.25))
        last = cleaned * inverse
        last_gram = cleaned_gram * inverse
        up_column = shifted * inverse
        q = jnp.where(row == KEEP + 1 + k, last, q)
        qg = jnp.where(row == KEEP + 1 + k, last_gram, qg)
        length = jnp.sqrt(jnp.maximum(length_sq, 0.0))
        entries = jnp.where(row == KEEP + 1 + k, length, c + e)
        turned = jnp.sum(jnp.where(row == lane, entries, 0.0), axis=0, keepdims=True)
        hessenberg[k : k + 1, :] = turned[:, :ROWS]
        spread[pl.ds(8 * k, 8)] = jnp.broadcast_to(here * inverse, (SPAN, Z)).reshape(8, 8, Z)
        fields = [*range(KEEP * (k + 1)), *range(60, 62 + k)]
        acc = [jnp.zeros(TILE, F32) for _ in range(X)]
        for f in fields:
            w = spread[8 * k + f // 8, f % 8 : f % 8 + 1, :]
            for x in range(X):
                acc[x] = acc[x] + w * span[f, x]
        for x in range(X):
            fresh[1 + k, x] = acc[x]
        late[1 + k].start()
    early.wait()
    for copy in late:
        copy.wait()


def send(value, axis, forward):
    count = lax.axis_size(axis)
    up = [(i, i + 1) for i in range(count - 1)]
    return lax.ppermute(value, axis, up if forward else [(j, i) for i, j in up])


def per_device(krylov_basis, schur_vectors, next_vector, diag_shift, velocity):
    axes = (*GX, "gy", "gz")
    cell_count = next_vector.size
    for axis in axes:
        cell_count *= lax.axis_size(axis)
    held, rest, packed = call(
        edge_kernel,
        [krylov_basis.shape, (FIELDS - KEEP, X, Y, Z), (5, Y, Z)],
        [
            pltpu.with_memory_space_constraint(value, pltpu.HBM)
            for value in (krylov_basis, schur_vectors.T, next_vector, diag_shift, velocity)
        ],
        scratch=[
            pltpu.SMEM((KEEP, krylov_basis.shape[0]), F32),
            pltpu.VMEM((4, X, Y, Z), F32),
            pltpu.SemaphoreType.DMA((4 + krylov_basis.shape[0] // CHUNK,)),
        ],
        ins="hhhhh",
        limit=4,
    )
    z_lo, z_hi = send(packed, "gz", True), send(packed, "gz", False)
    (rotated,) = call(
        rotate_kernel,
        [(KEEP, X, Y, Z)],
        [held, schur_vectors.T],
        ins="vs",
        limit=4,
        flops=10**9,
    )
    up, down, halo = call(
        pack_y_kernel, [(27, Y, Z), (27, Y, Z), (5, Y, Z)], [rotated, rest, z_lo, z_hi]
    )
    count = lax.axis_size(GX)
    swap = [(i, i + 1) for i in range(1, count - 1, 2)]
    swap = swap + [(j, i) for i, j in swap]
    y_lo = send(up, "gy", True)
    y_hi = send(down, "gy", False)
    (early,) = call(planes_kernel, [(PLANES, Y, Z)], [rotated, rest])
    early = lax.ppermute(early, GX, swap)
    (rest,) = call(keep_kernel, [rest.shape], [rest])
    off, on = call(
        pack_x_kernel, [(61 - PLANES, Y, Z), (61, Y, Z)], [rotated, rest, halo, y_lo, y_hi]
    )
    off = lax.ppermute(off, GX, swap)
    on = lax.ppermute(on, "gx_1", [(0, 1), (1, 0)])
    stages = (("gx_1", "gz"), ("gx_0", "gy"))
    sizes = [lax.axis_size(stage) for stage in stages]
    coef_in, partial = call(
        inner_kernel,
        [(len(INNER), 7, Y, Z), (KEEP, len(ONCE) + 2, Y, Z)],
        [rotated, rest, halo, y_lo, y_hi],
        scratch=[pltpu.VMEM((5, Y, Z), F32)],
        limit=6,
        flops=10**9,
    )
    span, parts = call(
        functools.partial(stencil_kernel, sizes[0]),
        [(SPAN * X * Y, Z), (sizes[0], 1, WIRE)],
        [rotated, rest, halo, y_lo, y_hi, coef_in, partial, early, off, on],
        scratch=[
            pltpu.VMEM((len(OUTER), 7, Y, Z), F32),
            pltpu.VMEM((5, Y, Z), F32),
            pltpu.VMEM((2, Y, Z), F32),
            pltpu.VMEM((len(region(3)), Y, Z), F32),
            pltpu.VMEM((61, Y, Z), F32),
            pltpu.VMEM((61, Y, Z), F32),
        ],
        limit=8,
    )
    parts = exchange(parts, stages[0])
    (parts,) = call(functools.partial(sum_kernel, sizes[1]), [(sizes[1], 1, WIRE)], [parts])
    parts = exchange(parts, stages[1])
    (half,) = call(functools.partial(sum_kernel, 1), [(1, 1, WIRE)], [parts])
    whole = lax.all_gather(half, "gx_1", axis=0, tiled=True)
    basis, hessenberg = call(
        functools.partial(finish_kernel, cell_count),
        [(ROWS, X, Y, Z), (EXPAND, ROWS)],
        [whole, span.reshape(SPAN, X, Y, Z)],
        scratch=[
            pltpu.VMEM((8 * EXPAND, Y, Z), F32),
            pltpu.VMEM((ROWS - KEEP, X, Y, Z), F32),
            pltpu.SemaphoreType.DMA((1 + ROWS - KEEP,)),
        ],
        out="hv",
        limit=4,
    )
    return basis, hessenberg.T


def solution(mesh):
    split = Mesh(
        mesh.devices.reshape(-1, 2, mesh.shape["gy"], mesh.shape["gz"]),
        ("gx_0", "gx_1", "gy", "gz"),
    )
    return jax.shard_map(
        per_device,
        mesh=split,
        in_specs=(
            P(None, GX, "gy", "gz"),
            P(),
            P(GX, "gy", "gz"),
            P(GX, "gy", "gz"),
            P(None, GX, "gy", "gz"),
        ),
        out_specs=(P(None, GX, "gy", "gz"), P()),
        check_vma=False,
    )
```

```python
import functools

import jax
import jax.numpy as jnp
from jax import lax
from jax.experimental import pallas as pl
from jax.experimental.pallas import tpu as pltpu
from jax.sharding import Mesh
from jax.sharding import PartitionSpec as P

KEEP = 20
EXPAND = 3
ROWS = 24
FIELDS = 25
SPAN = 64
SIGMA = 7.125
PLANES = 51
WIRE = 1280
GX = ("gx_0", "gx_1")
X, Y, Z = (4, 8, 128)
TILE = (Y, Z)
F32 = jnp.float32


def rows_of():
    return lax.broadcasted_iota(jnp.int32, TILE, 0)


def lanes_of():
    return lax.broadcasted_iota(jnp.int32, TILE, 1)


def shift_rows(tile, by):
    by = by % Y
    return tile if by == 0 else pltpu.roll(tile, by, 0)


def shift_lanes(tile, by):
    return pltpu.roll(tile, by, 1)


def place_of(kind):
    return pl.BlockSpec(memory_space={"v": pltpu.VMEM, "s": pltpu.SMEM, "h": pltpu.HBM}[kind])


def call(kernel, outs, args, scratch=(), ins="", out="", flops=100000, limit=2):
    ins, out = ins or "v" * len(args), out or "v" * len(outs)
    return pl.pallas_call(
        kernel,
        out_shape=[jax.ShapeDtypeStruct(s, F32) for s in outs],
        in_specs=[place_of(k) for k in ins],
        out_specs=[place_of(k) for k in out],
        scratch_shapes=list(scratch),
        cost_estimate=pl.CostEstimate(flops=flops, bytes_accessed=100000, transcendentals=0),
        compiler_params=pltpu.CompilerParams(vmem_limit_bytes=limit * 2**20),
    )(*args)


CHUNK = 10


def edge_kernel(
    basis, schur, next_vector, diag, velocity, held, rest, packed, weights, small, sems
):
    chunks = basis.shape[0] // CHUNK
    copies = [
        pltpu.make_async_copy(schur, weights, sems.at[0]),
        *(
            pltpu.make_async_copy(
                basis.at[pl.ds(c * CHUNK, CHUNK)], held.at[pl.ds(c * CHUNK, CHUNK)], sems.at[1 + c]
            )
            for c in range(chunks)
        ),
        pltpu.make_async_copy(next_vector, rest.at[0], sems.at[1 + chunks]),
        pltpu.make_async_copy(diag, small.at[0], sems.at[2 + chunks]),
        pltpu.make_async_copy(velocity, small.at[pl.ds(1, 3)], sems.at[3 + chunks]),
    ]
    for copy in copies:
        copy.start()
    lane = lanes_of()
    copies[0].wait()
    acc = [jnp.zeros(TILE, F32) for _ in range(KEEP)]
    for c in range(chunks):
        copies[1 + c].wait()
        for i in range(c * CHUNK, (c + 1) * CHUNK):
            edge = jnp.zeros(TILE, F32)
            for x in range(X):
                here = (lane >= 6 * x) & (lane < 6 * x + 6)
                edge = jnp.where(here, shift_lanes(held[i, x], 6 * x + 3), edge)
            for f in range(KEEP):
                acc[f] = acc[f] + weights[f, i] * edge
    for p in range(4):
        total = acc[5 * p]
        for q in range(1, 5):
            total = jnp.where(lane < 24 * q, total, shift_lanes(acc[5 * p + q], 24 * q))
        packed[p] = total
    for copy in copies[1 + chunks :]:
        copy.wait()
    for x in range(X):
        rest[1, x] = 6.0 + small[0, x]
        for d in range(3):
            rest[2 + d, x] = 0.5 * small[1 + d, x]
    total = jnp.zeros(TILE, F32)
    for j in range(20):
        moved = shift_lanes(rest[j // 4, j % 4], 6 * j + 3)
        total = jnp.where((lane >= 6 * j) & (lane < 6 * j + 6), moved, total)
    packed[4] = total


def rotate_kernel(basis, schur, rotated):
    group = 5
    for g in range(KEEP // group):

        def body(i, acc, g=g):
            out = []
            tiles = [basis[i, x] for x in range(X)]
            for f in range(group):
                w = schur[g * group + f, i]
                for x in range(X):
                    out.append(acc[f * X + x] + w * tiles[x])
            return tuple(out)

        zero = tuple(jnp.zeros(TILE, F32) for _ in range(group * X))
        acc = lax.fori_loop(0, basis.shape[0], body, zero, unroll=4)
        for f in range(group):
            for x in range(X):
                rotated[g * group + f, x] = acc[f * X + x]


class Fields:
    def __init__(self, rotated, rest):
        self.rotated, self.rest = rotated, rest

    def __getitem__(self, at):
        f, x = at
        if isinstance(f, int) and f >= KEEP:
            return self.rest[f - KEEP, x]
        return self.rotated[f, x]


def pack_y_kernel(rotated, rest, from_lo, from_hi, up, down, halo):
    fields = Fields(rotated, rest)
    row, lane = rows_of(), lanes_of()
    left = lax.rem(lane, 6) < 3
    for f in range(FIELDS):
        a = jnp.zeros(TILE, F32)
        b = a
        for x in range(X):
            tile = fields[f, x]
            here = (row >= 2 * x) & (row < 2 * x + 2)
            a = jnp.where(here, shift_rows(tile, 2 * x - 6), a)
            b = jnp.where(here, shift_rows(tile, 2 * x), b)
        up[f] = a
        down[f] = b
    a = jnp.zeros(TILE, F32)
    b = a
    for x in range(X):
        tile = fields[20, x]
        a = jnp.where(row == x, shift_rows(tile, x - 5), a)
        b = jnp.where(row == x, shift_rows(tile, x - 2), b)
    up[25] = a
    down[25] = b
    a = jnp.zeros(TILE, F32)
    b = a
    for p in range(5):
        merged = jnp.where(left, from_lo[p], from_hi[p])
        halo[p] = merged
        a = jnp.where(row == p, shift_rows(merged, p - 7), a)
        b = jnp.where(row == p, shift_rows(merged, p), b)
    up[26] = jnp.where(row == 5, shift_rows(merged, -1), a)
    down[26] = jnp.where(row == 5, shift_rows(merged, 4), b)


def corner_of(p, y_lo, y_hi):
    row = rows_of()
    lo, hi = y_lo[26], y_hi[26]
    tile = jnp.where(row == 0, shift_rows(hi, -p), jnp.zeros(TILE, F32))
    tile = jnp.where(row == 7, shift_rows(lo, 7 - p), tile)
    if p == 4:
        tile = jnp.where(row == 1, shift_rows(hi, -4), tile)
        tile = jnp.where(row == 6, shift_rows(lo, 1), tile)
    return tile


def planes_kernel(rotated, rest, early):
    fields = Fields(rotated, rest)
    upper = lax.axis_index("gx_1") == 1
    for f in range(FIELDS):
        early[2 * f] = jnp.where(upper, fields[f, 2], fields[f, 0])
        early[2 * f + 1] = jnp.where(upper, fields[f, 3], fields[f, 1])
    early[PLANES - 1] = jnp.where(upper, fields[20, 1], fields[20, 2])


def pack_x_kernel(rotated, rest, halo, y_lo, y_hi, off, on):
    fields = Fields(rotated, rest)
    first, row = rows_of() < 4, rows_of()
    upper = lax.axis_index("gx_1") == 1

    def put(at, up, down):
        if at >= PLANES:
            off[at - PLANES] = jnp.where(upper, up, down)
        on[at] = jnp.where(upper, down, up)

    for f in range(FIELDS):
        put(2 * f, fields[f, 2], fields[f, 0])
        put(2 * f + 1, fields[f, 3], fields[f, 1])
    put(50, fields[20, 1], fields[20, 2])
    lo, hi = y_lo[20], y_hi[20]
    put(51, jnp.where(first, shift_rows(lo, 4), hi), jnp.where(first, lo, shift_rows(hi, 4)))
    for v in range(6):
        a = jnp.zeros(TILE, F32)
        b = a
        for k in range(4):
            f = 4 * v + k + (1 if v == 5 else 0)
            lo, hi = y_lo[f], y_hi[f]
            a = jnp.where(row == 2 * k, shift_rows(lo, 2 * k - 7), a)
            a = jnp.where(row == 2 * k + 1, shift_rows(hi, 2 * k - 5), a)
            b = jnp.where(row == 2 * k, shift_rows(lo, 2 * k - 1), b)
            b = jnp.where(row == 2 * k + 1, shift_rows(hi, 2 * k + 1), b)
        put(52 + v, a, b)
    part = lax.rem(lanes_of(), 24)
    a = jnp.zeros(TILE, F32)
    b = a
    for p in range(4):
        tile = halo[p]
        here = (part >= 18 - 6 * p) & (part < 24 - 6 * p)
        a = jnp.where(here, shift_lanes(tile, -6 * p % Z) if p else tile, a)
        here = (part >= 6 * p) & (part < 6 * p + 6)
        b = jnp.where(here, shift_lanes(tile, 6 * p) if p else tile, b)
    put(58, a, b)
    corner = corner_of(4, y_lo, y_hi)
    put(59, halo[4], halo[4])
    put(60, corner, corner)


def region(radius):
    out = []
    for a, b in ((0, 0), (1, 0), (0, 1), (1, 1)):
        reach = radius - a - b
        if reach >= 0:
            out.extend((x, a, b) for x in range(-reach, X + reach))
    return out


COEF = region(2)


def tile_of(f, key, refs):
    fields, halo, y_lo, y_hi, x_lo, x_hi, y_halo, x_corner = refs
    x, a, b = key
    first = rows_of() < 4
    if b == 0:
        if a == 0:
            if 0 <= x < X:
                return fields[f, x]
            if x == -3:
                return x_lo[50]
            if x == 6:
                return x_hi[50]
            return x_lo[2 * f + x + 2] if x < 0 else x_hi[2 * f + x - 4]
        if 0 <= x < X:
            lo, hi = y_lo[f], y_hi[f]
            tile = jnp.where(first, shift_rows(hi, -2 * x), shift_rows(lo, 6 - 2 * x))
            if isinstance(f, int) and f == 20:
                row = rows_of()
                tile = jnp.where(row == 2, shift_rows(y_hi[25], 2 - x), tile)
                tile = jnp.where(row == 5, shift_rows(y_lo[25], 5 - x), tile)
            return tile
        side = x_lo if x < 0 else x_hi
        if not (isinstance(f, int) and f == 20):
            g = f - 1 if isinstance(f, int) and f > 20 else f
            v, k = (g // 4, g % 4) if isinstance(g, int) else (lax.div(g, 4), lax.rem(g, 4))
            return pltpu.roll(side[52 + v], 7 - 2 * k, 0)
        packed = side[51]
        if x in (-1, 5):
            return jnp.where(first, shift_rows(packed, 2), shift_rows(packed, 4))
        return jnp.where(first, shift_rows(packed, 4), shift_rows(packed, 6))
    p, q = (f // 5, f % 5) if isinstance(f, int) else (lax.div(f, 5), lax.rem(f, 5))
    place = x if 0 <= x < X else (x + X if x < 0 else x - X)
    by = 128 - 3 - 6 * (4 * q + place)
    if a == 0 and not 0 <= x < X and not (isinstance(f, int) and f >= KEEP):
        packed = (x_lo if x < 0 else x_hi)[58]
        by = 128 - 3 - 24 * q - (18 - 6 * p if x < 0 else 6 * p)
    elif a == 0:
        packed = halo[p] if 0 <= x < X else (x_lo if x < 0 else x_hi)[59]
    elif 0 <= x < X:
        packed = y_halo[p]
    else:
        packed = x_corner[0 if x < 0 else 1]
    return shift_lanes(packed, by)


def along_y(get, key, coef):
    x, a, b = key
    row = rows_of()
    centre, other = get(key), get((x, 1 - a, b))
    ahead = shift_rows(jnp.where(row == 0, other, centre), 7)
    behind = shift_rows(jnp.where(row == 7, other, centre), 1)
    return coef(key, 3) * ahead + coef(key, 4) * behind


def apply(get, key, coef, skip=(), with_y=True):
    x, a, b = key
    lane = lanes_of()
    centre, other = get(key), get((x, a, 1 - b))
    ahead = shift_lanes(jnp.where(lane == 0, other, centre), 127)
    behind = shift_lanes(jnp.where(lane == 127, other, centre), 1)
    total = coef(key, 5) * ahead + coef(key, 6) * behind
    if with_y:
        total = along_y(get, key, coef) + total
    total = total + coef(key, 0) * centre
    for i, at in ((1, (x + 1, a, b)), (2, (x - 1, a, b))):
        if i not in skip:
            total = total + coef(key, i) * get(at)
    return total


def fill_coefficients(keys, out, refs):
    for at, key in enumerate(keys):
        diagonal = tile_of(21, key, refs)
        inside = diagonal != 0.0
        out[at, 0] = jnp.where(inside, diagonal - SIGMA, 0.0)
        for d in range(3):
            half = tile_of(22 + d, key, refs)
            out[at, 1 + 2 * d] = jnp.where(inside, half - 1.0, 0.0)
            out[at, 2 + 2 * d] = jnp.where(inside, -1.0 - half, 0.0)


def cached(f, refs):
    held = {}

    def get(key):
        if key not in held:
            held[key] = tile_of(f, key, refs)
        return held[key]

    return get


INNER = [key for key in COEF if 0 <= key[0] < X]
LEVEL = [key for key in INNER if not key[1]]
BESIDE = [key for key in INNER if key[1]]
OUTER = [key for key in COEF if not 0 <= key[0] < X]
ONCE = [key for key in region(1) if 0 <= key[0] < X]
SIDES = {0: (2, -1), X - 1: (1, X)}


def skip_of(key):
    return (SIDES[key[0]][0],) if key[0] in SIDES else ()


def level_kernel(rotated, rest, halo, coef_level, partial):
    refs = (Fields(rotated, rest), halo, None, None, None, None, None, None)
    fill_coefficients(LEVEL, coef_level, refs)
    coef = lambda key, i: coef_level[LEVEL.index(key), i]

    def body(f, carry):
        get = cached(f, refs)
        for at, key in enumerate(LEVEL):
            partial[f, at] = apply(get, key, coef, skip_of(key), with_y=False)
        return carry

    lax.fori_loop(0, KEEP, body, 0, unroll=4)


def inner_kernel(
    rotated, rest, halo, y_lo, y_hi, coef_level, level, coef_beside, partial, y_halo
):
    for p in range(5):
        y_halo[p] = corner_of(p, y_lo, y_hi)
    refs = (Fields(rotated, rest), halo, y_lo, y_hi, None, None, y_halo, None)
    fill_coefficients(BESIDE, coef_beside, refs)

    def coef(key, i):
        if key in LEVEL:
            return coef_level[LEVEL.index(key), i]
        return coef_beside[BESIDE.index(key), i]

    def body(f, carry):
        get = cached(f, refs)
        once = {}
        for at, key in enumerate(ONCE):
            if key in LEVEL:
                once[key] = level[f, LEVEL.index(key)] + along_y(get, key, coef)
            else:
                once[key] = apply(get, key, coef, skip_of(key))
            partial[f, at] = once[key]
        for x, skip in ((1, (2,)), (2, (1,))):
            partial[f, len(ONCE) + x - 1] = apply(once.__getitem__, (x, 0, 0), coef, skip)
        return carry

    lax.fori_loop(0, KEEP, body, 0, unroll=4)


def stencil_kernel(
    copies,
    rotated,
    rest,
    halo,
    y_lo,
    y_hi,
    coef_level,
    coef_beside,
    partial,
    early,
    off,
    on,
    span,
    gram,
    coef_out,
    y_halo,
    x_corner,
    chain,
    x_lo,
    x_hi,
):
    fields = Fields(rotated, rest)
    upper = lax.axis_index("gx_1") == 1
    for i in range(on.shape[0]):
        far = early[i] if i < PLANES else off[i - PLANES]
        x_lo[i] = jnp.where(upper, on[i], far)
        x_hi[i] = jnp.where(upper, far, on[i])
    refs = (fields, halo, y_lo, y_hi, x_lo, x_hi, y_halo, x_corner)
    for p in range(5):
        y_halo[p] = corner_of(p, y_lo, y_hi)
    x_corner[0] = x_lo[60]
    x_corner[1] = x_hi[60]
    fill_coefficients(OUTER, coef_out, refs)

    def coef(key, i):
        if key in LEVEL:
            return coef_level[LEVEL.index(key), i]
        if key in BESIDE:
            return coef_beside[BESIDE.index(key), i]
        return coef_out[OUTER.index(key), i]

    def store(f, x, tile):
        at = f * (X * Y) + x * Y
        if not isinstance(f, int):
            at = pl.multiple_of(at, Y)
        span[pl.ds(at, Y), :] = tile

    tiles = {key: tile_of(20, key, refs) for key in region(3)}
    for x in range(X):
        store(60, x, tiles[(x, 0, 0)])
    for step in range(EXPAND):
        place = {}
        for at, key in enumerate(tiles):
            chain[at] = tiles[key]
            place[key] = at
        get = lambda key, place=place: chain[place[key]]
        tiles = {key: apply(get, key, coef) for key in region(2 - step)}
        for x in range(X):
            store(61 + step, x, tiles[(x, 0, 0)])

    def body(f, carry):
        get = cached(f, refs)
        once = {}
        for at, key in enumerate(ONCE):
            x, a, b = key
            if x not in SIDES and (a or b):
                continue
            tile = partial[f, at]
            if x in SIDES:
                i, side = SIDES[x]
                tile = tile + coef(key, i) * get((side, a, b))
            once[key] = tile
        for x in (-1, X):
            once[(x, 0, 0)] = apply(get, (x, 0, 0), coef)
        for x in range(X):
            store(f, x, get((x, 0, 0)))
            store(f + 20, x, once[(x, 0, 0)])
        for x in SIDES:
            store(f + 40, x, apply(once.__getitem__, (x, 0, 0), coef))
        for x, i, near in ((1, 2, 0), (2, 1, 3)):
            term = coef((x, 0, 0), i) * once[(near, 0, 0)]
            store(f + 40, x, partial[f, len(ONCE) + x - 1] + term)
        return carry

    lax.fori_loop(0, KEEP, body, 0, unroll=4)

    total = jnp.zeros((SPAN, SPAN), F32)
    for r in range(0, X * Y, 2):
        pair = [span[pl.ds(r + i, SPAN, stride=X * Y), :] for i in range(2)]
        rows = jnp.concatenate(pair, axis=1)
        total = total + lax.dot_general(
            rows,
            rows,
            (((1,), (1,)), ((), ())),
            precision=lax.Precision.HIGHEST,
            preferred_element_type=F32,
        )
    wide = jnp.concatenate([total, jnp.zeros((SPAN, Z - SPAN), F32)], axis=1)
    lane = lax.broadcasted_iota(jnp.int32, (16, Z), 1)
    main = jnp.where(
        lane < 64,
        wide[:16],
        jnp.where(lane < 112, pltpu.roll(wide[16:32], 48, 1), pltpu.roll(wide[48:], 64, 1)),
    )
    lane = lanes_of()
    extra = jnp.zeros(TILE, F32)
    for g in range(4):
        tile = shift_rows(wide[32 + 8 * (g // 2) : 40 + 8 * (g // 2)], -4 * (g % 2))
        tile = tile if g == 1 else shift_lanes(tile, (32 * g - 32) % Z)
        extra = jnp.where((lane >= 32 * g) & (lane < 32 * g + 32), tile, extra)
    for i in range(copies):
        c = i // (copies // 2)
        for k in range(8):
            gram[i, :, Z * k : Z * (k + 1)] = main[8 * c + k : 8 * c + k + 1]
        for k in range(2):
            gram[i, :, Z * (8 + k) : Z * (9 + k)] = extra[2 * c + k : 2 * c + k + 1]


def sum_kernel(copies, parts, out):
    total = parts[0]
    for i in range(1, parts.shape[0]):
        total = total + parts[i]
    for i in range(copies):
        out[i] = total


def exchange(parts, axis):
    return lax.all_to_all(parts, axis, 0, 0)


def finish_kernel(cell_count, parts, span, basis, hessenberg, spread, fresh, sems):
    early = pltpu.make_async_copy(
        span.at[pl.ds(0, KEEP)], basis.at[pl.ds(0, KEEP)], sems.at[0]
    )
    early.start()
    late = [
        pltpu.make_async_copy(fresh.at[k], basis.at[KEEP + k], sems.at[1 + k])
        for k in range(ROWS - KEEP)
    ]
    row = lax.broadcasted_iota(jnp.int32, (16, Z), 0)
    lane = lax.broadcasted_iota(jnp.int32, (16, Z), 1)
    main = jnp.zeros((16, Z), F32)
    extra = jnp.zeros(TILE, F32)
    for c in range(2):
        for k in range(8):
            main = jnp.where(row == 8 * c + k, parts[c, :, Z * k : Z * (k + 1)], main)
        for k in range(2):
            here = rows_of() == 2 * c + k
            extra = jnp.where(here, parts[c, :, Z * (8 + k) : Z * (9 + k)], extra)
    main, extra = main * (1.0 / cell_count), extra * (1.0 / cell_count)
    upper = []
    for g in (0, 2):
        tile = jnp.where(
            rows_of() < 4,
            shift_lanes(extra, (32 - 32 * g) % Z),
            shift_lanes(shift_rows(extra, 4), -32 * g % Z) if g else shift_rows(extra, 4),
        )
        upper.append(jnp.where((lanes_of() >= 32) & (lanes_of() < SPAN), tile, 0.0))
    blocks = jnp.concatenate(
        [
            jnp.where(lane < SPAN, main, 0.0),
            jnp.where((lane >= 16) & (lane < SPAN), pltpu.roll(main, Z - 48, 1), 0.0),
            *upper,
            jnp.where((lane >= 48) & (lane < SPAN), pltpu.roll(main, 64, 1), 0.0),
            jnp.zeros((Z - SPAN, Z), F32),
        ],
        axis=0,
    )
    across = lax.broadcasted_iota(jnp.int32, (Z, Z), 1) // 16
    down = lax.broadcasted_iota(jnp.int32, (Z, Z), 0) // 16
    gram = (blocks + jnp.where(across < down, blocks.T, 0.0))[:SPAN]
    row64 = lax.broadcasted_iota(jnp.int32, (SPAN, Z), 0)
    lane64 = lax.broadcasted_iota(jnp.int32, (SPAN, Z), 1)
    eye = row64 == lane64
    moved = ((row64 >= KEEP) & (row64 < 60) & (lane64 == row64 - KEEP)) | (
        (row64 > 60) & (lane64 == row64 - 1)
    )
    row = lax.broadcasted_iota(jnp.int32, (ROWS, Z), 0)
    lane = lax.broadcasted_iota(jnp.int32, (ROWS, Z), 1)
    lane1 = lax.broadcasted_iota(jnp.int32, (1, Z), 1)

    def column(vector, picks):
        return jnp.sum(jnp.where(picks, vector, 0.0), axis=1, keepdims=True)

    first_row = gram[60:61, :]
    norm_sq = jnp.sum(jnp.where(lane1 == 60, first_row, 0.0), axis=1, keepdims=True)
    inverse = lax.rsqrt(jnp.maximum(norm_sq, 0.25))
    last = jnp.where(lane1 == 60, inverse, 0.0)
    last_gram = first_row * inverse
    up_column = jnp.where(lax.broadcasted_iota(jnp.int32, (SPAN, 1), 0) == 61, inverse, 0.0)
    q = jnp.where((row == lane) & (row < KEEP), 1.0, 0.0)
    q = jnp.where(row == KEEP, last, q)
    qg = jnp.where(row < KEEP, gram[:ROWS, :], 0.0)
    qg = jnp.where(row == KEEP, last_gram, qg)
    scale = jnp.broadcast_to(inverse, TILE)
    for x in range(X):
        fresh[0, x] = span[60, x] * scale
    late[0].start()
    for k in range(EXPAND):
        up = jnp.where(
            (lane1 >= KEEP) & (lane1 < 60),
            pltpu.roll(last, KEEP, 1),
            jnp.where((lane1 > 60) & (lane1 < SPAN), pltpu.roll(last, 1, 1), 0.0),
        )
        image = up + SIGMA * last
        image_gram = jnp.sum(up_column * gram, axis=0, keepdims=True) + SIGMA * last_gram
        c = jnp.sum(q * image_gram, axis=1, keepdims=True)
        partly = image - jnp.sum(c * q, axis=0, keepdims=True)
        partly_gram = image_gram - jnp.sum(c * qg, axis=0, keepdims=True)
        e = jnp.sum(q * partly_gram, axis=1, keepdims=True)
        cleaned = partly - jnp.sum(e * q, axis=0, keepdims=True)
        cleaned_gram = partly_gram - jnp.sum(e * qg, axis=0, keepdims=True)
        length_sq = jnp.sum(cleaned * cleaned_gram, axis=1, keepdims=True)
        here, shifted = column(cleaned, eye), column(cleaned, moved)
        inverse = lax.rsqrt(jnp.maximum(length_sq, 0.25))
        last = cleaned * inverse
        last_gram = cleaned_gram * inverse
        up_column = shifted * inverse
        q = jnp.where(row == KEEP + 1 + k, last, q)
        qg = jnp.where(row == KEEP + 1 + k, last_gram, qg)
        length = jnp.sqrt(jnp.maximum(length_sq, 0.0))
        entries = jnp.where(row == KEEP + 1 + k, length, c + e)
        turned = jnp.sum(jnp.where(row == lane, entries, 0.0), axis=0, keepdims=True)
        hessenberg[k : k + 1, :] = turned[:, :ROWS]
        spread[pl.ds(8 * k, 8)] = jnp.broadcast_to(here * inverse, (SPAN, Z)).reshape(8, 8, Z)
        fields = [*range(KEEP * (k + 1)), *range(60, 62 + k)]
        acc = [jnp.zeros(TILE, F32) for _ in range(X)]
        for f in fields:
            w = spread[8 * k + f // 8, f % 8 : f % 8 + 1, :]
            for x in range(X):
                acc[x] = acc[x] + w * span[f, x]
        for x in range(X):
            fresh[1 + k, x] = acc[x]
        late[1 + k].start()
    early.wait()
    for copy in late:
        copy.wait()


def send(value, axis, forward):
    count = lax.axis_size(axis)
    up = [(i, i + 1) for i in range(count - 1)]
    return lax.ppermute(value, axis, up if forward else [(j, i) for i, j in up])


def per_device(krylov_basis, schur_vectors, next_vector, diag_shift, velocity):
    axes = (*GX, "gy", "gz")
    cell_count = next_vector.size
    for axis in axes:
        cell_count *= lax.axis_size(axis)
    held, rest, packed = call(
        edge_kernel,
        [krylov_basis.shape, (FIELDS - KEEP, X, Y, Z), (5, Y, Z)],
        [
            pltpu.with_memory_space_constraint(value, pltpu.HBM)
            for value in (krylov_basis, schur_vectors.T, next_vector, diag_shift, velocity)
        ],
        scratch=[
            pltpu.SMEM((KEEP, krylov_basis.shape[0]), F32),
            pltpu.VMEM((4, X, Y, Z), F32),
            pltpu.SemaphoreType.DMA((4 + krylov_basis.shape[0] // CHUNK,)),
        ],
        ins="hhhhh",
        limit=4,
    )
    z_lo, z_hi = send(packed, "gz", True), send(packed, "gz", False)
    (rotated,) = call(
        rotate_kernel,
        [(KEEP, X, Y, Z)],
        [held, schur_vectors.T],
        ins="vs",
        limit=4,
        flops=10**9,
    )
    up, down, halo = call(
        pack_y_kernel, [(27, Y, Z), (27, Y, Z), (5, Y, Z)], [rotated, rest, z_lo, z_hi]
    )
    count = lax.axis_size(GX)
    swap = [(i, i + 1) for i in range(1, count - 1, 2)]
    swap = swap + [(j, i) for i, j in swap]
    y_lo = send(up, "gy", True)
    y_hi = send(down, "gy", False)
    (early,) = call(planes_kernel, [(PLANES, Y, Z)], [rotated, rest])
    early = lax.ppermute(early, GX, swap)
    coef_level, level = call(
        level_kernel,
        [(len(LEVEL), 7, Y, Z), (KEEP, len(LEVEL), Y, Z)],
        [rotated, rest, halo],
        limit=4,
    )
    off, on = call(
        pack_x_kernel, [(61 - PLANES, Y, Z), (61, Y, Z)], [rotated, rest, halo, y_lo, y_hi]
    )
    off = lax.ppermute(off, GX, swap)
    on = lax.ppermute(on, "gx_1", [(0, 1), (1, 0)])
    stages = (("gx_1", "gz"), ("gx_0", "gy"))
    sizes = [lax.axis_size(stage) for stage in stages]
    coef_beside, partial = call(
        inner_kernel,
        [(len(BESIDE), 7, Y, Z), (KEEP, len(ONCE) + 2, Y, Z)],
        [rotated, rest, halo, y_lo, y_hi, coef_level, level],
        scratch=[pltpu.VMEM((5, Y, Z), F32)],
        limit=6,
        flops=10**9,
    )
    span, parts = call(
        functools.partial(stencil_kernel, sizes[0]),
        [(SPAN * X * Y, Z), (sizes[0], 1, WIRE)],
        [rotated, rest, halo, y_lo, y_hi, coef_level, coef_beside, partial, early, off, on],
        scratch=[
            pltpu.VMEM((len(OUTER), 7, Y, Z), F32),
            pltpu.VMEM((5, Y, Z), F32),
            pltpu.VMEM((2, Y, Z), F32),
            pltpu.VMEM((len(region(3)), Y, Z), F32),
            pltpu.VMEM((61, Y, Z), F32),
            pltpu.VMEM((61, Y, Z), F32),
        ],
        limit=8,
    )
    parts = exchange(parts, stages[0])
    (parts,) = call(functools.partial(sum_kernel, sizes[1]), [(sizes[1], 1, WIRE)], [parts])
    parts = exchange(parts, stages[1])
    (half,) = call(functools.partial(sum_kernel, 1), [(1, 1, WIRE)], [parts])
    whole = lax.all_gather(half, "gx_1", axis=0, tiled=True)
    basis, hessenberg = call(
        functools.partial(finish_kernel, cell_count),
        [(ROWS, X, Y, Z), (EXPAND, ROWS)],
        [whole, span.reshape(SPAN, X, Y, Z)],
        scratch=[
            pltpu.VMEM((8 * EXPAND, Y, Z), F32),
            pltpu.VMEM((ROWS - KEEP, X, Y, Z), F32),
            pltpu.SemaphoreType.DMA((1 + ROWS - KEEP,)),
        ],
        out="hv",
        limit=4,
    )
    return basis, hessenberg.T


def solution(mesh):
    split = Mesh(
        mesh.devices.reshape(-1, 2, mesh.shape["gy"], mesh.shape["gz"]),
        ("gx_0", "gx_1", "gy", "gz"),
    )
    return jax.shard_map(
        per_device,
        mesh=split,
        in_specs=(
            P(None, GX, "gy", "gz"),
            P(),
            P(GX, "gy", "gz"),
            P(GX, "gy", "gz"),
            P(None, GX, "gy", "gz"),
        ),
        out_specs=(P(None, GX, "gy", "gz"), P()),
        check_vma=False,
    )
```

```python
import functools

import jax
import jax.numpy as jnp
from jax import lax
from jax.experimental import pallas as pl
from jax.experimental.pallas import tpu as pltpu
from jax.sharding import Mesh
from jax.sharding import PartitionSpec as P

KEEP = 20
EXPAND = 3
ROWS = 24
FIELDS = 25
SPAN = 64
SIGMA = 7.125
PLANES = 51
WIRE = 1280
GX = ("gx_0", "gx_1")
X, Y, Z = (4, 8, 128)
TILE = (Y, Z)
F32 = jnp.float32


def rows_of():
    return lax.broadcasted_iota(jnp.int32, TILE, 0)


def lanes_of():
    return lax.broadcasted_iota(jnp.int32, TILE, 1)


def shift_rows(tile, by):
    by = by % Y
    return tile if by == 0 else pltpu.roll(tile, by, 0)


def shift_lanes(tile, by):
    return pltpu.roll(tile, by, 1)


def place_of(kind):
    return pl.BlockSpec(memory_space={"v": pltpu.VMEM, "s": pltpu.SMEM, "h": pltpu.HBM}[kind])


def call(kernel, outs, args, scratch=(), ins="", out="", flops=100000, limit=2):
    ins, out = ins or "v" * len(args), out or "v" * len(outs)
    return pl.pallas_call(
        kernel,
        out_shape=[jax.ShapeDtypeStruct(s, F32) for s in outs],
        in_specs=[place_of(k) for k in ins],
        out_specs=[place_of(k) for k in out],
        scratch_shapes=list(scratch),
        cost_estimate=pl.CostEstimate(flops=flops, bytes_accessed=100000, transcendentals=0),
        compiler_params=pltpu.CompilerParams(vmem_limit_bytes=limit * 2**20),
    )(*args)


CHUNK = 10


def edge_kernel(
    basis, schur, next_vector, diag, velocity, held, rest, packed, passed, weights, small, sems
):
    chunks = basis.shape[0] // CHUNK
    copies = [
        pltpu.make_async_copy(schur, weights, sems.at[0]),
        *(
            pltpu.make_async_copy(
                basis.at[pl.ds(c * CHUNK, CHUNK)], held.at[pl.ds(c * CHUNK, CHUNK)], sems.at[1 + c]
            )
            for c in range(chunks)
        ),
        pltpu.make_async_copy(next_vector, rest.at[0], sems.at[1 + chunks]),
        pltpu.make_async_copy(diag, small.at[0], sems.at[2 + chunks]),
        pltpu.make_async_copy(velocity, small.at[pl.ds(1, 3)], sems.at[3 + chunks]),
        pltpu.make_async_copy(schur, passed, sems.at[4 + chunks]),
    ]
    for copy in copies[1 + chunks : 4 + chunks]:
        copy.start()
    for copy in copies[: 1 + chunks]:
        copy.start()
    copies[4 + chunks].start()
    lane = lanes_of()
    for copy in copies[1 + chunks : 4 + chunks]:
        copy.wait()
    for x in range(X):
        rest[1, x] = 6.0 + small[0, x]
        for d in range(3):
            rest[2 + d, x] = 0.5 * small[1 + d, x]
    total = jnp.zeros(TILE, F32)
    for j in range(20):
        moved = shift_lanes(rest[j // 4, j % 4], 6 * j + 3)
        total = jnp.where((lane >= 6 * j) & (lane < 6 * j + 6), moved, total)
    packed[4] = total
    copies[0].wait()
    acc = [jnp.zeros(TILE, F32) for _ in range(KEEP)]
    for c in range(chunks):
        copies[1 + c].wait()
        for i in range(c * CHUNK, (c + 1) * CHUNK):
            edge = jnp.zeros(TILE, F32)
            for x in range(X):
                here = (lane >= 6 * x) & (lane < 6 * x + 6)
                edge = jnp.where(here, shift_lanes(held[i, x], 6 * x + 3), edge)
            for f in range(KEEP):
                acc[f] = acc[f] + weights[f, i] * edge
    for p in range(4):
        total = acc[5 * p]
        for q in range(1, 5):
            total = jnp.where(lane < 24 * q, total, shift_lanes(acc[5 * p + q], 24 * q))
        packed[p] = total
    copies[4 + chunks].wait()


def rotate_kernel(basis, schur, rotated):
    group = 5
    for g in range(KEEP // group):

        def body(i, acc, g=g):
            out = []
            tiles = [basis[i, x] for x in range(X)]
            for f in range(group):
                w = schur[g * group + f, i]
                for x in range(X):
                    out.append(acc[f * X + x] + w * tiles[x])
            return tuple(out)

        zero = tuple(jnp.zeros(TILE, F32) for _ in range(group * X))
        acc = lax.fori_loop(0, basis.shape[0], body, zero, unroll=4)
        for f in range(group):
            for x in range(X):
                rotated[g * group + f, x] = acc[f * X + x]


class Fields:
    def __init__(self, rotated, rest):
        self.rotated, self.rest = rotated, rest

    def __getitem__(self, at):
        f, x = at
        if isinstance(f, int) and f >= KEEP:
            return self.rest[f - KEEP, x]
        return self.rotated[f, x]


def pack_y_kernel(rotated, rest, from_lo, from_hi, up, down, halo):
    fields = Fields(rotated, rest)
    row, lane = rows_of(), lanes_of()
    left = lax.rem(lane, 6) < 3
    for f in range(FIELDS):
        a = jnp.zeros(TILE, F32)
        b = a
        for x in range(X):
            tile = fields[f, x]
            here = (row >= 2 * x) & (row < 2 * x + 2)
            a = jnp.where(here, shift_rows(tile, 2 * x - 6), a)
            b = jnp.where(here, shift_rows(tile, 2 * x), b)
        up[f] = a
        down[f] = b
    a = jnp.zeros(TILE, F32)
    b = a
    for x in range(X):
        tile = fields[20, x]
        a = jnp.where(row == x, shift_rows(tile, x - 5), a)
        b = jnp.where(row == x, shift_rows(tile, x - 2), b)
    up[25] = a
    down[25] = b
    a = jnp.zeros(TILE, F32)
    b = a
    for p in range(5):
        merged = jnp.where(left, from_lo[p], from_hi[p])
        halo[p] = merged
        a = jnp.where(row == p, shift_rows(merged, p - 7), a)
        b = jnp.where(row == p, shift_rows(merged, p), b)
    up[26] = jnp.where(row == 5, shift_rows(merged, -1), a)
    down[26] = jnp.where(row == 5, shift_rows(merged, 4), b)


def corner_of(p, y_lo, y_hi):
    row = rows_of()
    lo, hi = y_lo[26], y_hi[26]
    tile = jnp.where(row == 0, shift_rows(hi, -p), jnp.zeros(TILE, F32))
    tile = jnp.where(row == 7, shift_rows(lo, 7 - p), tile)
    if p == 4:
        tile = jnp.where(row == 1, shift_rows(hi, -4), tile)
        tile = jnp.where(row == 6, shift_rows(lo, 1), tile)
    return tile


def planes_kernel(rotated, rest, early):
    fields = Fields(rotated, rest)
    upper = lax.axis_index("gx_1") == 1
    for f in range(FIELDS):
        early[2 * f] = jnp.where(upper, fields[f, 2], fields[f, 0])
        early[2 * f + 1] = jnp.where(upper, fields[f, 3], fields[f, 1])
    early[PLANES - 1] = jnp.where(upper, fields[20, 1], fields[20, 2])


def pack_x_kernel(rotated, rest, halo, y_lo, y_hi, off, on):
    fields = Fields(rotated, rest)
    first, row = rows_of() < 4, rows_of()
    upper = lax.axis_index("gx_1") == 1

    def put(at, up, down):
        if at >= PLANES:
            off[at - PLANES] = jnp.where(upper, up, down)
        on[at] = jnp.where(upper, down, up)

    for f in range(FIELDS):
        put(2 * f, fields[f, 2], fields[f, 0])
        put(2 * f + 1, fields[f, 3], fields[f, 1])
    put(50, fields[20, 1], fields[20, 2])
    lo, hi = y_lo[20], y_hi[20]
    put(51, jnp.where(first, shift_rows(lo, 4), hi), jnp.where(first, lo, shift_rows(hi, 4)))
    for v in range(6):
        a = jnp.zeros(TILE, F32)
        b = a
        for k in range(4):
            f = 4 * v + k + (1 if v == 5 else 0)
            lo, hi = y_lo[f], y_hi[f]
            a = jnp.where(row == 2 * k, shift_rows(lo, 2 * k - 7), a)
            a = jnp.where(row == 2 * k + 1, shift_rows(hi, 2 * k - 5), a)
            b = jnp.where(row == 2 * k, shift_rows(lo, 2 * k - 1), b)
            b = jnp.where(row == 2 * k + 1, shift_rows(hi, 2 * k + 1), b)
        put(52 + v, a, b)
    part = lax.rem(lanes_of(), 24)
    a = jnp.zeros(TILE, F32)
    b = a
    for p in range(4):
        tile = halo[p]
        here = (part >= 18 - 6 * p) & (part < 24 - 6 * p)
        a = jnp.where(here, shift_lanes(tile, -6 * p % Z) if p else tile, a)
        here = (part >= 6 * p) & (part < 6 * p + 6)
        b = jnp.where(here, shift_lanes(tile, 6 * p) if p else tile, b)
    put(58, a, b)
    corner = corner_of(4, y_lo, y_hi)
    put(59, halo[4], halo[4])
    put(60, corner, corner)


def region(radius):
    out = []
    for a, b in ((0, 0), (1, 0), (0, 1), (1, 1)):
        reach = radius - a - b
        if reach >= 0:
            out.extend((x, a, b) for x in range(-reach, X + reach))
    return out


COEF = region(2)


def tile_of(f, key, refs):
    fields, halo, y_lo, y_hi, x_lo, x_hi, y_halo, x_corner = refs
    x, a, b = key
    first = rows_of() < 4
    if b == 0:
        if a == 0:
            if 0 <= x < X:
                return fields[f, x]
            if x == -3:
                return x_lo[50]
            if x == 6:
                return x_hi[50]
            return x_lo[2 * f + x + 2] if x < 0 else x_hi[2 * f + x - 4]
        if 0 <= x < X:
            lo, hi = y_lo[f], y_hi[f]
            tile = jnp.where(first, shift_rows(hi, -2 * x), shift_rows(lo, 6 - 2 * x))
            if isinstance(f, int) and f == 20:
                row = rows_of()
                tile = jnp.where(row == 2, shift_rows(y_hi[25], 2 - x), tile)
                tile = jnp.where(row == 5, shift_rows(y_lo[25], 5 - x), tile)
            return tile
        side = x_lo if x < 0 else x_hi
        if not (isinstance(f, int) and f == 20):
            g = f - 1 if isinstance(f, int) and f > 20 else f
            v, k = (g // 4, g % 4) if isinstance(g, int) else (lax.div(g, 4), lax.rem(g, 4))
            return pltpu.roll(side[52 + v], 7 - 2 * k, 0)
        packed = side[51]
        if x in (-1, 5):
            return jnp.where(first, shift_rows(packed, 2), shift_rows(packed, 4))
        return jnp.where(first, shift_rows(packed, 4), shift_rows(packed, 6))
    p, q = (f // 5, f % 5) if isinstance(f, int) else (lax.div(f, 5), lax.rem(f, 5))
    place = x if 0 <= x < X else (x + X if x < 0 else x - X)
    by = 128 - 3 - 6 * (4 * q + place)
    if a == 0 and not 0 <= x < X and not (isinstance(f, int) and f >= KEEP):
        packed = (x_lo if x < 0 else x_hi)[58]
        by = 128 - 3 - 24 * q - (18 - 6 * p if x < 0 else 6 * p)
    elif a == 0:
        packed = halo[p] if 0 <= x < X else (x_lo if x < 0 else x_hi)[59]
    elif 0 <= x < X:
        packed = y_halo[p]
    else:
        packed = x_corner[0 if x < 0 else 1]
    return shift_lanes(packed, by)


def along_y(get, key, coef):
    x, a, b = key
    row = rows_of()
    centre, other = get(key), get((x, 1 - a, b))
    ahead = shift_rows(jnp.where(row == 0, other, centre), 7)
    behind = shift_rows(jnp.where(row == 7, other, centre), 1)
    return coef(key, 3) * ahead + coef(key, 4) * behind


def apply(get, key, coef, skip=(), with_y=True):
    x, a, b = key
    lane = lanes_of()
    centre, other = get(key), get((x, a, 1 - b))
    ahead = shift_lanes(jnp.where(lane == 0, other, centre), 127)
    behind = shift_lanes(jnp.where(lane == 127, other, centre), 1)
    total = coef(key, 5) * ahead + coef(key, 6) * behind
    if with_y:
        total = along_y(get, key, coef) + total
    total = total + coef(key, 0) * centre
    for i, at in ((1, (x + 1, a, b)), (2, (x - 1, a, b))):
        if i not in skip:
            total = total + coef(key, i) * get(at)
    return total


def fill_coefficients(keys, out, refs):
    for at, key in enumerate(keys):
        diagonal = tile_of(21, key, refs)
        inside = diagonal != 0.0
        out[at, 0] = jnp.where(inside, diagonal - SIGMA, 0.0)
        for d in range(3):
            half = tile_of(22 + d, key, refs)
            out[at, 1 + 2 * d] = jnp.where(inside, half - 1.0, 0.0)
            out[at, 2 + 2 * d] = jnp.where(inside, -1.0 - half, 0.0)


def cached(f, refs):
    held = {}

    def get(key):
        if key not in held:
            held[key] = tile_of(f, key, refs)
        return held[key]

    return get


INNER = [key for key in COEF if 0 <= key[0] < X]
LEVEL = [key for key in INNER if not key[1]]
BESIDE = [key for key in INNER if key[1]]
OUTER = [key for key in COEF if not 0 <= key[0] < X]
ONCE = [key for key in region(1) if 0 <= key[0] < X]
SIDES = {0: (2, -1), X - 1: (1, X)}


def skip_of(key):
    return (SIDES[key[0]][0],) if key[0] in SIDES else ()


def level_kernel(rotated, rest, halo, coef_level, partial):
    refs = (Fields(rotated, rest), halo, None, None, None, None, None, None)
    fill_coefficients(LEVEL, coef_level, refs)
    coef = lambda key, i: coef_level[LEVEL.index(key), i]

    def body(f, carry):
        get = cached(f, refs)
        for at, key in enumerate(LEVEL):
            partial[f, at] = apply(get, key, coef, skip_of(key), with_y=False)
        return carry

    lax.fori_loop(0, KEEP, body, 0, unroll=4)


def inner_kernel(
    rotated, rest, halo, y_lo, y_hi, coef_level, level, coef_beside, partial, y_halo
):
    for p in range(5):
        y_halo[p] = corner_of(p, y_lo, y_hi)
    refs = (Fields(rotated, rest), halo, y_lo, y_hi, None, None, y_halo, None)
    fill_coefficients(BESIDE, coef_beside, refs)

    def coef(key, i):
        if key in LEVEL:
            return coef_level[LEVEL.index(key), i]
        return coef_beside[BESIDE.index(key), i]

    def body(f, carry):
        get = cached(f, refs)
        once = {}
        for at, key in enumerate(ONCE):
            if key in LEVEL:
                once[key] = level[f, LEVEL.index(key)] + along_y(get, key, coef)
            else:
                once[key] = apply(get, key, coef, skip_of(key))
            partial[f, at] = once[key]
        for x, skip in ((1, (2,)), (2, (1,))):
            partial[f, len(ONCE) + x - 1] = apply(once.__getitem__, (x, 0, 0), coef, skip)
        return carry

    lax.fori_loop(0, KEEP, body, 0, unroll=4)


def inner(a, b):
    return lax.dot_general(a, b, (((1,), (1,)), ((), ())), preferred_element_type=F32)


def stencil_kernel(
    copies,
    rotated,
    rest,
    halo,
    y_lo,
    y_hi,
    coef_level,
    coef_beside,
    partial,
    early,
    off,
    on,
    span,
    gram,
    coef_out,
    y_halo,
    x_corner,
    chain,
    x_lo,
    x_hi,
):
    fields = Fields(rotated, rest)
    upper = lax.axis_index("gx_1") == 1
    for i in range(on.shape[0]):
        far = early[i] if i < PLANES else off[i - PLANES]
        x_lo[i] = jnp.where(upper, on[i], far)
        x_hi[i] = jnp.where(upper, far, on[i])
    refs = (fields, halo, y_lo, y_hi, x_lo, x_hi, y_halo, x_corner)
    for p in range(5):
        y_halo[p] = corner_of(p, y_lo, y_hi)
    x_corner[0] = x_lo[60]
    x_corner[1] = x_hi[60]
    fill_coefficients(OUTER, coef_out, refs)

    def coef(key, i):
        if key in LEVEL:
            return coef_level[LEVEL.index(key), i]
        if key in BESIDE:
            return coef_beside[BESIDE.index(key), i]
        return coef_out[OUTER.index(key), i]

    def store(f, x, tile):
        at = f * (X * Y) + x * Y
        if not isinstance(f, int):
            at = pl.multiple_of(at, Y)
        span[pl.ds(at, Y), :] = tile

    tiles = {key: tile_of(20, key, refs) for key in region(3)}
    for x in range(X):
        store(60, x, tiles[(x, 0, 0)])
    for step in range(EXPAND):
        place = {}
        for at, key in enumerate(tiles):
            chain[at] = tiles[key]
            place[key] = at
        get = lambda key, place=place: chain[place[key]]
        tiles = {key: apply(get, key, coef) for key in region(2 - step)}
        for x in range(X):
            store(61 + step, x, tiles[(x, 0, 0)])

    def body(f, carry):
        get = cached(f, refs)
        once = {}
        for at, key in enumerate(ONCE):
            x, a, b = key
            if x not in SIDES and (a or b):
                continue
            tile = partial[f, at]
            if x in SIDES:
                i, side = SIDES[x]
                tile = tile + coef(key, i) * get((side, a, b))
            once[key] = tile
        for x in (-1, X):
            once[(x, 0, 0)] = apply(get, (x, 0, 0), coef)
        for x in range(X):
            store(f, x, get((x, 0, 0)))
            store(f + 20, x, once[(x, 0, 0)])
        for x in SIDES:
            store(f + 40, x, apply(once.__getitem__, (x, 0, 0), coef))
        for x, i, near in ((1, 2, 0), (2, 1, 3)):
            term = coef((x, 0, 0), i) * once[(near, 0, 0)]
            store(f + 40, x, partial[f, len(ONCE) + x - 1] + term)
        return carry

    lax.fori_loop(0, KEEP, body, 0, unroll=5)

    even = jnp.zeros((SPAN, SPAN), F32)
    mixed = even
    for r in range(0, X * Y, 2):
        pair = [span[pl.ds(r + i, SPAN, stride=X * Y), :] for i in range(2)]
        rows = jnp.concatenate(pair, axis=1)
        high = rows.astype(jnp.bfloat16)
        left = rows - high.astype(F32)
        middle = left.astype(jnp.bfloat16)
        low = (left - middle.astype(F32)).astype(jnp.bfloat16)
        even = even + (inner(high, high) + inner(middle, middle))
        mixed = mixed + (inner(high, middle) + inner(high, low))
    square = jnp.concatenate([mixed, jnp.zeros((SPAN, Z - SPAN), F32)], axis=1)
    square = jnp.concatenate([square, jnp.zeros((Z - SPAN, Z), F32)], axis=0)
    total = even + (mixed + square.T[:SPAN, :SPAN])
    wide = jnp.concatenate([total, jnp.zeros((SPAN, Z - SPAN), F32)], axis=1)
    lane = lax.broadcasted_iota(jnp.int32, (16, Z), 1)
    main = jnp.where(
        lane < 64,
        wide[:16],
        jnp.where(lane < 112, pltpu.roll(wide[16:32], 48, 1), pltpu.roll(wide[48:], 64, 1)),
    )
    lane = lanes_of()
    extra = jnp.zeros(TILE, F32)
    for g in range(4):
        tile = shift_rows(wide[32 + 8 * (g // 2) : 40 + 8 * (g // 2)], -4 * (g % 2))
        tile = tile if g == 1 else shift_lanes(tile, (32 * g - 32) % Z)
        extra = jnp.where((lane >= 32 * g) & (lane < 32 * g + 32), tile, extra)
    for i in range(copies):
        c = i // (copies // 2)
        for k in range(8):
            gram[i, :, Z * k : Z * (k + 1)] = main[8 * c + k : 8 * c + k + 1]
        for k in range(2):
            gram[i, :, Z * (8 + k) : Z * (9 + k)] = extra[2 * c + k : 2 * c + k + 1]


def sum_kernel(copies, parts, out):
    total = parts[0]
    for i in range(1, parts.shape[0]):
        total = total + parts[i]
    for i in range(copies):
        out[i] = total


def exchange(parts, axis):
    return lax.all_to_all(parts, axis, 0, 0)


def finish_kernel(cell_count, parts, span, basis, hessenberg, spread, fresh, sems):
    early = pltpu.make_async_copy(
        span.at[pl.ds(0, KEEP)], basis.at[pl.ds(0, KEEP)], sems.at[0]
    )
    early.start()
    late = [
        pltpu.make_async_copy(fresh.at[k], basis.at[KEEP + k], sems.at[1 + k])
        for k in range(ROWS - KEEP)
    ]
    row = lax.broadcasted_iota(jnp.int32, (16, Z), 0)
    lane = lax.broadcasted_iota(jnp.int32, (16, Z), 1)
    main = jnp.zeros((16, Z), F32)
    extra = jnp.zeros(TILE, F32)
    for c in range(2):
        for k in range(8):
            main = jnp.where(row == 8 * c + k, parts[c, :, Z * k : Z * (k + 1)], main)
        for k in range(2):
            here = rows_of() == 2 * c + k
            extra = jnp.where(here, parts[c, :, Z * (8 + k) : Z * (9 + k)], extra)
    main, extra = main * (1.0 / cell_count), extra * (1.0 / cell_count)
    upper = []
    for g in (0, 2):
        tile = jnp.where(
            rows_of() < 4,
            shift_lanes(extra, (32 - 32 * g) % Z),
            shift_lanes(shift_rows(extra, 4), -32 * g % Z) if g else shift_rows(extra, 4),
        )
        upper.append(jnp.where((lanes_of() >= 32) & (lanes_of() < SPAN), tile, 0.0))
    blocks = jnp.concatenate(
        [
            jnp.where(lane < SPAN, main, 0.0),
            jnp.where((lane >= 16) & (lane < SPAN), pltpu.roll(main, Z - 48, 1), 0.0),
            *upper,
            jnp.where((lane >= 48) & (lane < SPAN), pltpu.roll(main, 64, 1), 0.0),
            jnp.zeros((Z - SPAN, Z), F32),
        ],
        axis=0,
    )
    across = lax.broadcasted_iota(jnp.int32, (Z, Z), 1) // 16
    down = lax.broadcasted_iota(jnp.int32, (Z, Z), 0) // 16
    gram = (blocks + jnp.where(across < down, blocks.T, 0.0))[:SPAN]
    row64 = lax.broadcasted_iota(jnp.int32, (SPAN, Z), 0)
    lane64 = lax.broadcasted_iota(jnp.int32, (SPAN, Z), 1)
    eye = row64 == lane64
    moved = ((row64 >= KEEP) & (row64 < 60) & (lane64 == row64 - KEEP)) | (
        (row64 > 60) & (lane64 == row64 - 1)
    )
    row = lax.broadcasted_iota(jnp.int32, (ROWS, Z), 0)
    lane = lax.broadcasted_iota(jnp.int32, (ROWS, Z), 1)
    lane1 = lax.broadcasted_iota(jnp.int32, (1, Z), 1)

    def column(vector, picks):
        return jnp.sum(jnp.where(picks, vector, 0.0), axis=1, keepdims=True)

    first_row = gram[60:61, :]
    norm_sq = jnp.sum(jnp.where(lane1 == 60, first_row, 0.0), axis=1, keepdims=True)
    inverse = lax.rsqrt(jnp.maximum(norm_sq, 0.25))
    last = jnp.where(lane1 == 60, inverse, 0.0)
    last_gram = first_row * inverse
    up_column = jnp.where(lax.broadcasted_iota(jnp.int32, (SPAN, 1), 0) == 61, inverse, 0.0)
    q = jnp.where((row == lane) & (row < KEEP), 1.0, 0.0)
    q = jnp.where(row == KEEP, last, q)
    qg = jnp.where(row < KEEP, gram[:ROWS, :], 0.0)
    qg = jnp.where(row == KEEP, last_gram, qg)
    scale = jnp.broadcast_to(inverse, TILE)
    for x in range(X):
        fresh[0, x] = span[60, x] * scale
    late[0].start()
    for k in range(EXPAND):
        up = jnp.where(
            (lane1 >= KEEP) & (lane1 < 60),
            pltpu.roll(last, KEEP, 1),
            jnp.where((lane1 > 60) & (lane1 < SPAN), pltpu.roll(last, 1, 1), 0.0),
        )
        image = up + SIGMA * last
        image_gram = jnp.sum(up_column * gram, axis=0, keepdims=True) + SIGMA * last_gram
        c = jnp.sum(q * image_gram, axis=1, keepdims=True)
        partly = image - jnp.sum(c * q, axis=0, keepdims=True)
        partly_gram = image_gram - jnp.sum(c * qg, axis=0, keepdims=True)
        e = jnp.sum(q * partly_gram, axis=1, keepdims=True)
        cleaned = partly - jnp.sum(e * q, axis=0, keepdims=True)
        cleaned_gram = partly_gram - jnp.sum(e * qg, axis=0, keepdims=True)
        length_sq = jnp.sum(cleaned * cleaned_gram, axis=1, keepdims=True)
        here, shifted = column(cleaned, eye), column(cleaned, moved)
        inverse = lax.rsqrt(jnp.maximum(length_sq, 0.25))
        last = cleaned * inverse
        last_gram = cleaned_gram * inverse
        up_column = shifted * inverse
        q = jnp.where(row == KEEP + 1 + k, last, q)
        qg = jnp.where(row == KEEP + 1 + k, last_gram, qg)
        length = jnp.sqrt(jnp.maximum(length_sq, 0.0))
        entries = jnp.where(row == KEEP + 1 + k, length, c + e)
        turned = jnp.sum(jnp.where(row == lane, entries, 0.0), axis=0, keepdims=True)
        hessenberg[k : k + 1, :] = turned[:, :ROWS]
        spread[pl.ds(8 * k, 8)] = jnp.broadcast_to(here * inverse, (SPAN, Z)).reshape(8, 8, Z)
        fields = [*range(KEEP * (k + 1)), *range(60, 62 + k)]
        acc = [jnp.zeros(TILE, F32) for _ in range(X)]
        for f in fields:
            w = spread[8 * k + f // 8, f % 8 : f % 8 + 1, :]
            for x in range(X):
                acc[x] = acc[x] + w * span[f, x]
        for x in range(X):
            fresh[1 + k, x] = acc[x]
        late[1 + k].start()
    early.wait()
    for copy in late:
        copy.wait()


def send(value, axis, forward):
    count = lax.axis_size(axis)
    up = [(i, i + 1) for i in range(count - 1)]
    return lax.ppermute(value, axis, up if forward else [(j, i) for i, j in up])


def per_device(krylov_basis, schur_vectors, next_vector, diag_shift, velocity):
    axes = (*GX, "gy", "gz")
    cell_count = next_vector.size
    for axis in axes:
        cell_count *= lax.axis_size(axis)
    held, rest, packed, passed = call(
        edge_kernel,
        [
            krylov_basis.shape,
            (FIELDS - KEEP, X, Y, Z),
            (5, Y, Z),
            (KEEP, krylov_basis.shape[0]),
        ],
        [
            pltpu.with_memory_space_constraint(value, pltpu.HBM)
            for value in (krylov_basis, schur_vectors.T, next_vector, diag_shift, velocity)
        ],
        scratch=[
            pltpu.SMEM((KEEP, krylov_basis.shape[0]), F32),
            pltpu.VMEM((4, X, Y, Z), F32),
            pltpu.SemaphoreType.DMA((5 + krylov_basis.shape[0] // CHUNK,)),
        ],
        ins="hhhhh",
        limit=4,
    )
    z_lo, z_hi = send(packed, "gz", True), send(packed, "gz", False)
    (rotated,) = call(
        rotate_kernel,
        [(KEEP, X, Y, Z)],
        [held, passed],
        ins="vs",
        limit=4,
        flops=10**9,
    )
    up, down, halo = call(
        pack_y_kernel, [(27, Y, Z), (27, Y, Z), (5, Y, Z)], [rotated, rest, z_lo, z_hi]
    )
    count = lax.axis_size(GX)
    swap = [(i, i + 1) for i in range(1, count - 1, 2)]
    swap = swap + [(j, i) for i, j in swap]
    y_lo = send(up, "gy", True)
    y_hi = send(down, "gy", False)
    (early,) = call(planes_kernel, [(PLANES, Y, Z)], [rotated, rest])
    early = lax.ppermute(early, GX, swap)
    coef_level, level = call(
        level_kernel,
        [(len(LEVEL), 7, Y, Z), (KEEP, len(LEVEL), Y, Z)],
        [rotated, rest, halo],
        limit=4,
    )
    off, on = call(
        pack_x_kernel, [(61 - PLANES, Y, Z), (61, Y, Z)], [rotated, rest, halo, y_lo, y_hi]
    )
    off = lax.ppermute(off, GX, swap)
    on = lax.ppermute(on, "gx_1", [(0, 1), (1, 0)])
    stages = (("gx_1", "gz"), ("gx_0", "gy"))
    sizes = [lax.axis_size(stage) for stage in stages]
    coef_beside, partial = call(
        inner_kernel,
        [(len(BESIDE), 7, Y, Z), (KEEP, len(ONCE) + 2, Y, Z)],
        [rotated, rest, halo, y_lo, y_hi, coef_level, level],
        scratch=[pltpu.VMEM((5, Y, Z), F32)],
        limit=6,
        flops=10**9,
    )
    span, parts = call(
        functools.partial(stencil_kernel, sizes[0]),
        [(SPAN * X * Y, Z), (sizes[0], 1, WIRE)],
        [rotated, rest, halo, y_lo, y_hi, coef_level, coef_beside, partial, early, off, on],
        scratch=[
            pltpu.VMEM((len(OUTER), 7, Y, Z), F32),
            pltpu.VMEM((5, Y, Z), F32),
            pltpu.VMEM((2, Y, Z), F32),
            pltpu.VMEM((len(region(3)), Y, Z), F32),
            pltpu.VMEM((61, Y, Z), F32),
            pltpu.VMEM((61, Y, Z), F32),
        ],
        limit=8,
    )
    parts = exchange(parts, stages[0])
    (parts,) = call(functools.partial(sum_kernel, sizes[1]), [(sizes[1], 1, WIRE)], [parts])
    parts = exchange(parts, stages[1])
    (half,) = call(functools.partial(sum_kernel, 1), [(1, 1, WIRE)], [parts])
    whole = lax.all_gather(half, "gx_1", axis=0, tiled=True)
    basis, hessenberg = call(
        functools.partial(finish_kernel, cell_count),
        [(ROWS, X, Y, Z), (EXPAND, ROWS)],
        [whole, span.reshape(SPAN, X, Y, Z)],
        scratch=[
            pltpu.VMEM((8 * EXPAND, Y, Z), F32),
            pltpu.VMEM((ROWS - KEEP, X, Y, Z), F32),
            pltpu.SemaphoreType.DMA((1 + ROWS - KEEP,)),
        ],
        out="hv",
        limit=4,
    )
    return basis, hessenberg.T


def solution(mesh):
    split = Mesh(
        mesh.devices.reshape(-1, 2, mesh.shape["gy"], mesh.shape["gz"]),
        ("gx_0", "gx_1", "gy", "gz"),
    )
    return jax.shard_map(
        per_device,
        mesh=split,
        in_specs=(
            P(None, GX, "gy", "gz"),
            P(),
            P(GX, "gy", "gz"),
            P(GX, "gy", "gz"),
            P(None, GX, "gy", "gz"),
        ),
        out_specs=(P(None, GX, "gy", "gz"), P()),
        check_vma=False,
    )
```

```python
import functools

import jax
import jax.numpy as jnp
from jax import lax
from jax.experimental import pallas as pl
from jax.experimental.pallas import tpu as pltpu
from jax.sharding import Mesh
from jax.sharding import PartitionSpec as P

KEEP = 20
EXPAND = 3
ROWS = 24
FIELDS = 25
SPAN = 64
SIGMA = 7.125
PLANES = 51
WIRE = 1152
GX = ("gx_0", "gx_1")
X, Y, Z = (4, 8, 128)
TILE = (Y, Z)
F32 = jnp.float32


def rows_of():
    return lax.broadcasted_iota(jnp.int32, TILE, 0)


def lanes_of():
    return lax.broadcasted_iota(jnp.int32, TILE, 1)


def shift_rows(tile, by):
    by = by % Y
    return tile if by == 0 else pltpu.roll(tile, by, 0)


def shift_lanes(tile, by):
    return pltpu.roll(tile, by, 1)


def place_of(kind):
    return pl.BlockSpec(memory_space={"v": pltpu.VMEM, "s": pltpu.SMEM, "h": pltpu.HBM}[kind])


def call(kernel, outs, args, scratch=(), ins="", out="", flops=100000, limit=2):
    ins, out = ins or "v" * len(args), out or "v" * len(outs)
    return pl.pallas_call(
        kernel,
        out_shape=[jax.ShapeDtypeStruct(s, F32) for s in outs],
        in_specs=[place_of(k) for k in ins],
        out_specs=[place_of(k) for k in out],
        scratch_shapes=list(scratch),
        cost_estimate=pl.CostEstimate(flops=flops, bytes_accessed=100000, transcendentals=0),
        compiler_params=pltpu.CompilerParams(vmem_limit_bytes=limit * 2**20),
    )(*args)


CHUNK = 10


def edge_kernel(
    basis, schur, next_vector, diag, velocity, held, rest, packed, passed, weights, small, sems
):
    chunks = basis.shape[0] // CHUNK
    copies = [
        pltpu.make_async_copy(schur, weights, sems.at[0]),
        *(
            pltpu.make_async_copy(
                basis.at[pl.ds(c * CHUNK, CHUNK)], held.at[pl.ds(c * CHUNK, CHUNK)], sems.at[1 + c]
            )
            for c in range(chunks)
        ),
        pltpu.make_async_copy(next_vector, rest.at[0], sems.at[1 + chunks]),
        pltpu.make_async_copy(diag, small.at[0], sems.at[2 + chunks]),
        pltpu.make_async_copy(velocity, small.at[pl.ds(1, 3)], sems.at[3 + chunks]),
        pltpu.make_async_copy(schur, passed, sems.at[4 + chunks]),
    ]
    for copy in copies[1 + chunks : 4 + chunks]:
        copy.start()
    for copy in copies[: 1 + chunks]:
        copy.start()
    copies[4 + chunks].start()
    lane = lanes_of()
    for copy in copies[1 + chunks : 4 + chunks]:
        copy.wait()
    for x in range(X):
        rest[1, x] = 6.0 + small[0, x]
        for d in range(3):
            rest[2 + d, x] = 0.5 * small[1 + d, x]
    total = jnp.zeros(TILE, F32)
    for j in range(20):
        moved = shift_lanes(rest[j // 4, j % 4], 6 * j + 3)
        total = jnp.where((lane >= 6 * j) & (lane < 6 * j + 6), moved, total)
    packed[4] = total
    copies[0].wait()
    acc = [jnp.zeros(TILE, F32) for _ in range(KEEP)]
    for c in range(chunks):
        copies[1 + c].wait()
        for i in range(c * CHUNK, (c + 1) * CHUNK):
            edge = jnp.zeros(TILE, F32)
            for x in range(X):
                here = (lane >= 6 * x) & (lane < 6 * x + 6)
                edge = jnp.where(here, shift_lanes(held[i, x], 6 * x + 3), edge)
            for f in range(KEEP):
                acc[f] = acc[f] + weights[f, i] * edge
    for p in range(4):
        total = acc[5 * p]
        for q in range(1, 5):
            total = jnp.where(lane < 24 * q, total, shift_lanes(acc[5 * p + q], 24 * q))
        packed[p] = total
    copies[4 + chunks].wait()


def rotate_kernel(basis, schur, rotated):
    group = 5
    for g in range(KEEP // group):

        def body(i, acc, g=g):
            out = []
            tiles = [basis[i, x] for x in range(X)]
            for f in range(group):
                w = schur[g * group + f, i]
                for x in range(X):
                    out.append(acc[f * X + x] + w * tiles[x])
            return tuple(out)

        zero = tuple(jnp.zeros(TILE, F32) for _ in range(group * X))
        acc = lax.fori_loop(0, basis.shape[0], body, zero, unroll=4)
        for f in range(group):
            for x in range(X):
                rotated[g * group + f, x] = acc[f * X + x]


class Fields:
    def __init__(self, rotated, rest):
        self.rotated, self.rest = rotated, rest

    def __getitem__(self, at):
        f, x = at
        if isinstance(f, int) and f >= KEEP:
            return self.rest[f - KEEP, x]
        return self.rotated[f, x]


def pack_y_kernel(rotated, rest, from_lo, from_hi, up, down, halo):
    fields = Fields(rotated, rest)
    row, lane = rows_of(), lanes_of()
    left = lax.rem(lane, 6) < 3
    for f in range(FIELDS):
        a = jnp.zeros(TILE, F32)
        b = a
        for x in range(X):
            tile = fields[f, x]
            here = (row >= 2 * x) & (row < 2 * x + 2)
            a = jnp.where(here, shift_rows(tile, 2 * x - 6), a)
            b = jnp.where(here, shift_rows(tile, 2 * x), b)
        up[f] = a
        down[f] = b
    a = jnp.zeros(TILE, F32)
    b = a
    for x in range(X):
        tile = fields[20, x]
        a = jnp.where(row == x, shift_rows(tile, x - 5), a)
        b = jnp.where(row == x, shift_rows(tile, x - 2), b)
    up[25] = a
    down[25] = b
    a = jnp.zeros(TILE, F32)
    b = a
    for p in range(5):
        merged = jnp.where(left, from_lo[p], from_hi[p])
        halo[p] = merged
        a = jnp.where(row == p, shift_rows(merged, p - 7), a)
        b = jnp.where(row == p, shift_rows(merged, p), b)
    up[26] = jnp.where(row == 5, shift_rows(merged, -1), a)
    down[26] = jnp.where(row == 5, shift_rows(merged, 4), b)


def corner_of(p, y_lo, y_hi):
    row = rows_of()
    lo, hi = y_lo[26], y_hi[26]
    tile = jnp.where(row == 0, shift_rows(hi, -p), jnp.zeros(TILE, F32))
    tile = jnp.where(row == 7, shift_rows(lo, 7 - p), tile)
    if p == 4:
        tile = jnp.where(row == 1, shift_rows(hi, -4), tile)
        tile = jnp.where(row == 6, shift_rows(lo, 1), tile)
    return tile


def planes_kernel(rotated, rest, early):
    fields = Fields(rotated, rest)
    upper = lax.axis_index("gx_1") == 1
    for f in range(FIELDS):
        early[2 * f] = jnp.where(upper, fields[f, 2], fields[f, 0])
        early[2 * f + 1] = jnp.where(upper, fields[f, 3], fields[f, 1])
    early[PLANES - 1] = jnp.where(upper, fields[20, 1], fields[20, 2])


def pack_x_kernel(rotated, rest, halo, y_lo, y_hi, off, on):
    fields = Fields(rotated, rest)
    first, row = rows_of() < 4, rows_of()
    upper = lax.axis_index("gx_1") == 1

    def put(at, up, down):
        if at >= PLANES:
            off[at - PLANES] = jnp.where(upper, up, down)
        on[at] = jnp.where(upper, down, up)

    for f in range(FIELDS):
        put(2 * f, fields[f, 2], fields[f, 0])
        put(2 * f + 1, fields[f, 3], fields[f, 1])
    put(50, fields[20, 1], fields[20, 2])
    lo, hi = y_lo[20], y_hi[20]
    put(51, jnp.where(first, shift_rows(lo, 4), hi), jnp.where(first, lo, shift_rows(hi, 4)))
    for v in range(6):
        a = jnp.zeros(TILE, F32)
        b = a
        for k in range(4):
            f = 4 * v + k + (1 if v == 5 else 0)
            lo, hi = y_lo[f], y_hi[f]
            a = jnp.where(row == 2 * k, shift_rows(lo, 2 * k - 7), a)
            a = jnp.where(row == 2 * k + 1, shift_rows(hi, 2 * k - 5), a)
            b = jnp.where(row == 2 * k, shift_rows(lo, 2 * k - 1), b)
            b = jnp.where(row == 2 * k + 1, shift_rows(hi, 2 * k + 1), b)
        put(52 + v, a, b)
    part = lax.rem(lanes_of(), 24)
    a = jnp.zeros(TILE, F32)
    b = a
    for p in range(4):
        tile = halo[p]
        here = (part >= 18 - 6 * p) & (part < 24 - 6 * p)
        a = jnp.where(here, shift_lanes(tile, -6 * p % Z) if p else tile, a)
        here = (part >= 6 * p) & (part < 6 * p + 6)
        b = jnp.where(here, shift_lanes(tile, 6 * p) if p else tile, b)
    put(58, a, b)
    corner = corner_of(4, y_lo, y_hi)
    put(59, halo[4], halo[4])
    put(60, corner, corner)


def region(radius):
    out = []
    for a, b in ((0, 0), (1, 0), (0, 1), (1, 1)):
        reach = radius - a - b
        if reach >= 0:
            out.extend((x, a, b) for x in range(-reach, X + reach))
    return out


COEF = region(2)


def tile_of(f, key, refs):
    fields, halo, y_lo, y_hi, x_lo, x_hi, y_halo, x_corner = refs
    x, a, b = key
    first = rows_of() < 4
    if b == 0:
        if a == 0:
            if 0 <= x < X:
                return fields[f, x]
            if x == -3:
                return x_lo[50]
            if x == 6:
                return x_hi[50]
            return x_lo[2 * f + x + 2] if x < 0 else x_hi[2 * f + x - 4]
        if 0 <= x < X:
            lo, hi = y_lo[f], y_hi[f]
            tile = jnp.where(first, shift_rows(hi, -2 * x), shift_rows(lo, 6 - 2 * x))
            if isinstance(f, int) and f == 20:
                row = rows_of()
                tile = jnp.where(row == 2, shift_rows(y_hi[25], 2 - x), tile)
                tile = jnp.where(row == 5, shift_rows(y_lo[25], 5 - x), tile)
            return tile
        side = x_lo if x < 0 else x_hi
        if not (isinstance(f, int) and f == 20):
            g = f - 1 if isinstance(f, int) and f > 20 else f
            v, k = (g // 4, g % 4) if isinstance(g, int) else (lax.div(g, 4), lax.rem(g, 4))
            return pltpu.roll(side[52 + v], 7 - 2 * k, 0)
        packed = side[51]
        if x in (-1, 5):
            return jnp.where(first, shift_rows(packed, 2), shift_rows(packed, 4))
        return jnp.where(first, shift_rows(packed, 4), shift_rows(packed, 6))
    p, q = (f // 5, f % 5) if isinstance(f, int) else (lax.div(f, 5), lax.rem(f, 5))
    place = x if 0 <= x < X else (x + X if x < 0 else x - X)
    by = 128 - 3 - 6 * (4 * q + place)
    if a == 0 and not 0 <= x < X and not (isinstance(f, int) and f >= KEEP):
        packed = (x_lo if x < 0 else x_hi)[58]
        by = 128 - 3 - 24 * q - (18 - 6 * p if x < 0 else 6 * p)
    elif a == 0:
        packed = halo[p] if 0 <= x < X else (x_lo if x < 0 else x_hi)[59]
    elif 0 <= x < X:
        packed = y_halo[p]
    else:
        packed = x_corner[0 if x < 0 else 1]
    return shift_lanes(packed, by)


def along_y(get, key, coef):
    x, a, b = key
    row = rows_of()
    centre, other = get(key), get((x, 1 - a, b))
    ahead = shift_rows(jnp.where(row == 0, other, centre), 7)
    behind = shift_rows(jnp.where(row == 7, other, centre), 1)
    return coef(key, 3) * ahead + coef(key, 4) * behind


def apply(get, key, coef, skip=(), with_y=True):
    x, a, b = key
    lane = lanes_of()
    centre, other = get(key), get((x, a, 1 - b))
    ahead = shift_lanes(jnp.where(lane == 0, other, centre), 127)
    behind = shift_lanes(jnp.where(lane == 127, other, centre), 1)
    total = coef(key, 5) * ahead + coef(key, 6) * behind
    if with_y:
        total = along_y(get, key, coef) + total
    total = total + coef(key, 0) * centre
    for i, at in ((1, (x + 1, a, b)), (2, (x - 1, a, b))):
        if i not in skip:
            total = total + coef(key, i) * get(at)
    return total


def fill_coefficients(keys, out, refs):
    for at, key in enumerate(keys):
        diagonal = tile_of(21, key, refs)
        inside = diagonal != 0.0
        out[at, 0] = jnp.where(inside, diagonal - SIGMA, 0.0)
        for d in range(3):
            half = tile_of(22 + d, key, refs)
            out[at, 1 + 2 * d] = jnp.where(inside, half - 1.0, 0.0)
            out[at, 2 + 2 * d] = jnp.where(inside, -1.0 - half, 0.0)


def cached(f, refs):
    held = {}

    def get(key):
        if key not in held:
            held[key] = tile_of(f, key, refs)
        return held[key]

    return get


INNER = [key for key in COEF if 0 <= key[0] < X]
LEVEL = [key for key in INNER if not key[1]]
BESIDE = [key for key in INNER if key[1]]
OUTER = [key for key in COEF if not 0 <= key[0] < X]
ONCE = [key for key in region(1) if 0 <= key[0] < X]
SIDES = {0: (2, -1), X - 1: (1, X)}


def skip_of(key):
    return (SIDES[key[0]][0],) if key[0] in SIDES else ()


def level_kernel(rotated, rest, halo, coef_level, partial):
    refs = (Fields(rotated, rest), halo, None, None, None, None, None, None)
    fill_coefficients(LEVEL, coef_level, refs)
    coef = lambda key, i: coef_level[LEVEL.index(key), i]

    def body(f, carry):
        get = cached(f, refs)
        for at, key in enumerate(LEVEL):
            partial[f, at] = apply(get, key, coef, skip_of(key), with_y=False)
        return carry

    lax.fori_loop(0, KEEP, body, 0, unroll=5)


def inner_kernel(
    rotated, rest, halo, y_lo, y_hi, coef_level, level, coef_beside, partial, y_halo
):
    for p in range(5):
        y_halo[p] = corner_of(p, y_lo, y_hi)
    refs = (Fields(rotated, rest), halo, y_lo, y_hi, None, None, y_halo, None)
    fill_coefficients(BESIDE, coef_beside, refs)

    def coef(key, i):
        if key in LEVEL:
            return coef_level[LEVEL.index(key), i]
        return coef_beside[BESIDE.index(key), i]

    def body(f, carry):
        get = cached(f, refs)
        once = {}
        for at, key in enumerate(ONCE):
            if key in LEVEL:
                once[key] = level[f, LEVEL.index(key)] + along_y(get, key, coef)
            else:
                once[key] = apply(get, key, coef, skip_of(key))
            partial[f, at] = once[key]
        for x, skip in ((1, (2,)), (2, (1,))):
            partial[f, len(ONCE) + x - 1] = apply(once.__getitem__, (x, 0, 0), coef, skip)
        return carry

    lax.fori_loop(0, KEEP, body, 0, unroll=5)


def inner(a, b):
    return lax.dot_general(a, b, (((1,), (1,)), ((), ())), preferred_element_type=F32)


def stencil_kernel(
    copies,
    rotated,
    rest,
    halo,
    y_lo,
    y_hi,
    coef_level,
    coef_beside,
    partial,
    early,
    off,
    on,
    span,
    gram,
    coef_out,
    y_halo,
    x_corner,
    chain,
    x_lo,
    x_hi,
):
    fields = Fields(rotated, rest)
    upper = lax.axis_index("gx_1") == 1
    for i in range(on.shape[0]):
        far = early[i] if i < PLANES else off[i - PLANES]
        x_lo[i] = jnp.where(upper, on[i], far)
        x_hi[i] = jnp.where(upper, far, on[i])
    refs = (fields, halo, y_lo, y_hi, x_lo, x_hi, y_halo, x_corner)
    for p in range(5):
        y_halo[p] = corner_of(p, y_lo, y_hi)
    x_corner[0] = x_lo[60]
    x_corner[1] = x_hi[60]
    fill_coefficients(OUTER, coef_out, refs)

    def coef(key, i):
        if key in LEVEL:
            return coef_level[LEVEL.index(key), i]
        if key in BESIDE:
            return coef_beside[BESIDE.index(key), i]
        return coef_out[OUTER.index(key), i]

    def store(f, x, tile):
        at = f * (X * Y) + x * Y
        if not isinstance(f, int):
            at = pl.multiple_of(at, Y)
        span[pl.ds(at, Y), :] = tile

    tiles = {key: tile_of(20, key, refs) for key in region(3)}
    for x in range(X):
        store(60, x, tiles[(x, 0, 0)])
    for step in range(EXPAND):
        place = {}
        for at, key in enumerate(tiles):
            chain[at] = tiles[key]
            place[key] = at
        get = lambda key, place=place: chain[place[key]]
        tiles = {key: apply(get, key, coef) for key in region(2 - step)}
        for x in range(X):
            store(61 + step, x, tiles[(x, 0, 0)])

    def body(f, carry):
        get = cached(f, refs)
        once = {}
        for at, key in enumerate(ONCE):
            x, a, b = key
            if x not in SIDES and (a or b):
                continue
            tile = partial[f, at]
            if x in SIDES:
                i, side = SIDES[x]
                tile = tile + coef(key, i) * get((side, a, b))
            once[key] = tile
        for x in (-1, X):
            once[(x, 0, 0)] = apply(get, (x, 0, 0), coef)
        for x in range(X):
            store(f, x, get((x, 0, 0)))
            store(f + 20, x, once[(x, 0, 0)])
        for x in SIDES:
            store(f + 40, x, apply(once.__getitem__, (x, 0, 0), coef))
        for x, i, near in ((1, 2, 0), (2, 1, 3)):
            term = coef((x, 0, 0), i) * once[(near, 0, 0)]
            store(f + 40, x, partial[f, len(ONCE) + x - 1] + term)
        return carry

    lax.fori_loop(0, KEEP, body, 0, unroll=5)

    even = jnp.zeros((SPAN, SPAN), F32)
    mixed = even
    for r in range(0, X * Y, 2):
        pair = [span[pl.ds(r + i, SPAN, stride=X * Y), :] for i in range(2)]
        rows = jnp.concatenate(pair, axis=1)
        high = rows.astype(jnp.bfloat16)
        left = rows - high.astype(F32)
        middle = left.astype(jnp.bfloat16)
        low = (left - middle.astype(F32)).astype(jnp.bfloat16)
        even = even + (inner(high, high) + inner(middle, middle))
        mixed = mixed + (inner(high, middle) + inner(high, low))
    square = jnp.concatenate([mixed, jnp.zeros((SPAN, Z - SPAN), F32)], axis=1)
    square = jnp.concatenate([square, jnp.zeros((Z - SPAN, Z), F32)], axis=0)
    total = even + (mixed + square.T[:SPAN, :SPAN])
    wide = jnp.concatenate([total, jnp.zeros((SPAN, Z - SPAN), F32)], axis=1)
    lane = lanes_of()
    tiles = []
    for pieces in PIECES:
        tile = jnp.zeros(TILE, F32)
        for i, at in pieces:
            moved = wide[Y * i : Y * (i + 1)]
            moved = shift_lanes(moved, (at - Y * i) % Z) if at != Y * i else moved
            tile = jnp.where((lane >= at) & (lane < at + SPAN - Y * i), moved, tile)
        tiles.append(tile)
    extra = jnp.zeros(TILE, F32)
    for g in range(4):
        tile = shift_rows(wide[32:40], -2 * g)
        tile = shift_lanes(tile, (32 * g - 32) % Z) if g != 1 else tile
        extra = jnp.where((lane >= 32 * g) & (lane < 32 * g + 32), tile, extra)
    for i in range(copies):
        c = i // (copies // 2)
        for k in range(Y):
            gram[i, :, Z * k : Z * (k + 1)] = tiles[c][k : k + 1]
        gram[i, :, Z * Y :] = extra[c : c + 1]


PIECES = (((0, 0), (1, 64), (7, 120)), ((2, 0), (3, 48), (5, 88), (6, 112)))


def sum_kernel(copies, parts, out):
    total = parts[0]
    for i in range(1, parts.shape[0]):
        total = total + parts[i]
    for i in range(copies):
        out[i] = total


def exchange(parts, axis):
    return lax.all_to_all(parts, axis, 0, 0)


def finish_kernel(cell_count, parts, span, basis, hessenberg, spread, fresh, sems):
    early = pltpu.make_async_copy(
        span.at[pl.ds(0, KEEP)], basis.at[pl.ds(0, KEEP)], sems.at[0]
    )
    early.start()
    late = [
        pltpu.make_async_copy(fresh.at[k], basis.at[KEEP + k], sems.at[1 + k])
        for k in range(ROWS - KEEP)
    ]
    row, lane = rows_of(), lanes_of()
    rows = [None] * 8
    extra = jnp.zeros(TILE, F32)
    for c in range(2):
        tile = jnp.zeros(TILE, F32)
        for k in range(Y):
            tile = jnp.where(row == k, parts[c, :, Z * k : Z * (k + 1)], tile)
        tile = tile * (1.0 / cell_count)
        for i, at in PIECES[c]:
            moved = shift_lanes(tile, (Y * i - at) % Z) if at != Y * i else tile
            rows[i] = jnp.where((lane >= Y * i) & (lane < SPAN), moved, 0.0)
        extra = jnp.where(row == c, parts[c, :, Z * Y :], extra)
    extra = extra * (1.0 / cell_count)
    tile = jnp.zeros(TILE, F32)
    for g in range(4):
        moved = shift_lanes(extra, (32 - 32 * g) % Z) if g != 1 else extra
        tile = jnp.where((row >= 2 * g) & (row < 2 * g + 2), shift_rows(moved, 2 * g), tile)
    rows[4] = jnp.where((lane >= 32) & (lane < SPAN), tile, 0.0)
    blocks = jnp.concatenate([*rows, jnp.zeros((Z - SPAN, Z), F32)], axis=0)
    across = lax.broadcasted_iota(jnp.int32, (Z, Z), 1) // Y
    down = lax.broadcasted_iota(jnp.int32, (Z, Z), 0) // Y
    gram = (blocks + jnp.where(across < down, blocks.T, 0.0))[:SPAN]
    row64 = lax.broadcasted_iota(jnp.int32, (SPAN, Z), 0)
    lane64 = lax.broadcasted_iota(jnp.int32, (SPAN, Z), 1)
    eye = row64 == lane64
    moved = ((row64 >= KEEP) & (row64 < 60) & (lane64 == row64 - KEEP)) | (
        (row64 > 60) & (lane64 == row64 - 1)
    )
    row = lax.broadcasted_iota(jnp.int32, (ROWS, Z), 0)
    lane = lax.broadcasted_iota(jnp.int32, (ROWS, Z), 1)
    lane1 = lax.broadcasted_iota(jnp.int32, (1, Z), 1)

    def column(vector, picks):
        return jnp.sum(jnp.where(picks, vector, 0.0), axis=1, keepdims=True)

    first_row = gram[60:61, :]
    norm_sq = jnp.sum(jnp.where(lane1 == 60, first_row, 0.0), axis=1, keepdims=True)
    inverse = lax.rsqrt(jnp.maximum(norm_sq, 0.25))
    last = jnp.where(lane1 == 60, inverse, 0.0)
    last_gram = first_row * inverse
    up_column = jnp.where(lax.broadcasted_iota(jnp.int32, (SPAN, 1), 0) == 61, inverse, 0.0)
    q = jnp.where((row == lane) & (row < KEEP), 1.0, 0.0)
    q = jnp.where(row == KEEP, last, q)
    qg = jnp.where(row < KEEP, gram[:ROWS, :], 0.0)
    qg = jnp.where(row == KEEP, last_gram, qg)
    scale = jnp.broadcast_to(inverse, TILE)
    for x in range(X):
        fresh[0, x] = span[60, x] * scale
    late[0].start()
    for k in range(EXPAND):
        up = jnp.where(
            (lane1 >= KEEP) & (lane1 < 60),
            pltpu.roll(last, KEEP, 1),
            jnp.where((lane1 > 60) & (lane1 < SPAN), pltpu.roll(last, 1, 1), 0.0),
        )
        image = up + SIGMA * last
        image_gram = jnp.sum(up_column * gram, axis=0, keepdims=True) + SIGMA * last_gram
        c = jnp.sum(q * image_gram, axis=1, keepdims=True)
        partly = image - jnp.sum(c * q, axis=0, keepdims=True)
        partly_gram = image_gram - jnp.sum(c * qg, axis=0, keepdims=True)
        e = jnp.sum(q * partly_gram, axis=1, keepdims=True)
        cleaned = partly - jnp.sum(e * q, axis=0, keepdims=True)
        cleaned_gram = partly_gram - jnp.sum(e * qg, axis=0, keepdims=True)
        length_sq = jnp.sum(cleaned * cleaned_gram, axis=1, keepdims=True)
        here, shifted = column(cleaned, eye), column(cleaned, moved)
        inverse = lax.rsqrt(jnp.maximum(length_sq, 0.25))
        last = cleaned * inverse
        last_gram = cleaned_gram * inverse
        up_column = shifted * inverse
        q = jnp.where(row == KEEP + 1 + k, last, q)
        qg = jnp.where(row == KEEP + 1 + k, last_gram, qg)
        length = jnp.sqrt(jnp.maximum(length_sq, 0.0))
        entries = jnp.where(row == KEEP + 1 + k, length, c + e)
        turned = jnp.sum(jnp.where(row == lane, entries, 0.0), axis=0, keepdims=True)
        hessenberg[k : k + 1, :] = turned[:, :ROWS]
        spread[pl.ds(8 * k, 8)] = jnp.broadcast_to(here * inverse, (SPAN, Z)).reshape(8, 8, Z)
        fields = [*range(KEEP * (k + 1)), *range(60, 62 + k)]
        acc = [jnp.zeros(TILE, F32) for _ in range(X)]
        for f in fields:
            w = spread[8 * k + f // 8, f % 8 : f % 8 + 1, :]
            for x in range(X):
                acc[x] = acc[x] + w * span[f, x]
        for x in range(X):
            fresh[1 + k, x] = acc[x]
        late[1 + k].start()
    early.wait()
    for copy in late:
        copy.wait()


def send(value, axis, forward):
    count = lax.axis_size(axis)
    up = [(i, i + 1) for i in range(count - 1)]
    return lax.ppermute(value, axis, up if forward else [(j, i) for i, j in up])


def per_device(krylov_basis, schur_vectors, next_vector, diag_shift, velocity):
    axes = (*GX, "gy", "gz")
    cell_count = next_vector.size
    for axis in axes:
        cell_count *= lax.axis_size(axis)
    held, rest, packed, passed = call(
        edge_kernel,
        [
            krylov_basis.shape,
            (FIELDS - KEEP, X, Y, Z),
            (5, Y, Z),
            (KEEP, krylov_basis.shape[0]),
        ],
        [
            pltpu.with_memory_space_constraint(value, pltpu.HBM)
            for value in (krylov_basis, schur_vectors.T, next_vector, diag_shift, velocity)
        ],
        scratch=[
            pltpu.SMEM((KEEP, krylov_basis.shape[0]), F32),
            pltpu.VMEM((4, X, Y, Z), F32),
            pltpu.SemaphoreType.DMA((5 + krylov_basis.shape[0] // CHUNK,)),
        ],
        ins="hhhhh",
        limit=4,
    )
    z_lo, z_hi = send(packed, "gz", True), send(packed, "gz", False)
    (rotated,) = call(
        rotate_kernel,
        [(KEEP, X, Y, Z)],
        [held, passed],
        ins="vs",
        limit=4,
        flops=10**9,
    )
    up, down, halo = call(
        pack_y_kernel, [(27, Y, Z), (27, Y, Z), (5, Y, Z)], [rotated, rest, z_lo, z_hi]
    )
    count = lax.axis_size(GX)
    swap = [(i, i + 1) for i in range(1, count - 1, 2)]
    swap = swap + [(j, i) for i, j in swap]
    y_lo = send(up, "gy", True)
    y_hi = send(down, "gy", False)
    (early,) = call(planes_kernel, [(PLANES, Y, Z)], [rotated, rest])
    early = lax.ppermute(early, GX, swap)
    coef_level, level = call(
        level_kernel,
        [(len(LEVEL), 7, Y, Z), (KEEP, len(LEVEL), Y, Z)],
        [rotated, rest, halo],
        limit=4,
    )
    off, on = call(
        pack_x_kernel, [(61 - PLANES, Y, Z), (61, Y, Z)], [rotated, rest, halo, y_lo, y_hi]
    )
    off = lax.ppermute(off, GX, swap)
    on = lax.ppermute(on, "gx_1", [(0, 1), (1, 0)])
    stages = (("gx_1", "gz"), ("gx_0", "gy"))
    sizes = [lax.axis_size(stage) for stage in stages]
    coef_beside, partial = call(
        inner_kernel,
        [(len(BESIDE), 7, Y, Z), (KEEP, len(ONCE) + 2, Y, Z)],
        [rotated, rest, halo, y_lo, y_hi, coef_level, level],
        scratch=[pltpu.VMEM((5, Y, Z), F32)],
        limit=6,
        flops=10**9,
    )
    span, parts = call(
        functools.partial(stencil_kernel, sizes[0]),
        [(SPAN * X * Y, Z), (sizes[0], 1, WIRE)],
        [rotated, rest, halo, y_lo, y_hi, coef_level, coef_beside, partial, early, off, on],
        scratch=[
            pltpu.VMEM((len(OUTER), 7, Y, Z), F32),
            pltpu.VMEM((5, Y, Z), F32),
            pltpu.VMEM((2, Y, Z), F32),
            pltpu.VMEM((len(region(3)), Y, Z), F32),
            pltpu.VMEM((61, Y, Z), F32),
            pltpu.VMEM((61, Y, Z), F32),
        ],
        limit=8,
    )
    parts = exchange(parts, stages[0])
    (parts,) = call(functools.partial(sum_kernel, sizes[1]), [(sizes[1], 1, WIRE)], [parts])
    parts = exchange(parts, stages[1])
    (half,) = call(functools.partial(sum_kernel, 1), [(1, 1, WIRE)], [parts])
    whole = lax.all_gather(half, "gx_1", axis=0, tiled=True)
    basis, hessenberg = call(
        functools.partial(finish_kernel, cell_count),
        [(ROWS, X, Y, Z), (EXPAND, ROWS)],
        [whole, span.reshape(SPAN, X, Y, Z)],
        scratch=[
            pltpu.VMEM((8 * EXPAND, Y, Z), F32),
            pltpu.VMEM((ROWS - KEEP, X, Y, Z), F32),
            pltpu.SemaphoreType.DMA((1 + ROWS - KEEP,)),
        ],
        out="hv",
        limit=4,
    )
    return basis, hessenberg.T


def solution(mesh):
    split = Mesh(
        mesh.devices.reshape(-1, 2, mesh.shape["gy"], mesh.shape["gz"]),
        ("gx_0", "gx_1", "gy", "gz"),
    )
    return jax.shard_map(
        per_device,
        mesh=split,
        in_specs=(
            P(None, GX, "gy", "gz"),
            P(),
            P(GX, "gy", "gz"),
            P(GX, "gy", "gz"),
            P(None, GX, "gy", "gz"),
        ),
        out_specs=(P(None, GX, "gy", "gz"), P()),
        check_vma=False,
    )
```

```python
import functools

import jax
import jax.numpy as jnp
from jax import lax
from jax.experimental import pallas as pl
from jax.experimental.pallas import tpu as pltpu
from jax.sharding import Mesh
from jax.sharding import PartitionSpec as P

KEEP = 20
EXPAND = 3
ROWS = 24
FIELDS = 25
SPAN = 64
SIGMA = 7.125
PLANES = 51
WIRE = 1152
GX = ("gx_0", "gx_1")
X, Y, Z = (4, 8, 128)
TILE = (Y, Z)
F32 = jnp.float32


def rows_of():
    return lax.broadcasted_iota(jnp.int32, TILE, 0)


def lanes_of():
    return lax.broadcasted_iota(jnp.int32, TILE, 1)


def shift_rows(tile, by):
    by = by % Y
    return tile if by == 0 else pltpu.roll(tile, by, 0)


def shift_lanes(tile, by):
    return pltpu.roll(tile, by, 1)


def place_of(kind):
    return pl.BlockSpec(memory_space={"v": pltpu.VMEM, "s": pltpu.SMEM, "h": pltpu.HBM}[kind])


def call(kernel, outs, args, scratch=(), ins="", out="", flops=100000, limit=2):
    ins, out = ins or "v" * len(args), out or "v" * len(outs)
    return pl.pallas_call(
        kernel,
        out_shape=[jax.ShapeDtypeStruct(s, F32) for s in outs],
        in_specs=[place_of(k) for k in ins],
        out_specs=[place_of(k) for k in out],
        scratch_shapes=list(scratch),
        cost_estimate=pl.CostEstimate(flops=flops, bytes_accessed=100000, transcendentals=0),
        compiler_params=pltpu.CompilerParams(vmem_limit_bytes=limit * 2**20),
    )(*args)


CHUNK = 20


def edge_kernel(
    basis, schur, next_vector, diag, velocity, held, rest, packed, passed, weights, small, sems
):
    chunks = basis.shape[0] // CHUNK
    copies = [
        pltpu.make_async_copy(schur, weights, sems.at[0]),
        *(
            pltpu.make_async_copy(
                basis.at[pl.ds(c * CHUNK, CHUNK)], held.at[pl.ds(c * CHUNK, CHUNK)], sems.at[1 + c]
            )
            for c in range(chunks)
        ),
        pltpu.make_async_copy(next_vector, rest.at[0], sems.at[1 + chunks]),
        pltpu.make_async_copy(diag, small.at[0], sems.at[2 + chunks]),
        pltpu.make_async_copy(velocity, small.at[pl.ds(1, 3)], sems.at[3 + chunks]),
        pltpu.make_async_copy(schur, passed, sems.at[4 + chunks]),
    ]
    for copy in copies[1 + chunks : 4 + chunks]:
        copy.start()
    for copy in copies[: 1 + chunks]:
        copy.start()
    copies[4 + chunks].start()
    lane = lanes_of()
    for copy in copies[1 + chunks : 4 + chunks]:
        copy.wait()
    for x in range(X):
        rest[1, x] = 6.0 + small[0, x]
        for d in range(3):
            rest[2 + d, x] = 0.5 * small[1 + d, x]
    total = jnp.zeros(TILE, F32)
    for j in range(20):
        moved = shift_lanes(rest[j // 4, j % 4], 6 * j + 3)
        total = jnp.where((lane >= 6 * j) & (lane < 6 * j + 6), moved, total)
    packed[4] = total
    copies[0].wait()
    acc = [jnp.zeros(TILE, F32) for _ in range(KEEP)]
    for c in range(chunks):
        copies[1 + c].wait()
        for i in range(c * CHUNK, (c + 1) * CHUNK):
            edge = jnp.zeros(TILE, F32)
            for x in range(X):
                here = (lane >= 6 * x) & (lane < 6 * x + 6)
                edge = jnp.where(here, shift_lanes(held[i, x], 6 * x + 3), edge)
            for f in range(KEEP):
                acc[f] = acc[f] + weights[f, i] * edge
    for p in range(4):
        total = acc[5 * p]
        for q in range(1, 5):
            total = jnp.where(lane < 24 * q, total, shift_lanes(acc[5 * p + q], 24 * q))
        packed[p] = total
    copies[4 + chunks].wait()


def rotate_kernel(basis, schur, rotated):
    group = 5
    for g in range(KEEP // group):

        def body(i, acc, g=g):
            out = []
            tiles = [basis[i, x] for x in range(X)]
            for f in range(group):
                w = schur[g * group + f, i]
                for x in range(X):
                    out.append(acc[f * X + x] + w * tiles[x])
            return tuple(out)

        zero = tuple(jnp.zeros(TILE, F32) for _ in range(group * X))
        acc = lax.fori_loop(0, basis.shape[0], body, zero, unroll=4)
        for f in range(group):
            for x in range(X):
                rotated[g * group + f, x] = acc[f * X + x]


class Fields:
    def __init__(self, rotated, rest):
        self.rotated, self.rest = rotated, rest

    def __getitem__(self, at):
        f, x = at
        if isinstance(f, int) and f >= KEEP:
            return self.rest[f - KEEP, x]
        return self.rotated[f, x]


def pack_y_kernel(rotated, rest, from_lo, from_hi, up, down, halo):
    fields = Fields(rotated, rest)
    row, lane = rows_of(), lanes_of()
    left = lax.rem(lane, 6) < 3
    for f in range(FIELDS):
        a = jnp.zeros(TILE, F32)
        b = a
        for x in range(X):
            tile = fields[f, x]
            here = (row >= 2 * x) & (row < 2 * x + 2)
            a = jnp.where(here, shift_rows(tile, 2 * x - 6), a)
            b = jnp.where(here, shift_rows(tile, 2 * x), b)
        up[f] = a
        down[f] = b
    a = jnp.zeros(TILE, F32)
    b = a
    for x in range(X):
        tile = fields[20, x]
        a = jnp.where(row == x, shift_rows(tile, x - 5), a)
        b = jnp.where(row == x, shift_rows(tile, x - 2), b)
    up[25] = a
    down[25] = b
    a = jnp.zeros(TILE, F32)
    b = a
    for p in range(5):
        merged = jnp.where(left, from_lo[p], from_hi[p])
        halo[p] = merged
        a = jnp.where(row == p, shift_rows(merged, p - 7), a)
        b = jnp.where(row == p, shift_rows(merged, p), b)
    up[26] = jnp.where(row == 5, shift_rows(merged, -1), a)
    down[26] = jnp.where(row == 5, shift_rows(merged, 4), b)


def corner_of(p, y_lo, y_hi):
    row = rows_of()
    lo, hi = y_lo[26], y_hi[26]
    tile = jnp.where(row == 0, shift_rows(hi, -p), jnp.zeros(TILE, F32))
    tile = jnp.where(row == 7, shift_rows(lo, 7 - p), tile)
    if p == 4:
        tile = jnp.where(row == 1, shift_rows(hi, -4), tile)
        tile = jnp.where(row == 6, shift_rows(lo, 1), tile)
    return tile


def planes_kernel(rotated, rest, early):
    fields = Fields(rotated, rest)
    upper = lax.axis_index("gx_1") == 1
    for f in range(FIELDS):
        early[2 * f] = jnp.where(upper, fields[f, 2], fields[f, 0])
        early[2 * f + 1] = jnp.where(upper, fields[f, 3], fields[f, 1])
    early[PLANES - 1] = jnp.where(upper, fields[20, 1], fields[20, 2])


def pack_x_kernel(rotated, rest, halo, y_lo, y_hi, off, on):
    fields = Fields(rotated, rest)
    first, row = rows_of() < 4, rows_of()
    upper = lax.axis_index("gx_1") == 1

    def put(at, up, down):
        if at >= PLANES:
            off[at - PLANES] = jnp.where(upper, up, down)
        on[at] = jnp.where(upper, down, up)

    for f in range(FIELDS):
        put(2 * f, fields[f, 2], fields[f, 0])
        put(2 * f + 1, fields[f, 3], fields[f, 1])
    put(50, fields[20, 1], fields[20, 2])
    lo, hi = y_lo[20], y_hi[20]
    put(51, jnp.where(first, shift_rows(lo, 4), hi), jnp.where(first, lo, shift_rows(hi, 4)))
    for v in range(6):
        a = jnp.zeros(TILE, F32)
        b = a
        for k in range(4):
            f = 4 * v + k + (1 if v == 5 else 0)
            lo, hi = y_lo[f], y_hi[f]
            a = jnp.where(row == 2 * k, shift_rows(lo, 2 * k - 7), a)
            a = jnp.where(row == 2 * k + 1, shift_rows(hi, 2 * k - 5), a)
            b = jnp.where(row == 2 * k, shift_rows(lo, 2 * k - 1), b)
            b = jnp.where(row == 2 * k + 1, shift_rows(hi, 2 * k + 1), b)
        put(52 + v, a, b)
    part = lax.rem(lanes_of(), 24)
    a = jnp.zeros(TILE, F32)
    b = a
    for p in range(4):
        tile = halo[p]
        here = (part >= 18 - 6 * p) & (part < 24 - 6 * p)
        a = jnp.where(here, shift_lanes(tile, -6 * p % Z) if p else tile, a)
        here = (part >= 6 * p) & (part < 6 * p + 6)
        b = jnp.where(here, shift_lanes(tile, 6 * p) if p else tile, b)
    put(58, a, b)
    corner = corner_of(4, y_lo, y_hi)
    put(59, halo[4], halo[4])
    put(60, corner, corner)


def region(radius):
    out = []
    for a, b in ((0, 0), (1, 0), (0, 1), (1, 1)):
        reach = radius - a - b
        if reach >= 0:
            out.extend((x, a, b) for x in range(-reach, X + reach))
    return out


COEF = region(2)


def tile_of(f, key, refs):
    fields, halo, y_lo, y_hi, x_lo, x_hi, y_halo, x_corner = refs
    x, a, b = key
    first = rows_of() < 4
    if b == 0:
        if a == 0:
            if 0 <= x < X:
                return fields[f, x]
            if x == -3:
                return x_lo[50]
            if x == 6:
                return x_hi[50]
            return x_lo[2 * f + x + 2] if x < 0 else x_hi[2 * f + x - 4]
        if 0 <= x < X:
            lo, hi = y_lo[f], y_hi[f]
            tile = jnp.where(first, shift_rows(hi, -2 * x), shift_rows(lo, 6 - 2 * x))
            if isinstance(f, int) and f == 20:
                row = rows_of()
                tile = jnp.where(row == 2, shift_rows(y_hi[25], 2 - x), tile)
                tile = jnp.where(row == 5, shift_rows(y_lo[25], 5 - x), tile)
            return tile
        side = x_lo if x < 0 else x_hi
        if not (isinstance(f, int) and f == 20):
            g = f - 1 if isinstance(f, int) and f > 20 else f
            v, k = (g // 4, g % 4) if isinstance(g, int) else (lax.div(g, 4), lax.rem(g, 4))
            return pltpu.roll(side[52 + v], 7 - 2 * k, 0)
        packed = side[51]
        if x in (-1, 5):
            return jnp.where(first, shift_rows(packed, 2), shift_rows(packed, 4))
        return jnp.where(first, shift_rows(packed, 4), shift_rows(packed, 6))
    p, q = (f // 5, f % 5) if isinstance(f, int) else (lax.div(f, 5), lax.rem(f, 5))
    place = x if 0 <= x < X else (x + X if x < 0 else x - X)
    by = 128 - 3 - 6 * (4 * q + place)
    if a == 0 and not 0 <= x < X and not (isinstance(f, int) and f >= KEEP):
        packed = (x_lo if x < 0 else x_hi)[58]
        by = 128 - 3 - 24 * q - (18 - 6 * p if x < 0 else 6 * p)
    elif a == 0:
        packed = halo[p] if 0 <= x < X else (x_lo if x < 0 else x_hi)[59]
    elif 0 <= x < X:
        packed = y_halo[p]
    else:
        packed = x_corner[0 if x < 0 else 1]
    return shift_lanes(packed, by)


def along_y(get, key, coef):
    x, a, b = key
    row = rows_of()
    centre, other = get(key), get((x, 1 - a, b))
    ahead = shift_rows(jnp.where(row == 0, other, centre), 7)
    behind = shift_rows(jnp.where(row == 7, other, centre), 1)
    return coef(key, 3) * ahead + coef(key, 4) * behind


def apply(get, key, coef, skip=(), with_y=True):
    x, a, b = key
    lane = lanes_of()
    centre, other = get(key), get((x, a, 1 - b))
    ahead = shift_lanes(jnp.where(lane == 0, other, centre), 127)
    behind = shift_lanes(jnp.where(lane == 127, other, centre), 1)
    total = coef(key, 5) * ahead + coef(key, 6) * behind
    if with_y:
        total = along_y(get, key, coef) + total
    total = total + coef(key, 0) * centre
    for i, at in ((1, (x + 1, a, b)), (2, (x - 1, a, b))):
        if i not in skip:
            total = total + coef(key, i) * get(at)
    return total


def fill_coefficients(keys, out, refs):
    for at, key in enumerate(keys):
        diagonal = tile_of(21, key, refs)
        inside = diagonal != 0.0
        out[at, 0] = jnp.where(inside, diagonal - SIGMA, 0.0)
        for d in range(3):
            half = tile_of(22 + d, key, refs)
            out[at, 1 + 2 * d] = jnp.where(inside, half - 1.0, 0.0)
            out[at, 2 + 2 * d] = jnp.where(inside, -1.0 - half, 0.0)


def cached(f, refs):
    held = {}

    def get(key):
        if key not in held:
            held[key] = tile_of(f, key, refs)
        return held[key]

    return get


INNER = [key for key in COEF if 0 <= key[0] < X]
LEVEL = [key for key in INNER if not key[1] and not key[2]]
BESIDE = [key for key in INNER if key[1] or key[2]]
OUTER = [key for key in COEF if not 0 <= key[0] < X]
ONCE = [key for key in region(1) if 0 <= key[0] < X]
SIDES = {0: (2, -1), X - 1: (1, X)}


def skip_of(key):
    return (SIDES[key[0]][0],) if key[0] in SIDES else ()


def level_kernel(rotated, rest, halo, coef_level, partial):
    refs = (Fields(rotated, rest), halo, None, None, None, None, None, None)
    fill_coefficients(LEVEL, coef_level, refs)
    coef = lambda key, i: coef_level[LEVEL.index(key), i]

    def body(f, carry):
        get = cached(f, refs)
        for at, key in enumerate(LEVEL):
            partial[f, at] = apply(get, key, coef, skip_of(key), with_y=False)
        return carry

    lax.fori_loop(0, KEEP, body, 0, unroll=5)


def inner_kernel(
    rotated, rest, halo, y_lo, y_hi, coef_level, level, coef_beside, partial, y_halo
):
    for p in range(5):
        y_halo[p] = corner_of(p, y_lo, y_hi)
    refs = (Fields(rotated, rest), halo, y_lo, y_hi, None, None, y_halo, None)
    fill_coefficients(BESIDE, coef_beside, refs)

    def coef(key, i):
        if key in LEVEL:
            return coef_level[LEVEL.index(key), i]
        return coef_beside[BESIDE.index(key), i]

    def body(f, carry):
        get = cached(f, refs)
        once = {}
        for at, key in enumerate(ONCE):
            if key in LEVEL:
                once[key] = level[f, LEVEL.index(key)] + along_y(get, key, coef)
            else:
                once[key] = apply(get, key, coef, skip_of(key))
            partial[f, at] = once[key]
        for x, skip in ((1, (2,)), (2, (1,))):
            partial[f, len(ONCE) + x - 1] = apply(once.__getitem__, (x, 0, 0), coef, skip)
        return carry

    lax.fori_loop(0, KEEP, body, 0, unroll=5)


def inner(a, b):
    return lax.dot_general(a, b, (((1,), (1,)), ((), ())), preferred_element_type=F32)


def stencil_kernel(
    copies,
    rotated,
    rest,
    halo,
    y_lo,
    y_hi,
    coef_level,
    coef_beside,
    partial,
    early,
    off,
    on,
    span,
    gram,
    coef_out,
    y_halo,
    x_corner,
    chain,
    x_lo,
    x_hi,
):
    fields = Fields(rotated, rest)
    upper = lax.axis_index("gx_1") == 1
    for i in range(on.shape[0]):
        far = early[i] if i < PLANES else off[i - PLANES]
        x_lo[i] = jnp.where(upper, on[i], far)
        x_hi[i] = jnp.where(upper, far, on[i])
    refs = (fields, halo, y_lo, y_hi, x_lo, x_hi, y_halo, x_corner)
    for p in range(5):
        y_halo[p] = corner_of(p, y_lo, y_hi)
    x_corner[0] = x_lo[60]
    x_corner[1] = x_hi[60]
    fill_coefficients(OUTER, coef_out, refs)

    def coef(key, i):
        if key in LEVEL:
            return coef_level[LEVEL.index(key), i]
        if key in BESIDE:
            return coef_beside[BESIDE.index(key), i]
        return coef_out[OUTER.index(key), i]

    def store(f, x, tile):
        at = f * (X * Y) + x * Y
        if not isinstance(f, int):
            at = pl.multiple_of(at, Y)
        span[pl.ds(at, Y), :] = tile

    tiles = {key: tile_of(20, key, refs) for key in region(3)}
    for x in range(X):
        store(60, x, tiles[(x, 0, 0)])
    for step in range(EXPAND):
        place = {}
        for at, key in enumerate(tiles):
            chain[at] = tiles[key]
            place[key] = at
        get = lambda key, place=place: chain[place[key]]
        tiles = {key: apply(get, key, coef) for key in region(2 - step)}
        for x in range(X):
            store(61 + step, x, tiles[(x, 0, 0)])

    def body(f, carry):
        get = cached(f, refs)
        once = {}
        for at, key in enumerate(ONCE):
            x, a, b = key
            if x not in SIDES and (a or b):
                continue
            tile = partial[f, at]
            if x in SIDES:
                i, side = SIDES[x]
                tile = tile + coef(key, i) * get((side, a, b))
            once[key] = tile
        for x in (-1, X):
            once[(x, 0, 0)] = apply(get, (x, 0, 0), coef)
        for x in range(X):
            store(f, x, get((x, 0, 0)))
            store(f + 20, x, once[(x, 0, 0)])
        for x in SIDES:
            store(f + 40, x, apply(once.__getitem__, (x, 0, 0), coef))
        for x, i, near in ((1, 2, 0), (2, 1, 3)):
            term = coef((x, 0, 0), i) * once[(near, 0, 0)]
            store(f + 40, x, partial[f, len(ONCE) + x - 1] + term)
        return carry

    lax.fori_loop(0, KEEP, body, 0, unroll=5)

    even = jnp.zeros((SPAN, SPAN), F32)
    mixed = even
    for r in range(0, X * Y, 2):
        pair = [span[pl.ds(r + i, SPAN, stride=X * Y), :] for i in range(2)]
        rows = jnp.concatenate(pair, axis=1)
        high = rows.astype(jnp.bfloat16)
        left = rows - high.astype(F32)
        middle = left.astype(jnp.bfloat16)
        low = (left - middle.astype(F32)).astype(jnp.bfloat16)
        even = even + (inner(high, high) + inner(middle, middle))
        mixed = mixed + (inner(high, middle) + inner(high, low))
    square = jnp.concatenate([mixed, jnp.zeros((SPAN, Z - SPAN), F32)], axis=1)
    square = jnp.concatenate([square, jnp.zeros((Z - SPAN, Z), F32)], axis=0)
    total = even + (mixed + square.T[:SPAN, :SPAN])
    wide = jnp.concatenate([total, jnp.zeros((SPAN, Z - SPAN), F32)], axis=1)
    lane = lanes_of()
    tiles = []
    for pieces in PIECES:
        tile = jnp.zeros(TILE, F32)
        for i, at in pieces:
            moved = wide[Y * i : Y * (i + 1)]
            moved = shift_lanes(moved, (at - Y * i) % Z) if at != Y * i else moved
            tile = jnp.where((lane >= at) & (lane < at + SPAN - Y * i), moved, tile)
        tiles.append(tile)
    extra = jnp.zeros(TILE, F32)
    for g in range(4):
        tile = shift_rows(wide[32:40], -2 * g)
        tile = shift_lanes(tile, (32 * g - 32) % Z) if g != 1 else tile
        extra = jnp.where((lane >= 32 * g) & (lane < 32 * g + 32), tile, extra)
    for i in range(copies):
        c = i // (copies // 2)
        for k in range(Y):
            gram[i, :, Z * k : Z * (k + 1)] = tiles[c][k : k + 1]
        gram[i, :, Z * Y :] = extra[c : c + 1]


PIECES = (((0, 0), (1, 64), (7, 120)), ((2, 0), (3, 48), (5, 88), (6, 112)))


def sum_kernel(copies, parts, out):
    total = parts[0]
    for i in range(1, parts.shape[0]):
        total = total + parts[i]
    for i in range(copies):
        out[i] = total


def exchange(parts, axis):
    return lax.all_to_all(parts, axis, 0, 0)


def finish_kernel(cell_count, parts, span, basis, hessenberg, spread, fresh, sems):
    early = pltpu.make_async_copy(
        span.at[pl.ds(0, KEEP)], basis.at[pl.ds(0, KEEP)], sems.at[0]
    )
    early.start()
    late = [
        pltpu.make_async_copy(fresh.at[k], basis.at[KEEP + k], sems.at[1 + k])
        for k in range(ROWS - KEEP)
    ]
    row, lane = rows_of(), lanes_of()
    rows = [None] * 8
    extra = jnp.zeros(TILE, F32)
    for c in range(2):
        tile = jnp.zeros(TILE, F32)
        for k in range(Y):
            tile = jnp.where(row == k, parts[c, :, Z * k : Z * (k + 1)], tile)
        tile = tile * (1.0 / cell_count)
        for i, at in PIECES[c]:
            moved = shift_lanes(tile, (Y * i - at) % Z) if at != Y * i else tile
            rows[i] = jnp.where((lane >= Y * i) & (lane < SPAN), moved, 0.0)
        extra = jnp.where(row == c, parts[c, :, Z * Y :], extra)
    extra = extra * (1.0 / cell_count)
    tile = jnp.zeros(TILE, F32)
    for g in range(4):
        moved = shift_lanes(extra, (32 - 32 * g) % Z) if g != 1 else extra
        tile = jnp.where((row >= 2 * g) & (row < 2 * g + 2), shift_rows(moved, 2 * g), tile)
    rows[4] = jnp.where((lane >= 32) & (lane < SPAN), tile, 0.0)
    blocks = jnp.concatenate([*rows, jnp.zeros((Z - SPAN, Z), F32)], axis=0)
    across = lax.broadcasted_iota(jnp.int32, (Z, Z), 1) // Y
    down = lax.broadcasted_iota(jnp.int32, (Z, Z), 0) // Y
    gram = (blocks + jnp.where(across < down, blocks.T, 0.0))[:SPAN]
    row64 = lax.broadcasted_iota(jnp.int32, (SPAN, Z), 0)
    lane64 = lax.broadcasted_iota(jnp.int32, (SPAN, Z), 1)
    eye = row64 == lane64
    moved = ((row64 >= KEEP) & (row64 < 60) & (lane64 == row64 - KEEP)) | (
        (row64 > 60) & (lane64 == row64 - 1)
    )
    row = lax.broadcasted_iota(jnp.int32, (ROWS, Z), 0)
    lane = lax.broadcasted_iota(jnp.int32, (ROWS, Z), 1)
    lane1 = lax.broadcasted_iota(jnp.int32, (1, Z), 1)

    def column(vector, picks):
        return jnp.sum(jnp.where(picks, vector, 0.0), axis=1, keepdims=True)

    first_row = gram[60:61, :]
    norm_sq = jnp.sum(jnp.where(lane1 == 60, first_row, 0.0), axis=1, keepdims=True)
    inverse = lax.rsqrt(jnp.maximum(norm_sq, 0.25))
    last = jnp.where(lane1 == 60, inverse, 0.0)
    last_gram = first_row * inverse
    up_column = jnp.where(lax.broadcasted_iota(jnp.int32, (SPAN, 1), 0) == 61, inverse, 0.0)
    q = jnp.where((row == lane) & (row < KEEP), 1.0, 0.0)
    q = jnp.where(row == KEEP, last, q)
    qg = jnp.where(row < KEEP, gram[:ROWS, :], 0.0)
    qg = jnp.where(row == KEEP, last_gram, qg)
    scale = jnp.broadcast_to(inverse, TILE)
    for x in range(X):
        fresh[0, x] = span[60, x] * scale
    late[0].start()
    for k in range(EXPAND):
        up = jnp.where(
            (lane1 >= KEEP) & (lane1 < 60),
            pltpu.roll(last, KEEP, 1),
            jnp.where((lane1 > 60) & (lane1 < SPAN), pltpu.roll(last, 1, 1), 0.0),
        )
        image = up + SIGMA * last
        image_gram = jnp.sum(up_column * gram, axis=0, keepdims=True) + SIGMA * last_gram
        c = jnp.sum(q * image_gram, axis=1, keepdims=True)
        partly = image - jnp.sum(c * q, axis=0, keepdims=True)
        partly_gram = image_gram - jnp.sum(c * qg, axis=0, keepdims=True)
        e = jnp.sum(q * partly_gram, axis=1, keepdims=True)
        cleaned = partly - jnp.sum(e * q, axis=0, keepdims=True)
        cleaned_gram = partly_gram - jnp.sum(e * qg, axis=0, keepdims=True)
        length_sq = jnp.sum(cleaned * cleaned_gram, axis=1, keepdims=True)
        here, shifted = column(cleaned, eye), column(cleaned, moved)
        inverse = lax.rsqrt(jnp.maximum(length_sq, 0.25))
        last = cleaned * inverse
        last_gram = cleaned_gram * inverse
        up_column = shifted * inverse
        q = jnp.where(row == KEEP + 1 + k, last, q)
        qg = jnp.where(row == KEEP + 1 + k, last_gram, qg)
        length = jnp.sqrt(jnp.maximum(length_sq, 0.0))
        entries = jnp.where(row == KEEP + 1 + k, length, c + e)
        turned = jnp.sum(jnp.where(row == lane, entries, 0.0), axis=0, keepdims=True)
        hessenberg[k : k + 1, :] = turned[:, :ROWS]
        spread[pl.ds(8 * k, 8)] = jnp.broadcast_to(here * inverse, (SPAN, Z)).reshape(8, 8, Z)
        fields = [*range(KEEP * (k + 1)), *range(60, 62 + k)]
        acc = [jnp.zeros(TILE, F32) for _ in range(X)]
        for f in fields:
            w = spread[8 * k + f // 8, f % 8 : f % 8 + 1, :]
            for x in range(X):
                acc[x] = acc[x] + w * span[f, x]
        for x in range(X):
            fresh[1 + k, x] = acc[x]
        late[1 + k].start()
    early.wait()
    for copy in late:
        copy.wait()


def send(value, axis, forward):
    count = lax.axis_size(axis)
    up = [(i, i + 1) for i in range(count - 1)]
    return lax.ppermute(value, axis, up if forward else [(j, i) for i, j in up])


def per_device(krylov_basis, schur_vectors, next_vector, diag_shift, velocity):
    axes = (*GX, "gy", "gz")
    cell_count = next_vector.size
    for axis in axes:
        cell_count *= lax.axis_size(axis)
    held, rest, packed, passed = call(
        edge_kernel,
        [
            krylov_basis.shape,
            (FIELDS - KEEP, X, Y, Z),
            (5, Y, Z),
            (KEEP, krylov_basis.shape[0]),
        ],
        [
            pltpu.with_memory_space_constraint(value, pltpu.HBM)
            for value in (krylov_basis, schur_vectors.T, next_vector, diag_shift, velocity)
        ],
        scratch=[
            pltpu.SMEM((KEEP, krylov_basis.shape[0]), F32),
            pltpu.VMEM((4, X, Y, Z), F32),
            pltpu.SemaphoreType.DMA((5 + krylov_basis.shape[0] // CHUNK,)),
        ],
        ins="hhhhh",
        limit=4,
    )
    z_lo, z_hi = send(packed, "gz", True), send(packed, "gz", False)
    (rotated,) = call(
        rotate_kernel,
        [(KEEP, X, Y, Z)],
        [held, passed],
        ins="vs",
        limit=4,
        flops=10**9,
    )
    up, down, halo = call(
        pack_y_kernel, [(27, Y, Z), (27, Y, Z), (5, Y, Z)], [rotated, rest, z_lo, z_hi]
    )
    count = lax.axis_size(GX)
    swap = [(i, i + 1) for i in range(1, count - 1, 2)]
    swap = swap + [(j, i) for i, j in swap]
    y_lo = send(up, "gy", True)
    y_hi = send(down, "gy", False)
    (early,) = call(planes_kernel, [(PLANES, Y, Z)], [rotated, rest])
    early = lax.ppermute(early, GX, swap)
    coef_level, level = call(
        level_kernel,
        [(len(LEVEL), 7, Y, Z), (KEEP, len(LEVEL), Y, Z)],
        [rotated, rest, halo],
        limit=4,
    )
    off, on = call(
        pack_x_kernel, [(61 - PLANES, Y, Z), (61, Y, Z)], [rotated, rest, halo, y_lo, y_hi]
    )
    off = lax.ppermute(off, GX, swap)
    on = lax.ppermute(on, "gx_1", [(0, 1), (1, 0)])
    stages = (("gx_1", "gz"), ("gx_0", "gy"))
    sizes = [lax.axis_size(stage) for stage in stages]
    coef_beside, partial = call(
        inner_kernel,
        [(len(BESIDE), 7, Y, Z), (KEEP, len(ONCE) + 2, Y, Z)],
        [rotated, rest, halo, y_lo, y_hi, coef_level, level],
        scratch=[pltpu.VMEM((5, Y, Z), F32)],
        limit=6,
        flops=10**9,
    )
    span, parts = call(
        functools.partial(stencil_kernel, sizes[0]),
        [(SPAN * X * Y, Z), (sizes[0], 1, WIRE)],
        [rotated, rest, halo, y_lo, y_hi, coef_level, coef_beside, partial, early, off, on],
        scratch=[
            pltpu.VMEM((len(OUTER), 7, Y, Z), F32),
            pltpu.VMEM((5, Y, Z), F32),
            pltpu.VMEM((2, Y, Z), F32),
            pltpu.VMEM((len(region(3)), Y, Z), F32),
            pltpu.VMEM((61, Y, Z), F32),
            pltpu.VMEM((61, Y, Z), F32),
        ],
        limit=8,
    )
    parts = exchange(parts, stages[0])
    (parts,) = call(functools.partial(sum_kernel, sizes[1]), [(sizes[1], 1, WIRE)], [parts])
    parts = exchange(parts, stages[1])
    (half,) = call(functools.partial(sum_kernel, 1), [(1, 1, WIRE)], [parts])
    whole = lax.all_gather(half, "gx_1", axis=0, tiled=True)
    basis, hessenberg = call(
        functools.partial(finish_kernel, cell_count),
        [(ROWS, X, Y, Z), (EXPAND, ROWS)],
        [whole, span.reshape(SPAN, X, Y, Z)],
        scratch=[
            pltpu.VMEM((8 * EXPAND, Y, Z), F32),
            pltpu.VMEM((ROWS - KEEP, X, Y, Z), F32),
            pltpu.SemaphoreType.DMA((1 + ROWS - KEEP,)),
        ],
        out="hv",
        limit=4,
    )
    return basis, hessenberg.T


def solution(mesh):
    split = Mesh(
        mesh.devices.reshape(-1, 2, mesh.shape["gy"], mesh.shape["gz"]),
        ("gx_0", "gx_1", "gy", "gz"),
    )
    return jax.shard_map(
        per_device,
        mesh=split,
        in_specs=(
            P(None, GX, "gy", "gz"),
            P(),
            P(GX, "gy", "gz"),
            P(GX, "gy", "gz"),
            P(None, GX, "gy", "gz"),
        ),
        out_specs=(P(None, GX, "gy", "gz"), P()),
        check_vma=False,
    )
```

```python
import functools

import jax
import jax.numpy as jnp
from jax import lax
from jax.experimental import pallas as pl
from jax.experimental.pallas import tpu as pltpu
from jax.sharding import Mesh
from jax.sharding import PartitionSpec as P

KEEP = 20
EXPAND = 3
ROWS = 24
FIELDS = 25
SPAN = 64
SIGMA = 7.125
PLANES = 51
WIRE = 1152
GX = ("gx_0", "gx_1")
X, Y, Z = (4, 8, 128)
TILE = (Y, Z)
F32 = jnp.float32


def rows_of():
    return lax.broadcasted_iota(jnp.int32, TILE, 0)


def lanes_of():
    return lax.broadcasted_iota(jnp.int32, TILE, 1)


def shift_rows(tile, by):
    by = by % Y
    return tile if by == 0 else pltpu.roll(tile, by, 0)


def shift_lanes(tile, by):
    return pltpu.roll(tile, by, 1)


def place_of(kind):
    return pl.BlockSpec(memory_space={"v": pltpu.VMEM, "s": pltpu.SMEM, "h": pltpu.HBM}[kind])


def call(kernel, outs, args, scratch=(), ins="", out="", flops=100000, limit=2):
    ins, out = ins or "v" * len(args), out or "v" * len(outs)
    return pl.pallas_call(
        kernel,
        out_shape=[jax.ShapeDtypeStruct(s, F32) for s in outs],
        in_specs=[place_of(k) for k in ins],
        out_specs=[place_of(k) for k in out],
        scratch_shapes=list(scratch),
        cost_estimate=pl.CostEstimate(flops=flops, bytes_accessed=100000, transcendentals=0),
        compiler_params=pltpu.CompilerParams(vmem_limit_bytes=limit * 2**20),
    )(*args)


CHUNK = 20


def edge_kernel(
    basis, schur, next_vector, diag, velocity, held, rest, packed, passed, weights, small, sems
):
    chunks = basis.shape[0] // CHUNK
    copies = [
        pltpu.make_async_copy(schur, weights, sems.at[0]),
        *(
            pltpu.make_async_copy(
                basis.at[pl.ds(c * CHUNK, CHUNK)], held.at[pl.ds(c * CHUNK, CHUNK)], sems.at[1 + c]
            )
            for c in range(chunks)
        ),
        pltpu.make_async_copy(next_vector, rest.at[0], sems.at[1 + chunks]),
        pltpu.make_async_copy(diag, small.at[0], sems.at[2 + chunks]),
        pltpu.make_async_copy(velocity, small.at[pl.ds(1, 3)], sems.at[3 + chunks]),
        pltpu.make_async_copy(schur, passed, sems.at[4 + chunks]),
    ]
    for copy in copies[1 + chunks : 4 + chunks]:
        copy.start()
    for copy in copies[: 1 + chunks]:
        copy.start()
    copies[4 + chunks].start()
    lane = lanes_of()
    for copy in copies[1 + chunks : 4 + chunks]:
        copy.wait()
    for x in range(X):
        rest[1, x] = 6.0 + small[0, x]
        for d in range(3):
            rest[2 + d, x] = 0.5 * small[1 + d, x]
    total = jnp.zeros(TILE, F32)
    for j in range(20):
        moved = shift_lanes(rest[j // 4, j % 4], 6 * j + 3)
        total = jnp.where((lane >= 6 * j) & (lane < 6 * j + 6), moved, total)
    packed[4] = total
    copies[0].wait()
    acc = [jnp.zeros(TILE, F32) for _ in range(KEEP)]
    for c in range(chunks):
        copies[1 + c].wait()
        for i in range(c * CHUNK, (c + 1) * CHUNK):
            edge = jnp.zeros(TILE, F32)
            for x in range(X):
                here = (lane >= 6 * x) & (lane < 6 * x + 6)
                edge = jnp.where(here, shift_lanes(held[i, x], 6 * x + 3), edge)
            for f in range(KEEP):
                acc[f] = acc[f] + weights[f, i] * edge
    for p in range(4):
        total = acc[5 * p]
        for q in range(1, 5):
            total = jnp.where(lane < 24 * q, total, shift_lanes(acc[5 * p + q], 24 * q))
        packed[p] = total
    copies[4 + chunks].wait()


def rotate_kernel(basis, schur, rotated):
    group = 5
    for g in range(KEEP // group):

        def body(i, acc, g=g):
            out = []
            tiles = [basis[i, x] for x in range(X)]
            for f in range(group):
                w = schur[g * group + f, i]
                for x in range(X):
                    out.append(acc[f * X + x] + w * tiles[x])
            return tuple(out)

        zero = tuple(jnp.zeros(TILE, F32) for _ in range(group * X))
        acc = lax.fori_loop(0, basis.shape[0], body, zero, unroll=4)
        for f in range(group):
            for x in range(X):
                rotated[g * group + f, x] = acc[f * X + x]


class Fields:
    def __init__(self, rotated, rest):
        self.rotated, self.rest = rotated, rest

    def __getitem__(self, at):
        f, x = at
        if isinstance(f, int) and f >= KEEP:
            return self.rest[f - KEEP, x]
        return self.rotated[f, x]


def pack_y_kernel(rotated, rest, from_lo, from_hi, up, down, halo):
    fields = Fields(rotated, rest)
    row, lane = rows_of(), lanes_of()
    left = lax.rem(lane, 6) < 3
    for f in range(FIELDS):
        a = jnp.zeros(TILE, F32)
        b = a
        for x in range(X):
            tile = fields[f, x]
            here = (row >= 2 * x) & (row < 2 * x + 2)
            a = jnp.where(here, shift_rows(tile, 2 * x - 6), a)
            b = jnp.where(here, shift_rows(tile, 2 * x), b)
        up[f] = a
        down[f] = b
    a = jnp.zeros(TILE, F32)
    b = a
    for x in range(X):
        tile = fields[20, x]
        a = jnp.where(row == x, shift_rows(tile, x - 5), a)
        b = jnp.where(row == x, shift_rows(tile, x - 2), b)
    up[25] = a
    down[25] = b
    a = jnp.zeros(TILE, F32)
    b = a
    for p in range(5):
        merged = jnp.where(left, from_lo[p], from_hi[p])
        halo[p] = merged
        a = jnp.where(row == p, shift_rows(merged, p - 7), a)
        b = jnp.where(row == p, shift_rows(merged, p), b)
    up[26] = jnp.where(row == 5, shift_rows(merged, -1), a)
    down[26] = jnp.where(row == 5, shift_rows(merged, 4), b)


def corner_of(p, y_lo, y_hi):
    row = rows_of()
    lo, hi = y_lo[26], y_hi[26]
    tile = jnp.where(row == 0, shift_rows(hi, -p), jnp.zeros(TILE, F32))
    tile = jnp.where(row == 7, shift_rows(lo, 7 - p), tile)
    if p == 4:
        tile = jnp.where(row == 1, shift_rows(hi, -4), tile)
        tile = jnp.where(row == 6, shift_rows(lo, 1), tile)
    return tile


def planes_kernel(rotated, rest, early):
    fields = Fields(rotated, rest)
    upper = lax.axis_index("gx_1") == 1
    for f in range(FIELDS):
        early[2 * f] = jnp.where(upper, fields[f, 2], fields[f, 0])
        early[2 * f + 1] = jnp.where(upper, fields[f, 3], fields[f, 1])
    early[PLANES - 1] = jnp.where(upper, fields[20, 1], fields[20, 2])


def pack_x_kernel(rotated, rest, halo, y_lo, y_hi, off, on):
    fields = Fields(rotated, rest)
    first, row = rows_of() < 4, rows_of()
    upper = lax.axis_index("gx_1") == 1

    def put(at, up, down):
        if at >= PLANES:
            off[at - PLANES] = jnp.where(upper, up, down)
        on[at] = jnp.where(upper, down, up)

    for f in range(FIELDS):
        put(2 * f, fields[f, 2], fields[f, 0])
        put(2 * f + 1, fields[f, 3], fields[f, 1])
    put(50, fields[20, 1], fields[20, 2])
    lo, hi = y_lo[20], y_hi[20]
    put(51, jnp.where(first, shift_rows(lo, 4), hi), jnp.where(first, lo, shift_rows(hi, 4)))
    for v in range(6):
        a = jnp.zeros(TILE, F32)
        b = a
        for k in range(4):
            f = 4 * v + k + (1 if v == 5 else 0)
            lo, hi = y_lo[f], y_hi[f]
            a = jnp.where(row == 2 * k, shift_rows(lo, 2 * k - 7), a)
            a = jnp.where(row == 2 * k + 1, shift_rows(hi, 2 * k - 5), a)
            b = jnp.where(row == 2 * k, shift_rows(lo, 2 * k - 1), b)
            b = jnp.where(row == 2 * k + 1, shift_rows(hi, 2 * k + 1), b)
        put(52 + v, a, b)
    part = lax.rem(lanes_of(), 24)
    a = jnp.zeros(TILE, F32)
    b = a
    for p in range(4):
        tile = halo[p]
        here = (part >= 18 - 6 * p) & (part < 24 - 6 * p)
        a = jnp.where(here, shift_lanes(tile, -6 * p % Z) if p else tile, a)
        here = (part >= 6 * p) & (part < 6 * p + 6)
        b = jnp.where(here, shift_lanes(tile, 6 * p) if p else tile, b)
    put(58, a, b)
    corner = corner_of(4, y_lo, y_hi)
    put(59, halo[4], halo[4])
    put(60, corner, corner)


def region(radius):
    out = []
    for a, b in ((0, 0), (1, 0), (0, 1), (1, 1)):
        reach = radius - a - b
        if reach >= 0:
            out.extend((x, a, b) for x in range(-reach, X + reach))
    return out


COEF = region(2)


def tile_of(f, key, refs):
    fields, halo, y_lo, y_hi, x_lo, x_hi, y_halo, x_corner = refs
    x, a, b = key
    first = rows_of() < 4
    if b == 0:
        if a == 0:
            if 0 <= x < X:
                return fields[f, x]
            if x == -3:
                return x_lo[50]
            if x == 6:
                return x_hi[50]
            return x_lo[2 * f + x + 2] if x < 0 else x_hi[2 * f + x - 4]
        if 0 <= x < X:
            lo, hi = y_lo[f], y_hi[f]
            tile = jnp.where(first, shift_rows(hi, -2 * x), shift_rows(lo, 6 - 2 * x))
            if isinstance(f, int) and f == 20:
                row = rows_of()
                tile = jnp.where(row == 2, shift_rows(y_hi[25], 2 - x), tile)
                tile = jnp.where(row == 5, shift_rows(y_lo[25], 5 - x), tile)
            return tile
        side = x_lo if x < 0 else x_hi
        if not (isinstance(f, int) and f == 20):
            g = f - 1 if isinstance(f, int) and f > 20 else f
            v, k = (g // 4, g % 4) if isinstance(g, int) else (lax.div(g, 4), lax.rem(g, 4))
            return pltpu.roll(side[52 + v], 7 - 2 * k, 0)
        packed = side[51]
        if x in (-1, 5):
            return jnp.where(first, shift_rows(packed, 2), shift_rows(packed, 4))
        return jnp.where(first, shift_rows(packed, 4), shift_rows(packed, 6))
    p, q = (f // 5, f % 5) if isinstance(f, int) else (lax.div(f, 5), lax.rem(f, 5))
    place = x if 0 <= x < X else (x + X if x < 0 else x - X)
    by = 128 - 3 - 6 * (4 * q + place)
    if a == 0 and not 0 <= x < X and not (isinstance(f, int) and f >= KEEP):
        packed = (x_lo if x < 0 else x_hi)[58]
        by = 128 - 3 - 24 * q - (18 - 6 * p if x < 0 else 6 * p)
    elif a == 0:
        packed = halo[p] if 0 <= x < X else (x_lo if x < 0 else x_hi)[59]
    elif 0 <= x < X:
        packed = y_halo[p]
    else:
        packed = x_corner[0 if x < 0 else 1]
    return shift_lanes(packed, by)


def along_y(get, key, coef):
    x, a, b = key
    row = rows_of()
    centre, other = get(key), get((x, 1 - a, b))
    ahead = shift_rows(jnp.where(row == 0, other, centre), 7)
    behind = shift_rows(jnp.where(row == 7, other, centre), 1)
    return coef(key, 3) * ahead + coef(key, 4) * behind


def apply(get, key, coef, skip=()):
    x, a, b = key
    lane = lanes_of()
    centre, other = get(key), get((x, a, 1 - b))
    ahead = shift_lanes(jnp.where(lane == 0, other, centre), 127)
    behind = shift_lanes(jnp.where(lane == 127, other, centre), 1)
    total = coef(key, 5) * ahead + coef(key, 6) * behind
    total = along_y(get, key, coef) + total
    total = total + coef(key, 0) * centre
    for i, at in ((1, (x + 1, a, b)), (2, (x - 1, a, b))):
        if i not in skip:
            total = total + coef(key, i) * get(at)
    return total


def fill_coefficients(keys, out, refs):
    for at, key in enumerate(keys):
        diagonal = tile_of(21, key, refs)
        inside = diagonal != 0.0
        out[at, 0] = jnp.where(inside, diagonal - SIGMA, 0.0)
        for d in range(3):
            half = tile_of(22 + d, key, refs)
            out[at, 1 + 2 * d] = jnp.where(inside, half - 1.0, 0.0)
            out[at, 2 + 2 * d] = jnp.where(inside, -1.0 - half, 0.0)


def cached(f, refs):
    held = {}

    def get(key):
        if key not in held:
            held[key] = tile_of(f, key, refs)
        return held[key]

    return get


INNER = [key for key in COEF if 0 <= key[0] < X]
LEVEL = [key for key in INNER if not key[1] and not key[2]]
BESIDE = [key for key in INNER if key[1] or key[2]]
OUTER = [key for key in COEF if not 0 <= key[0] < X]
ONCE = [key for key in region(1) if 0 <= key[0] < X]
SIDES = {0: (2, -1), X - 1: (1, X)}


def skip_of(key):
    return (SIDES[key[0]][0],) if key[0] in SIDES else ()


def level_kernel(rest, coef_level):
    refs = (Fields(None, rest), None, None, None, None, None, None, None)
    fill_coefficients(LEVEL, coef_level, refs)


def inner_kernel(rotated, rest, halo, y_lo, y_hi, coef_level, coef_beside, partial, y_halo):
    for p in range(5):
        y_halo[p] = corner_of(p, y_lo, y_hi)
    refs = (Fields(rotated, rest), halo, y_lo, y_hi, None, None, y_halo, None)
    fill_coefficients(BESIDE, coef_beside, refs)

    def coef(key, i):
        if key in LEVEL:
            return coef_level[LEVEL.index(key), i]
        return coef_beside[BESIDE.index(key), i]

    def body(f, carry):
        get = cached(f, refs)
        once = {}
        for at, key in enumerate(ONCE):
            once[key] = apply(get, key, coef, skip_of(key))
            partial[f, at] = once[key]
        for x, skip in ((1, (2,)), (2, (1,))):
            partial[f, len(ONCE) + x - 1] = apply(once.__getitem__, (x, 0, 0), coef, skip)
        return carry

    lax.fori_loop(0, KEEP, body, 0, unroll=5)


def inner(a, b):
    return lax.dot_general(a, b, (((1,), (1,)), ((), ())), preferred_element_type=F32)


def stencil_kernel(
    copies,
    rotated,
    rest,
    halo,
    y_lo,
    y_hi,
    coef_level,
    coef_beside,
    partial,
    early,
    off,
    on,
    span,
    gram,
    coef_out,
    y_halo,
    x_corner,
    chain,
    x_lo,
    x_hi,
):
    fields = Fields(rotated, rest)
    upper = lax.axis_index("gx_1") == 1
    for i in range(on.shape[0]):
        far = early[i] if i < PLANES else off[i - PLANES]
        x_lo[i] = jnp.where(upper, on[i], far)
        x_hi[i] = jnp.where(upper, far, on[i])
    refs = (fields, halo, y_lo, y_hi, x_lo, x_hi, y_halo, x_corner)
    for p in range(5):
        y_halo[p] = corner_of(p, y_lo, y_hi)
    x_corner[0] = x_lo[60]
    x_corner[1] = x_hi[60]
    fill_coefficients(OUTER, coef_out, refs)

    def coef(key, i):
        if key in LEVEL:
            return coef_level[LEVEL.index(key), i]
        if key in BESIDE:
            return coef_beside[BESIDE.index(key), i]
        return coef_out[OUTER.index(key), i]

    def store(f, x, tile):
        at = f * (X * Y) + x * Y
        if not isinstance(f, int):
            at = pl.multiple_of(at, Y)
        span[pl.ds(at, Y), :] = tile

    tiles = {key: tile_of(20, key, refs) for key in region(3)}
    for x in range(X):
        store(60, x, tiles[(x, 0, 0)])
    for step in range(EXPAND):
        place = {}
        for at, key in enumerate(tiles):
            chain[at] = tiles[key]
            place[key] = at
        get = lambda key, place=place: chain[place[key]]
        tiles = {key: apply(get, key, coef) for key in region(2 - step)}
        for x in range(X):
            store(61 + step, x, tiles[(x, 0, 0)])

    def body(f, carry):
        get = cached(f, refs)
        once = {}
        for at, key in enumerate(ONCE):
            x, a, b = key
            if x not in SIDES and (a or b):
                continue
            tile = partial[f, at]
            if x in SIDES:
                i, side = SIDES[x]
                tile = tile + coef(key, i) * get((side, a, b))
            once[key] = tile
        for x in (-1, X):
            once[(x, 0, 0)] = apply(get, (x, 0, 0), coef)
        for x in range(X):
            store(f, x, get((x, 0, 0)))
            store(f + 20, x, once[(x, 0, 0)])
        for x in SIDES:
            store(f + 40, x, apply(once.__getitem__, (x, 0, 0), coef))
        for x, i, near in ((1, 2, 0), (2, 1, 3)):
            term = coef((x, 0, 0), i) * once[(near, 0, 0)]
            store(f + 40, x, partial[f, len(ONCE) + x - 1] + term)
        return carry

    lax.fori_loop(0, KEEP, body, 0, unroll=5)

    even = jnp.zeros((SPAN, SPAN), F32)
    mixed = even
    for r in range(0, X * Y, 2):
        pair = [span[pl.ds(r + i, SPAN, stride=X * Y), :] for i in range(2)]
        rows = jnp.concatenate(pair, axis=1)
        high = rows.astype(jnp.bfloat16)
        left = rows - high.astype(F32)
        middle = left.astype(jnp.bfloat16)
        low = (left - middle.astype(F32)).astype(jnp.bfloat16)
        even = even + (inner(high, high) + inner(middle, middle))
        mixed = mixed + (inner(high, middle) + inner(high, low))
    square = jnp.concatenate([mixed, jnp.zeros((SPAN, Z - SPAN), F32)], axis=1)
    square = jnp.concatenate([square, jnp.zeros((Z - SPAN, Z), F32)], axis=0)
    total = even + (mixed + square.T[:SPAN, :SPAN])
    wide = jnp.concatenate([total, jnp.zeros((SPAN, Z - SPAN), F32)], axis=1)
    lane = lanes_of()
    tiles = []
    for pieces in PIECES:
        tile = jnp.zeros(TILE, F32)
        for i, at in pieces:
            moved = wide[Y * i : Y * (i + 1)]
            moved = shift_lanes(moved, (at - Y * i) % Z) if at != Y * i else moved
            tile = jnp.where((lane >= at) & (lane < at + SPAN - Y * i), moved, tile)
        tiles.append(tile)
    extra = jnp.zeros(TILE, F32)
    for g in range(4):
        tile = shift_rows(wide[32:40], -2 * g)
        tile = shift_lanes(tile, (32 * g - 32) % Z) if g != 1 else tile
        extra = jnp.where((lane >= 32 * g) & (lane < 32 * g + 32), tile, extra)
    for i in range(copies):
        c = i // (copies // 2)
        for k in range(Y):
            gram[i, :, Z * k : Z * (k + 1)] = tiles[c][k : k + 1]
        gram[i, :, Z * Y :] = extra[c : c + 1]


PIECES = (((0, 0), (1, 64), (7, 120)), ((2, 0), (3, 48), (5, 88), (6, 112)))


def sum_kernel(copies, parts, out):
    total = parts[0]
    for i in range(1, parts.shape[0]):
        total = total + parts[i]
    for i in range(copies):
        out[i] = total


def exchange(parts, axis):
    return lax.all_to_all(parts, axis, 0, 0)


def finish_kernel(cell_count, parts, span, basis, hessenberg, spread, fresh, sems):
    early = pltpu.make_async_copy(
        span.at[pl.ds(0, KEEP)], basis.at[pl.ds(0, KEEP)], sems.at[0]
    )
    early.start()
    late = [
        pltpu.make_async_copy(fresh.at[k], basis.at[KEEP + k], sems.at[1 + k])
        for k in range(ROWS - KEEP)
    ]
    row, lane = rows_of(), lanes_of()
    rows = [None] * 8
    extra = jnp.zeros(TILE, F32)
    for c in range(2):
        tile = jnp.zeros(TILE, F32)
        for k in range(Y):
            tile = jnp.where(row == k, parts[c, :, Z * k : Z * (k + 1)], tile)
        tile = tile * (1.0 / cell_count)
        for i, at in PIECES[c]:
            moved = shift_lanes(tile, (Y * i - at) % Z) if at != Y * i else tile
            rows[i] = jnp.where((lane >= Y * i) & (lane < SPAN), moved, 0.0)
        extra = jnp.where(row == c, parts[c, :, Z * Y :], extra)
    extra = extra * (1.0 / cell_count)
    tile = jnp.zeros(TILE, F32)
    for g in range(4):
        moved = shift_lanes(extra, (32 - 32 * g) % Z) if g != 1 else extra
        tile = jnp.where((row >= 2 * g) & (row < 2 * g + 2), shift_rows(moved, 2 * g), tile)
    rows[4] = jnp.where((lane >= 32) & (lane < SPAN), tile, 0.0)
    blocks = jnp.concatenate([*rows, jnp.zeros((Z - SPAN, Z), F32)], axis=0)
    across = lax.broadcasted_iota(jnp.int32, (Z, Z), 1) // Y
    down = lax.broadcasted_iota(jnp.int32, (Z, Z), 0) // Y
    gram = (blocks + jnp.where(across < down, blocks.T, 0.0))[:SPAN]
    row64 = lax.broadcasted_iota(jnp.int32, (SPAN, Z), 0)
    lane64 = lax.broadcasted_iota(jnp.int32, (SPAN, Z), 1)
    eye = row64 == lane64
    moved = ((row64 >= KEEP) & (row64 < 60) & (lane64 == row64 - KEEP)) | (
        (row64 > 60) & (lane64 == row64 - 1)
    )
    row = lax.broadcasted_iota(jnp.int32, (ROWS, Z), 0)
    lane = lax.broadcasted_iota(jnp.int32, (ROWS, Z), 1)
    lane1 = lax.broadcasted_iota(jnp.int32, (1, Z), 1)

    def column(vector, picks):
        return jnp.sum(jnp.where(picks, vector, 0.0), axis=1, keepdims=True)

    first_row = gram[60:61, :]
    norm_sq = jnp.sum(jnp.where(lane1 == 60, first_row, 0.0), axis=1, keepdims=True)
    inverse = lax.rsqrt(jnp.maximum(norm_sq, 0.25))
    last = jnp.where(lane1 == 60, inverse, 0.0)
    last_gram = first_row * inverse
    up_column = jnp.where(lax.broadcasted_iota(jnp.int32, (SPAN, 1), 0) == 61, inverse, 0.0)
    q = jnp.where((row == lane) & (row < KEEP), 1.0, 0.0)
    q = jnp.where(row == KEEP, last, q)
    qg = jnp.where(row < KEEP, gram[:ROWS, :], 0.0)
    qg = jnp.where(row == KEEP, last_gram, qg)
    scale = jnp.broadcast_to(inverse, TILE)
    for x in range(X):
        fresh[0, x] = span[60, x] * scale
    late[0].start()
    for k in range(EXPAND):
        up = jnp.where(
            (lane1 >= KEEP) & (lane1 < 60),
            pltpu.roll(last, KEEP, 1),
            jnp.where((lane1 > 60) & (lane1 < SPAN), pltpu.roll(last, 1, 1), 0.0),
        )
        image = up + SIGMA * last
        image_gram = jnp.sum(up_column * gram, axis=0, keepdims=True) + SIGMA * last_gram
        c = jnp.sum(q * image_gram, axis=1, keepdims=True)
        partly = image - jnp.sum(c * q, axis=0, keepdims=True)
        partly_gram = image_gram - jnp.sum(c * qg, axis=0, keepdims=True)
        e = jnp.sum(q * partly_gram, axis=1, keepdims=True)
        cleaned = partly - jnp.sum(e * q, axis=0, keepdims=True)
        cleaned_gram = partly_gram - jnp.sum(e * qg, axis=0, keepdims=True)
        length_sq = jnp.sum(cleaned * cleaned_gram, axis=1, keepdims=True)
        here, shifted = column(cleaned, eye), column(cleaned, moved)
        inverse = lax.rsqrt(jnp.maximum(length_sq, 0.25))
        last = cleaned * inverse
        last_gram = cleaned_gram * inverse
        up_column = shifted * inverse
        q = jnp.where(row == KEEP + 1 + k, last, q)
        qg = jnp.where(row == KEEP + 1 + k, last_gram, qg)
        length = jnp.sqrt(jnp.maximum(length_sq, 0.0))
        entries = jnp.where(row == KEEP + 1 + k, length, c + e)
        turned = jnp.sum(jnp.where(row == lane, entries, 0.0), axis=0, keepdims=True)
        hessenberg[k : k + 1, :] = turned[:, :ROWS]
        spread[pl.ds(8 * k, 8)] = jnp.broadcast_to(here * inverse, (SPAN, Z)).reshape(8, 8, Z)
        fields = [*range(KEEP * (k + 1)), *range(60, 62 + k)]
        acc = [jnp.zeros(TILE, F32) for _ in range(X)]
        for f in fields:
            w = spread[8 * k + f // 8, f % 8 : f % 8 + 1, :]
            for x in range(X):
                acc[x] = acc[x] + w * span[f, x]
        for x in range(X):
            fresh[1 + k, x] = acc[x]
        late[1 + k].start()
    early.wait()
    for copy in late:
        copy.wait()


def send(value, axis, forward):
    count = lax.axis_size(axis)
    up = [(i, i + 1) for i in range(count - 1)]
    return lax.ppermute(value, axis, up if forward else [(j, i) for i, j in up])


def per_device(krylov_basis, schur_vectors, next_vector, diag_shift, velocity):
    axes = (*GX, "gy", "gz")
    cell_count = next_vector.size
    for axis in axes:
        cell_count *= lax.axis_size(axis)
    held, rest, packed, passed = call(
        edge_kernel,
        [
            krylov_basis.shape,
            (FIELDS - KEEP, X, Y, Z),
            (5, Y, Z),
            (KEEP, krylov_basis.shape[0]),
        ],
        [
            pltpu.with_memory_space_constraint(value, pltpu.HBM)
            for value in (krylov_basis, schur_vectors.T, next_vector, diag_shift, velocity)
        ],
        scratch=[
            pltpu.SMEM((KEEP, krylov_basis.shape[0]), F32),
            pltpu.VMEM((4, X, Y, Z), F32),
            pltpu.SemaphoreType.DMA((5 + krylov_basis.shape[0] // CHUNK,)),
        ],
        ins="hhhhh",
        limit=4,
    )
    z_lo, z_hi = send(packed, "gz", True), send(packed, "gz", False)
    (rotated,) = call(
        rotate_kernel,
        [(KEEP, X, Y, Z)],
        [held, passed],
        ins="vs",
        limit=4,
        flops=10**9,
    )
    up, down, halo = call(
        pack_y_kernel, [(27, Y, Z), (27, Y, Z), (5, Y, Z)], [rotated, rest, z_lo, z_hi]
    )
    count = lax.axis_size(GX)
    swap = [(i, i + 1) for i in range(1, count - 1, 2)]
    swap = swap + [(j, i) for i, j in swap]
    y_lo = send(up, "gy", True)
    y_hi = send(down, "gy", False)
    (early,) = call(planes_kernel, [(PLANES, Y, Z)], [rotated, rest])
    early = lax.ppermute(early, GX, swap)
    (coef_level,) = call(level_kernel, [(len(LEVEL), 7, Y, Z)], [rest])
    off, on = call(
        pack_x_kernel, [(61 - PLANES, Y, Z), (61, Y, Z)], [rotated, rest, halo, y_lo, y_hi]
    )
    off = lax.ppermute(off, GX, swap)
    on = lax.ppermute(on, "gx_1", [(0, 1), (1, 0)])
    stages = (("gx_1", "gz"), ("gx_0", "gy"))
    sizes = [lax.axis_size(stage) for stage in stages]
    coef_beside, partial = call(
        inner_kernel,
        [(len(BESIDE), 7, Y, Z), (KEEP, len(ONCE) + 2, Y, Z)],
        [rotated, rest, halo, y_lo, y_hi, coef_level],
        scratch=[pltpu.VMEM((5, Y, Z), F32)],
        limit=6,
        flops=10**9,
    )
    span, parts = call(
        functools.partial(stencil_kernel, sizes[0]),
        [(SPAN * X * Y, Z), (sizes[0], 1, WIRE)],
        [rotated, rest, halo, y_lo, y_hi, coef_level, coef_beside, partial, early, off, on],
        scratch=[
            pltpu.VMEM((len(OUTER), 7, Y, Z), F32),
            pltpu.VMEM((5, Y, Z), F32),
            pltpu.VMEM((2, Y, Z), F32),
            pltpu.VMEM((len(region(3)), Y, Z), F32),
            pltpu.VMEM((61, Y, Z), F32),
            pltpu.VMEM((61, Y, Z), F32),
        ],
        limit=8,
    )
    parts = exchange(parts, stages[0])
    (parts,) = call(functools.partial(sum_kernel, sizes[1]), [(sizes[1], 1, WIRE)], [parts])
    parts = exchange(parts, stages[1])
    (half,) = call(functools.partial(sum_kernel, 1), [(1, 1, WIRE)], [parts])
    whole = lax.all_gather(half, "gx_1", axis=0, tiled=True)
    basis, hessenberg = call(
        functools.partial(finish_kernel, cell_count),
        [(ROWS, X, Y, Z), (EXPAND, ROWS)],
        [whole, span.reshape(SPAN, X, Y, Z)],
        scratch=[
            pltpu.VMEM((8 * EXPAND, Y, Z), F32),
            pltpu.VMEM((ROWS - KEEP, X, Y, Z), F32),
            pltpu.SemaphoreType.DMA((1 + ROWS - KEEP,)),
        ],
        out="hv",
        limit=4,
    )
    return basis, hessenberg.T


def solution(mesh):
    split = Mesh(
        mesh.devices.reshape(-1, 2, mesh.shape["gy"], mesh.shape["gz"]),
        ("gx_0", "gx_1", "gy", "gz"),
    )
    return jax.shard_map(
        per_device,
        mesh=split,
        in_specs=(
            P(None, GX, "gy", "gz"),
            P(),
            P(GX, "gy", "gz"),
            P(GX, "gy", "gz"),
            P(None, GX, "gy", "gz"),
        ),
        out_specs=(P(None, GX, "gy", "gz"), P()),
        check_vma=False,
    )
```
